256 devices in a mesh: gx: 8 (over z), gy: 16 (over y_hi, x, core), ens: 2 (over y_lo).
Axes of the slice: x: 4, y: 4 (y_hi: 2, y_lo: 2; y = y_hi * 2 + y_lo), z: 8, core: 2. Of those that a mesh axis runs over, the one named last changes fastest.
Arguments:
- state: float32 [128, 256, 1024], P('ens', 'gy', 'gx'), may hold values from -6 to 6
- u_vel: float32 [256, 1024], P('gy', 'gx'), may hold values from -0.4 to 0.4
- v_vel: float32 [256, 1024], P('gy', 'gx'), may hold values from -0.4 to 0.4
- land: int32 [256, 1024], P('gy', 'gx'), may hold values 0 or 1
- forcing: float32 [8, 256, 1024], P(None, 'gy', 'gx'), may hold values from -3 to 3
- member_mode: int32 [128], P('ens'), may hold values from 0 to 7
- theta: float32 [128, 4], P('ens'), may hold values from -1 to 1
- obs_index: int32 [16, 8, 128], P('gy', 'gx'), may hold values from 0 to 2047
- obs_values: float32 [16, 8, 128], P('gy', 'gx'), may hold values from -6 to 6
- obs_sigma: float32 [16, 8, 128], P('gy', 'gx'), may hold values from 0.5 to 4
Outputs:
- final_state: float32 [128, 256, 1024], P('ens', 'gy', 'gx')
- new_theta: float32 [128, 4], P('ens')
The draws below stay inside these ranges and needn't reach their ends.
All inputs are finite; a program needn't handle non-finite values. No bound on the sum of `land` on one device may be relied on, other than what follows from the above.
Results may differ from the reference program's by a relative error of at most 0.0003.
Values sent between devices are 32-bit elements; how exact they have to be, the bound alone decides.
A program may use at most 64 MiB of HBM per device.

```python
import math
import jax
import jax.numpy as jnp
from jax import lax

M = 128
P_SIZE = 4
K = 8
CX = 128
CY = 16
OBS_T = 128
STEPS = 4
NX = 1024
NY = 256
N_GX = 8
N_GY = 16


def plant(entries, own_key, least, top_value):
    extent = entries.shape
    place = [jax.random.randint(jax.random.fold_in(own_key, axis), (), 0, extent[axis]) for axis in range(len(extent))]
    entries = entries.at[tuple(place)].set(least)
    longest = extent.index(max(extent))
    place[longest] = (place[longest] + 1) % extent[longest]
    return entries.at[tuple(place)].set(top_value)


def block_scale(stream_key, extent, cuts, low, largest):
    def one(dim, blocks):
        draws = jax.random.uniform(jax.random.fold_in(jax.random.fold_in(stream_key, 6), dim), (blocks,), jnp.float32, low / len(cuts), largest / len(cuts))
        return jnp.repeat(jnp.exp(draws), extent[dim] // blocks).reshape((-1,) + (1,) * (len(extent) - dim - 1))

    level = one(*cuts[0])
    for cut in cuts[1:]:
        level = level * one(*cut)
    return level


def scatter_about(key, dims, width, bound, shards=(), kind=jnp.bfloat16):
    gain = block_scale(key, dims, shards, -0.22, 0.18) if shards else 1.0
    drawn = jax.random.normal(key, dims, jnp.float32) * width * gain
    return jnp.minimum(jnp.maximum(drawn, -bound), bound).astype(kind)


def setup_inputs(seed: int = 0) -> dict:
    streams_of = jax.random.split(jax.random.key(seed), 11)
    return {
        "state": scatter_about(streams_of[0], (M, NY, NX), 1.0, 6.0, ((0, 2), (1, 16), (2, 8)), jnp.float32),
        "u_vel": jnp.clip(jax.random.uniform(streams_of[1], (NY, NX), jnp.float32, -0.4, 0.4) * block_scale(streams_of[1], (NY, NX), ((0, 16), (1, 8)), -0.4, 0.0), -0.4, 0.4),
        "v_vel": jnp.clip(jax.random.uniform(streams_of[2], (NY, NX), jnp.float32, -0.4, 0.4) * block_scale(streams_of[2], (NY, NX), ((0, 16), (1, 8)), -0.4, 0.0), -0.4, 0.4),
        "land": plant((jax.random.randint(streams_of[3], (NY, NX), 0, 8) < 1).astype(jnp.int32), jax.random.fold_in(streams_of[3], 1), 0, 1),
        "forcing": scatter_about(streams_of[4], (K, NY, NX), 0.5, 3.0, ((1, 16), (2, 8)), jnp.float32),
        "member_mode": plant(jax.random.randint(streams_of[5], (M,), 0, K), jax.random.fold_in(streams_of[5], 1), 0, K - 1).astype(jnp.int32),
        "theta": jnp.clip(jax.random.uniform(streams_of[6], (M, P_SIZE), jnp.float32, -1.0, 1.0) * block_scale(streams_of[6], (M, P_SIZE), ((0, 2),), -0.4, 0.0), -1.0, 1.0),
        "obs_index": plant(jax.random.randint(streams_of[7], (N_GY, N_GX, OBS_T), 0, CY * CX), jax.random.fold_in(streams_of[7], 1), 0, (CY * CX) - 1).astype(jnp.int32),
        "obs_values": scatter_about(streams_of[8], (N_GY, N_GX, OBS_T), 1.0, 6.0, ((0, 16), (1, 8)), jnp.float32),
        "obs_sigma": jnp.clip(jnp.exp(math.log(4.0) - 2.0794415 * jax.random.uniform(streams_of[9], (N_GY, N_GX, OBS_T), jnp.float32) ** block_scale(streams_of[9], (N_GY, N_GX, OBS_T), ((0, 16), (1, 8)), -0.2, 0.2)), 0.5, 4.0),
    }


def laplace(field):
    upper = jnp.pad(field[1:], ((0, 1), (0, 0)))
    lower = jnp.pad(field[:-1], ((1, 0), (0, 0)))
    return upper + lower + jnp.roll(field, -1, 1) + jnp.roll(field, 1, 1) - 4.0 * field

def reference(state, u_vel, v_vel, land, forcing, member_mode, theta, obs_index, obs_values, obs_sigma):
    ocean = (1 - land).astype(jnp.float32)
    tile_rows = jnp.arange(N_GY, dtype=jnp.int32)[:, None, None] * CY
    tile_cols = jnp.arange(N_GX, dtype=jnp.int32)[None, :, None] * CX
    site_rows = (tile_rows + obs_index // CX).reshape(-1)
    site_cols = (tile_cols + obs_index % CX).reshape(-1)

    def advance(member_data):
        field, mode, params = member_data
        diffuse = 0.05 * (1.0 + 0.5 * jnp.tanh(params[0]))
        hyper = 0.005 * (1.0 + 0.5 * jnp.tanh(params[1]))
        damping = 0.05 * (1.0 + 0.5 * jnp.tanh(params[2]))
        forced = params[3] * forcing[mode]
        for step_index in range(STEPS):
            lap_field = laplace(field)
            biharm = laplace(lap_field)
            upper = jnp.pad(field[1:], ((0, 1), (0, 0)))
            lower = jnp.pad(field[:-1], ((1, 0), (0, 0)))
            grad_x = 0.5 * (jnp.roll(field, -1, 1) - jnp.roll(field, 1, 1))
            grad_y = 0.5 * (upper - lower)
            tend = diffuse * lap_field - hyper * biharm - damping * field + forced - (u_vel * grad_x + v_vel * grad_y)
            field = (field + tend) * ocean
        return (field, field[site_rows, site_cols])
    final_state, observed = lax.map(advance, (state, member_mode, theta))
    sigma = obs_sigma.reshape(-1)
    target = obs_values.reshape(-1)
    anomaly = (observed - jnp.mean(observed, 0)) / sigma
    misfit = (target - observed) / sigma
    gram = jnp.dot(anomaly.astype(jnp.float32), anomaly.T.astype(jnp.float32), preferred_element_type=jnp.float32, precision=lax.Precision.HIGHEST)
    cross = jnp.dot(anomaly.astype(jnp.float32), misfit.T.astype(jnp.float32), preferred_element_type=jnp.float32, precision=lax.Precision.HIGHEST)
    system = gram + (M - 1) * jnp.eye(M, dtype=jnp.float32)
    weights = jnp.linalg.solve(system, cross)
    spread = theta - jnp.mean(theta, 0)
    new_theta = theta + jnp.dot(weights.T.astype(jnp.float32), spread.astype(jnp.float32), preferred_element_type=jnp.float32, precision=lax.Precision.HIGHEST)
    return (final_state, new_theta)
```

```python
import jax
import jax.numpy as jnp
from jax import lax
from jax.experimental import pallas as pl
from jax.experimental.pallas import tpu as pltpu
from jax.sharding import PartitionSpec as P

STEPS = 4
W = 2 * STEPS
MESH = pl.DeviceIdType.MESH
F32 = jnp.float32
HIGHEST = lax.Precision.HIGHEST
CHUNK = 16


def iota(shape, dim):
    return lax.broadcasted_iota(jnp.int32, shape, dim)


def pack_edges(ref, first, rows, count, r_ref, l_ref, group):
    lo, hi = rows
    slot = iota((hi - lo, 128), 1) // 16
    for n in range(count):
        right = left = None
        for k in range(8):
            x = ref[first + 8 * n + k, lo:hi, :]
            a = pltpu.roll(x, (16 * (k + 1)) % 128, 1) if k < 7 else x
            b = pltpu.roll(x, 16 * k, 1) if k else x
            right = a if right is None else jnp.where(slot == k, a, right)
            left = b if left is None else jnp.where(slot == k, b, left)
        r_ref[group + n, lo:hi, :] = right
        l_ref[group + n, lo:hi, :] = left


def strips_of(rv, lv, rvr, lvr, lo, hi):
    inner = iota((hi - lo, 128), 1) % 32 < 16
    left = (
        jnp.where(inner, rvr, pltpu.roll(lv, 16, 1)),
        jnp.where(inner, pltpu.roll(rvr, 112, 1), lv),
    )
    right = (
        jnp.where(inner, rv, pltpu.roll(lvr, 16, 1)),
        jnp.where(inner, pltpu.roll(rv, 112, 1), lvr),
    )
    return left, right


def advance(first, planes, coef, tables, forced, qs, lqs, es, mask, put):
    c0, c1, hy = coef
    ocean, uo, vo = tables
    for step in range(STEPS):
        lo = 2 * step
        nl = 4 * W - 2 - 4 * step
        nn = nl - 2
        for p in range(planes):
            get = (lambda a, n, p=p: first(p, a, n)) if step == 0 else (lambda a, n, p=p: qs[p, a : a + n, :])
            cen = get(lo + 1, nl)
            west = pltpu.roll(cen, 1, 1)
            east = pltpu.roll(cen, 127, 1)
            lap = (get(lo + 2, nl) + get(lo, nl)) + (west + east) - 4.0 * cen
            lqs[p, lo + 1 : lo + 1 + nl, :] = lap * mask[lo + 1 : lo + 1 + nl, :]
            es[p, lo + 1 : lo + 1 + nl, :] = east - west
        at = slice(lo + 2, lo + 2 + nn)
        for p in range(planes):
            get = (lambda a, n, p=p: first(p, a, n)) if step == 0 else (lambda a, n, p=p: qs[p, a : a + n, :])
            lap = lqs[p, at, :]
            around = (lqs[p, lo + 3 : lo + 3 + nn, :] + lqs[p, lo + 1 : lo + 1 + nn, :]) + (
                pltpu.roll(lap, 1, 1) + pltpu.roll(lap, 127, 1)
            )
            dy = get(lo + 3, nn) - get(lo + 1, nn)
            inner = c0(p) * get(lo + 2, nn) + c1(p) * lap - hy(p) * around + forced(p, lo + 2, nn)
            new = ocean(p, lo + 2, nn) * inner - (
                uo(p, lo + 2, nn) * es[p, at, :] + vo(p, lo + 2, nn) * dy
            )
            if step < STEPS - 1:
                qs[p, at, :] = new
            else:
                put(p, new)


def kernel(
    mode, state, u_vel, v_vel, land, forcing, theta, obs_index, obs_values, obs_sigma,
    fin_out, theta_out,
    qx, ex, landb, rv, lv, rvr, lvr, mask, tabs, ftab, stabs, coefs, pcoefs,
    qs, lqs, es, fos, qp, qps, lqps, eps, fops, endp, fin, oall, thx, thr,
    gp, rs, zs, ag, mat,
    lsem, osem, hs, hr, xs, xr, rss, rsr, zss, zsr, ags, agr,
):
    z, g, e = lax.axis_index("gx"), lax.axis_index("gy"), lax.axis_index("ens")
    nz, ng = 8, 16
    up_ok, down_ok = g > 0, g < ng - 1

    def dev(dz, dg):
        return {"gx": lax.rem(z + dz + nz, nz), "gy": lax.rem(g + dg + ng, ng), "ens": e}

    pair = {"gx": z, "gy": g, "ens": 1 - e}
    barrier = pltpu.get_barrier_semaphore()
    partners = [dev(0, d) for d in range(1, ng)] + [dev(d, 0) for d in range(1, nz)] + [pair]
    partners += [dev(a, b) for a in (-1, 1) for b in (-1, 1)]
    for where in partners:
        pl.semaphore_signal(barrier, inc=1, device_id=where, device_id_type=MESH)

    own = pl.ds(W, 16)
    loads = [
        pltpu.make_async_copy(state, qx.at[:, own, :], lsem.at[0]),
        pltpu.make_async_copy(forcing, ex.at[0:8, own, :], lsem.at[1]),
        pltpu.make_async_copy(u_vel, ex.at[8, own, :], lsem.at[2]),
        pltpu.make_async_copy(v_vel, ex.at[9, own, :], lsem.at[3]),
        pltpu.make_async_copy(land, landb, lsem.at[4]),
    ]
    for c in loads:
        c.start()

    lane64 = iota((64, 128), 1)
    diag = lane64 == iota((64, 128), 0) + 64 * e
    tt = theta[...]
    th = jnp.tanh(tt)
    spread4 = [jnp.broadcast_to(th[:, p : p + 1], (64, 128)) for p in range(3)]
    raw4 = [jnp.broadcast_to(tt[:, p : p + 1], (64, 128)) for p in range(4)]
    hyper = 0.005 * (1.0 + 0.5 * spread4[1])
    coefs[0] = 1.0 - 0.05 * (1.0 + 0.5 * spread4[2])
    coefs[1] = 0.05 * (1.0 + 0.5 * spread4[0]) + 4.0 * hyper
    coefs[2] = hyper
    coefs[3] = raw4[3]
    thx[...] = jnp.zeros((8, 128), F32)
    for p in range(4):
        thx[p : p + 1, :] = jnp.sum(jnp.where(diag, raw4[p], 0.0), axis=0, keepdims=True)
    slot8 = iota((8, 128), 1) // 32
    for t in range(4):
        for odd in range(2):
            acc = None
            for k in range(4):
                x = coefs[t, pl.ds(odd + 2 * k, 8, stride=8), :]
                acc = x if acc is None else jnp.where(slot8 == k, x, acc)
            pcoefs[t, odd] = acc
    row32 = iota((32, 128), 0)
    no_wall = (jnp.logical_or(row32 >= W, up_ok)) & (jnp.logical_or(row32 < W + 16, down_ok))
    mask[...] = no_wall.astype(F32)

    for c in loads[1:]:
        c.wait()
    ex[10, W : W + 16, :] = (1 - landb[...]).astype(F32)
    ex[11:16, W : W + 16, :] = jnp.zeros((5, 16, 128), F32)

    @pl.when(jnp.logical_not(up_ok))
    def _():
        for ref in (qx, ex, rvr, lvr):
            ref[:, 0:W, :] = jnp.zeros((ref.shape[0], W, 128), F32)

    @pl.when(jnp.logical_not(down_ok))
    def _():
        for ref in (qx, ex, rvr, lvr):
            ref[:, W + 16 :, :] = jnp.zeros((ref.shape[0], W, 128), F32)

    pack_edges(ex, 0, (W, W + 16), 2, rv, lv, 8)
    loads[0].wait()

    def pack_own(c, carry):
        pack_edges(qx, 16 * c, (W, W + 16), 2, rv, lv, 2 * c)
        return carry

    lax.fori_loop(0, 4, pack_own, 0)

    top, bottom, low, high = pl.ds(W, W), pl.ds(16, W), pl.ds(0, W), pl.ds(W + 16, W)

    def halo(c, planes, first, group):
        at, ga = pl.ds(first, 16), pl.ds(group, 2)
        plan = [
            (planes, at, top, planes, high, (0, -1), up_ok, down_ok),
            (planes, at, bottom, planes, low, (0, 1), down_ok, up_ok),
            (rv, ga, own, rvr, own, (1, 0), None, None),
            (lv, ga, own, lvr, own, (-1, 0), None, None),
            (rv, ga, bottom, rvr, low, (1, 1), down_ok, up_ok),
            (rv, ga, top, rvr, high, (1, -1), up_ok, down_ok),
            (lv, ga, bottom, lvr, low, (-1, 1), down_ok, up_ok),
            (lv, ga, top, lvr, high, (-1, -1), up_ok, down_ok),
        ]
        out = []
        for i, (src, a, sr, dst, dr, where, sends, gets) in enumerate(plan):
            copy = pltpu.make_async_remote_copy(
                src_ref=src.at[a, sr, :], dst_ref=dst.at[a, dr, :],
                send_sem=hs.at[c, i], recv_sem=hr.at[c, i],
                device_id=dev(*where), device_id_type=MESH,
            )
            out.append((copy, sends, gets))
        return out

    def when(cond, fn):
        if cond is None:
            fn()
        else:
            pl.when(cond)(fn)

    pl.semaphore_wait(barrier, len(partners))
    for copy, sends, _ in halo(4, ex, 0, 8):
        when(sends, copy.start)

    def send_chunk(c, carry):
        for copy, sends, _ in halo(c, qx, 16 * c, 2 * c):
            when(sends, copy.start)
        return carry

    lax.fori_loop(0, 4, send_chunk, 0)
    swap_theta = pltpu.make_async_remote_copy(
        src_ref=thx, dst_ref=thr, send_sem=xs.at[0], recv_sem=xr.at[0], device_id=pair, device_id_type=MESH
    )
    swap_theta.start()

    for copy, _, gets in halo(4, ex, 0, 8):
        when(gets, copy.wait_recv)
    for rows in ((0, W), (W + 16, 32)):
        pack_edges(ex, 0, rows, 2, rv, lv, 8)
    o = ex[10]
    tabs[0] = o
    tabs[1] = 0.5 * ex[8] * o
    tabs[2] = 0.5 * ex[9] * o
    slot32 = iota((32, 128), 1) // 32

    def spread(x, k):
        y = jnp.where(slot32 == k, x, 0.0)
        y = y + pltpu.roll(y, 32, 1)
        return y + pltpu.roll(y, 64, 1)

    both = strips_of(rv[8], lv[8], rvr[8], lvr[8], 0, 32)
    for side in range(2):
        for k in range(8):
            ftab[side, k] = spread(both[side][k % 2], k // 2)
    both = strips_of(rv[9], lv[9], rvr[9], lvr[9], 0, 32)
    for side in range(2):
        even, odd = both[side]
        o = spread(even, 1)
        stabs[side, 0] = o
        stabs[side, 1] = 0.5 * spread(even, 0) * o
        stabs[side, 2] = 0.5 * spread(odd, 0) * o

    site = obs_index[0]
    site_col = jnp.broadcast_to(site % 128, (16, 128))
    site_row = jnp.broadcast_to(site // 128, (16, 128)) == iota((16, 128), 0)
    lane = iota((16, 128), 1)
    slot16 = lane % 32 < 16
    edge = (lane < W) | (lane >= 128 - W)

    def out_copy(c):
        at = pl.ds(16 * c, 16)
        return pltpu.make_async_copy(fin.at[at], fin_out.at[at], osem.at[c])

    def chunk(c, carry):
        m0 = 16 * c
        for copy, _, gets in halo(c, qx, m0, 2 * c):
            when(gets, copy.wait_recv)
        for rows in ((0, W), (W + 16, 32)):
            pack_edges(qx, m0, rows, 2, rv, lv, 2 * c)
        for p in range(16):
            fos[p] = coefs[3, pl.ds(m0 + p, 1), :] * ex[mode[m0 + p]]

        def keep(p, new):
            fin[m0 + p] = new

        advance(
            lambda p, a, n: qx[m0 + p, a : a + n, :], 16,
            [lambda p, t=t: coefs[t, pl.ds(m0 + p, 1), :] for t in range(3)],
            [lambda p, a, n, t=t: tabs[t, a : a + n, :] for t in range(3)],
            lambda p, a, n: fos[p, a : a + n, :], qs, lqs, es, mask, keep,
        )
        for n in range(2):
            gr = 2 * c + n
            both = strips_of(rv[gr], lv[gr], rvr[gr], lvr[gr], 0, 32)
            for side in range(2):
                for odd in range(2):
                    p = 4 * n + 2 * side + odd
                    qp[p] = both[side][odd]
                    f = None
                    for k in range(4):
                        x = ftab[side, mode[m0 + 8 * n + 2 * k + odd]]
                        f = x if f is None else jnp.where(slot32 == k, x, f)
                    fops[p] = pcoefs[3, odd, pl.ds(gr, 1), :] * f

        def keep_strip(p, new):
            endp[p] = new

        advance(
            lambda p, a, n: qp[p, a : a + n, :], 8,
            [lambda p, t=t: pcoefs[t, p % 2, pl.ds(2 * c + p // 4, 1), :] for t in range(3)],
            [lambda p, a, n, t=t: stabs[(p // 2) % 2, t, a : a + n, :] for t in range(3)],
            lambda p, a, n: fops[p, a : a + n, :], qps, lqps, eps, mask, keep_strip,
        )
        for n in range(2):
            for odd in range(2):
                ends = jnp.where(slot16, endp[4 * n + 2 + odd], endp[4 * n + odd])
                for k in range(4):
                    p = 8 * n + 2 * k + odd
                    moved = pltpu.roll(ends, (112 - 32 * k) % 128, 1)
                    whole = jnp.where(edge, moved, fin[m0 + p])
                    fin[m0 + p] = whole
                    seen = jnp.where(site_row, jnp.take_along_axis(whole, site_col, axis=1), 0.0)
                    oall[e, pl.ds(m0 + p, 1), :] = jnp.sum(seen, axis=0, keepdims=True)
        out_copy(c).start()
        return carry

    lax.fori_loop(0, 4, chunk, 0)

    swap_seen = pltpu.make_async_remote_copy(
        src_ref=oall.at[e], dst_ref=oall.at[e], send_sem=xs.at[1], recv_sem=xr.at[1],
        device_id=pair, device_id_type=MESH,
    )
    swap_seen.start()
    got_seen = pltpu.make_async_remote_copy(
        src_ref=oall.at[e], dst_ref=oall.at[1 - e], send_sem=xs.at[1], recv_sem=xr.at[1],
        device_id=pair, device_id_type=MESH,
    )
    got_seen.wait_recv()
    swap_theta.wait_recv()

    seen = jnp.concatenate([oall[0], oall[1]], axis=0)
    mean = jnp.sum(seen, axis=0, keepdims=True) * (1.0 / 128.0)
    scale = 1.0 / obs_sigma[0]
    anomaly = (seen - mean) * scale
    miss = jnp.broadcast_to((obs_values[0] - mean) * scale, (8, 128))
    dims = (((1,), (1,)), ((), ()))
    gram = lax.dot_general(anomaly, anomaly, dims, precision=HIGHEST, preferred_element_type=F32)
    cvec = lax.dot_general(miss, anomaly, dims, precision=HIGHEST, preferred_element_type=F32)
    gp[...] = gram.reshape(16, 8, 128)
    last = iota((8, 128), 0) == 7
    gp[15] = jnp.where(last, cvec, gram[120:128])

    def spread_out(src, dst, ssem, rsem, count, me, axis):
        outs, ins = [], []
        for d in range(1, count):
            j = lax.rem(me + d, count)
            where = {"gx": z, "gy": g, "ens": e, axis: j}
            outs.append(pltpu.make_async_remote_copy(
                src_ref=src(j), dst_ref=dst.at[me], send_sem=ssem.at[d], recv_sem=rsem.at[me],
                device_id=where, device_id_type=MESH))
            ins.append(pltpu.make_async_remote_copy(
                src_ref=src(j), dst_ref=dst.at[j], send_sem=ssem.at[d], recv_sem=rsem.at[j],
                device_id=where, device_id_type=MESH))
        return outs, ins

    rs[g] = gp[g]
    rs_out, rs_in = spread_out(lambda j: gp.at[j], rs, rss, rsr, ng, g, "gy")
    for c in rs_out:
        c.start()
    for c in rs_in:
        c.wait_recv()
    zs[z] = jnp.sum(rs[...], axis=0)
    z_out, z_in = spread_out(lambda j: zs.at[z], zs, zss, zsr, nz, z, "gx")
    for c in z_out:
        c.start()
    for c in z_in:
        c.wait_recv()
    ag[g] = jnp.sum(zs[...], axis=0)
    ag_out, ag_in = spread_out(lambda j: ag.at[g], ag, ags, agr, ng, g, "gy")
    for c in ag_out:
        c.start()

    th_all = thx[...] + thr[...]
    th_mean = jnp.sum(th_all, axis=1, keepdims=True) * (1.0 / 128.0)
    mat[16] = th_all - th_mean
    for c in ag_in:
        c.wait_recv()

    crow = ag[15, 7:8, :]
    sub, ln = iota((8, 128), 0), iota((8, 128), 1)
    tiles = [ag[t] for t in range(16)]
    tiles[15] = jnp.where(last, 0.0, tiles[15])
    total = tiles[0]
    for t in range(1, 16):
        total = total + tiles[t]
    total = jnp.sum(total, axis=0, keepdims=True)
    tiles[15] = jnp.where(last, -total, tiles[15])
    for t in range(16):
        mat[t] = tiles[t] + jnp.where(ln == sub + 8 * t, 127.0, 0.0)

    front = ln < 8

    def block(k, carry):
        piv = mat[k]
        cols = [jnp.broadcast_to(piv[:, j : j + 1], (8, 128)) for j in range(8)]
        a = [[jnp.broadcast_to(cols[j][i : i + 1, :], (8, 128)) for j in range(8)] for i in range(8)]
        rows = [
            jnp.where(front, jnp.where(ln == i, 1.0, 0.0), jnp.broadcast_to(piv[i : i + 1, :], (8, 128)))
            for i in range(8)
        ]
        for i in range(8):
            inv = 1.0 / a[i][i]
            rows[i] = rows[i] * inv
            for j in range(i + 1, 8):
                a[i][j] = a[i][j] * inv
            for r in range(8):
                if r != i:
                    f = a[r][i]
                    rows[r] = rows[r] - f * rows[i]
                    for j in range(i + 1, 8):
                        a[r][j] = a[r][j] - f * a[i][j]
        rows = [jnp.where(front, -r, r) for r in rows]
        for t in range(17):
            x = mat[t]
            new = jnp.where(front, 0.0, x)
            for i in range(8):
                new = new - jnp.broadcast_to(x[:, i : i + 1], (8, 128)) * rows[i]
            mat[t] = pltpu.roll(new, 120, 1)
        return carry

    lax.fori_loop(0, 16, block, 0)
    zt = mat[16]
    shift = jnp.sum(zt * crow, axis=1, keepdims=True)
    fresh = th_mean + 127.0 * zt + shift
    for p in range(4):
        here = jnp.where(diag, jnp.broadcast_to(fresh[p : p + 1, :], (64, 128)), 0.0)
        theta_out[:, p : p + 1] = jnp.sum(here, axis=1, keepdims=True)

    for copy, sends, _ in halo(4, ex, 0, 8):
        when(sends, copy.wait_send)

    def drain(c, carry):
        for copy, sends, _ in halo(c, qx, 16 * c, 2 * c):
            when(sends, copy.wait_send)
        out_copy(c).wait()
        return carry

    lax.fori_loop(0, 4, drain, 0)
    swap_theta.wait_send()
    swap_seen.wait_send()
    for c in rs_out + z_out + ag_out:
        c.wait_send()


def local(state, u_vel, v_vel, land, forcing, member_mode, theta, obs_index, obs_values, obs_sigma):
    hbm = pl.BlockSpec(memory_space=pl.ANY)
    vmem = pl.BlockSpec(memory_space=pltpu.VMEM)
    dma, v = pltpu.SemaphoreType.DMA, lambda *s: pltpu.VMEM(s, F32)
    return pl.pallas_call(
        kernel,
        out_shape=(jax.ShapeDtypeStruct(state.shape, F32), jax.ShapeDtypeStruct(theta.shape, F32)),
        in_specs=[pl.BlockSpec(memory_space=pltpu.SMEM)] + [hbm] * 5 + [vmem] * 4,
        out_specs=(hbm, vmem),
        scratch_shapes=[
            v(64, 32, 128), v(16, 32, 128), pltpu.VMEM((16, 128), jnp.int32),
            v(10, 32, 128), v(10, 32, 128), v(10, 32, 128), v(10, 32, 128),
            v(32, 128), v(3, 32, 128), v(2, 8, 32, 128), v(2, 3, 32, 128), v(4, 64, 128), v(4, 2, 8, 128),
            v(16, 32, 128), v(16, 32, 128), v(16, 32, 128), v(16, 32, 128),
            v(8, 32, 128), v(8, 32, 128), v(8, 32, 128), v(8, 32, 128), v(8, 32, 128), v(8, 16, 128),
            v(64, 16, 128), v(2, 64, 128), v(8, 128), v(8, 128),
            v(16, 8, 128), v(16, 8, 128), v(8, 8, 128), v(16, 8, 128), v(17, 8, 128),
            dma((5,)), dma((4,)), dma((5, 8)), dma((5, 8)), dma((2,)), dma((2,)),
            dma((16,)), dma((16,)), dma((8,)), dma((8,)), dma((16,)), dma((16,)),
        ],
        compiler_params=pltpu.CompilerParams(collective_id=0, has_side_effects=True),
    )(member_mode, state, u_vel, v_vel, land, forcing, theta, obs_index, obs_values, obs_sigma)


def solution(mesh):
    in_specs = (
        P("ens", "gy", "gx"), P("gy", "gx"), P("gy", "gx"), P("gy", "gx"), P(None, "gy", "gx"),
        P("ens"), P("ens", None), P("gy", "gx", None), P("gy", "gx", None), P("gy", "gx", None),
    )
    out_specs = (P("ens", "gy", "gx"), P("ens", None))

    def run(state, u_vel, v_vel, land, forcing, member_mode, theta, obs_index, obs_values, obs_sigma):
        flat = [a.reshape(a.shape[1:]) for a in (obs_index, obs_values, obs_sigma)]
        return local(state, u_vel, v_vel, land, forcing, member_mode, theta, *flat)

    return jax.shard_map(run, mesh=mesh, in_specs=in_specs, out_specs=out_specs, check_vma=False)
```

```python
import jax
import jax.numpy as jnp
from jax import lax
from jax.experimental import pallas as pl
from jax.experimental.pallas import tpu as pltpu
from jax.sharding import PartitionSpec as P

STEPS = 4
W = 2 * STEPS
MESH = pl.DeviceIdType.MESH
F32 = jnp.float32
HIGHEST = lax.Precision.HIGHEST
CHUNK = 16


def iota(shape, dim):
    return lax.broadcasted_iota(jnp.int32, shape, dim)


def pack_edges(ref, first, rows, count, r_ref, l_ref, group):
    lo, hi = rows
    slot = iota((hi - lo, 128), 1) // 16
    for n in range(count):
        right = left = None
        for k in range(8):
            x = ref[first + 8 * n + k, lo:hi, :]
            a = pltpu.roll(x, (16 * (k + 1)) % 128, 1) if k < 7 else x
            b = pltpu.roll(x, 16 * k, 1) if k else x
            right = a if right is None else jnp.where(slot == k, a, right)
            left = b if left is None else jnp.where(slot == k, b, left)
        r_ref[group + n, lo:hi, :] = right
        l_ref[group + n, lo:hi, :] = left


def strips_of(rv, lv, rvr, lvr, lo, hi):
    inner = iota((hi - lo, 128), 1) % 32 < 16
    left = (
        jnp.where(inner, rvr, pltpu.roll(lv, 16, 1)),
        jnp.where(inner, pltpu.roll(rvr, 112, 1), lv),
    )
    right = (
        jnp.where(inner, rv, pltpu.roll(lvr, 16, 1)),
        jnp.where(inner, pltpu.roll(rv, 112, 1), lvr),
    )
    return left, right


def advance(first, planes, coef, tables, forced, qs, lqs, es, mask, put):
    c0, c1, hy = coef
    ocean, uo, vo = tables
    for step in range(STEPS):
        lo = 2 * step
        nl = 4 * W - 2 - 4 * step
        nn = nl - 2
        for p in range(planes):
            get = (lambda a, n, p=p: first(p, a, n)) if step == 0 else (lambda a, n, p=p: qs[p, a : a + n, :])
            cen = get(lo + 1, nl)
            west = pltpu.roll(cen, 1, 1)
            east = pltpu.roll(cen, 127, 1)
            lap = (get(lo + 2, nl) + get(lo, nl)) + (west + east) - 4.0 * cen
            lqs[p, lo + 1 : lo + 1 + nl, :] = lap * mask[lo + 1 : lo + 1 + nl, :]
            es[p, lo + 1 : lo + 1 + nl, :] = east - west
        at = slice(lo + 2, lo + 2 + nn)
        for p in range(planes):
            get = (lambda a, n, p=p: first(p, a, n)) if step == 0 else (lambda a, n, p=p: qs[p, a : a + n, :])
            lap = lqs[p, at, :]
            around = (lqs[p, lo + 3 : lo + 3 + nn, :] + lqs[p, lo + 1 : lo + 1 + nn, :]) + (
                pltpu.roll(lap, 1, 1) + pltpu.roll(lap, 127, 1)
            )
            dy = get(lo + 3, nn) - get(lo + 1, nn)
            inner = c0(p) * get(lo + 2, nn) + c1(p) * lap - hy(p) * around + forced(p, lo + 2, nn)
            new = ocean(p, lo + 2, nn) * inner - (
                uo(p, lo + 2, nn) * es[p, at, :] + vo(p, lo + 2, nn) * dy
            )
            if step < STEPS - 1:
                qs[p, at, :] = new
            else:
                put(p, new)


def kernel(
    mode_in, state, u_vel, v_vel, land, forcing, theta, obs_index, obs_values, obs_sigma,
    fin_out, theta_out,
    qx, ex, landb, rv, lv, rvr, lvr, mask, tabs, ftab, stabs, coefs, pcoefs,
    qs, lqs, es, fos, qp, qps, lqps, eps, fops, endp, fin, oall, thx, thr,
    gp, rs, zs, ag, mat,
    thl, oix, ova, osg, mode, lsem, osem, hs, hr, xs, xr, rss, rsr, zss, zsr, ags, agr,
):
    z, g, e = lax.axis_index("gx"), lax.axis_index("gy"), lax.axis_index("ens")
    nz, ng = 8, 16
    up_ok, down_ok = g > 0, g < ng - 1

    def dev(dz, dg):
        return {"gx": lax.rem(z + dz + nz, nz), "gy": lax.rem(g + dg + ng, ng), "ens": e}

    pair = {"gx": z, "gy": g, "ens": 1 - e}
    barrier = pltpu.get_barrier_semaphore()
    partners = [dev(0, d) for d in range(1, ng)] + [dev(d, 0) for d in range(1, nz)] + [pair]
    partners += [dev(a, b) for a in (-1, 1) for b in (-1, 1)]
    for where in partners:
        pl.semaphore_signal(barrier, inc=1, device_id=where, device_id_type=MESH)

    own = pl.ds(W, 16)
    loads = [
        pltpu.make_async_copy(state, qx.at[:, own, :], lsem.at[0]),
        pltpu.make_async_copy(forcing, ex.at[0:8, own, :], lsem.at[1]),
        pltpu.make_async_copy(u_vel, ex.at[8, own, :], lsem.at[2]),
        pltpu.make_async_copy(v_vel, ex.at[9, own, :], lsem.at[3]),
        pltpu.make_async_copy(land, landb, lsem.at[4]),
        pltpu.make_async_copy(theta, thl, lsem.at[5]),
        pltpu.make_async_copy(obs_index, oix, lsem.at[6]),
        pltpu.make_async_copy(obs_values, ova, lsem.at[7]),
        pltpu.make_async_copy(obs_sigma, osg, lsem.at[8]),
        pltpu.make_async_copy(mode_in, mode, lsem.at[9]),
    ]
    for c in (loads[5], *loads[:5], *loads[6:]):
        c.start()
    loads[5].wait()

    same = iota((64, 64), 0) == iota((64, 64), 1)

    def across(row):
        col = jnp.sum(jnp.where(same, jnp.broadcast_to(row, (64, 64)), 0.0), axis=1, keepdims=True)
        return jnp.broadcast_to(col, (64, 128))

    tt = thl[...]
    th = jnp.tanh(tt)
    hyper = 0.005 * (1.0 + 0.5 * th[1:2])
    coefs[0] = across(1.0 - 0.05 * (1.0 + 0.5 * th[2:3]))
    coefs[1] = across(0.05 * (1.0 + 0.5 * th[0:1]) + 4.0 * hyper)
    coefs[2] = across(hyper)
    coefs[3] = across(tt[3:4])
    thx[...] = jnp.zeros((8, 128), F32)

    @pl.when(e == 0)
    def _():
        thx[0:4, 0:64] = thl[...]

    @pl.when(e == 1)
    def _():
        thx[0:4, 64:128] = thl[...]

    slot8 = iota((8, 128), 1) // 32
    for t in range(4):
        for odd in range(2):
            acc = None
            for k in range(4):
                x = coefs[t, pl.ds(odd + 2 * k, 8, stride=8), :]
                acc = x if acc is None else jnp.where(slot8 == k, x, acc)
            pcoefs[t, odd] = acc
    row32 = iota((32, 128), 0)
    no_wall = (jnp.logical_or(row32 >= W, up_ok)) & (jnp.logical_or(row32 < W + 16, down_ok))
    mask[...] = no_wall.astype(F32)

    for c in loads[1:5] + loads[6:]:
        c.wait()
    ex[10, W : W + 16, :] = (1 - landb[...]).astype(F32)
    ex[11:16, W : W + 16, :] = jnp.zeros((5, 16, 128), F32)

    @pl.when(jnp.logical_not(up_ok))
    def _():
        for ref in (qx, ex, rvr, lvr):
            ref[:, 0:W, :] = jnp.zeros((ref.shape[0], W, 128), F32)

    @pl.when(jnp.logical_not(down_ok))
    def _():
        for ref in (qx, ex, rvr, lvr):
            ref[:, W + 16 :, :] = jnp.zeros((ref.shape[0], W, 128), F32)

    pack_edges(ex, 0, (W, W + 16), 2, rv, lv, 8)
    loads[0].wait()

    def pack_own(c, carry):
        pack_edges(qx, 16 * c, (W, W + 16), 2, rv, lv, 2 * c)
        return carry

    lax.fori_loop(0, 4, pack_own, 0)

    top, bottom, low, high = pl.ds(W, W), pl.ds(16, W), pl.ds(0, W), pl.ds(W + 16, W)

    def halo(c, planes, first, group):
        at, ga = pl.ds(first, 16), pl.ds(group, 2)
        plan = [
            (planes, at, top, planes, high, (0, -1), up_ok, down_ok),
            (planes, at, bottom, planes, low, (0, 1), down_ok, up_ok),
            (rv, ga, own, rvr, own, (1, 0), None, None),
            (lv, ga, own, lvr, own, (-1, 0), None, None),
            (rv, ga, bottom, rvr, low, (1, 1), down_ok, up_ok),
            (rv, ga, top, rvr, high, (1, -1), up_ok, down_ok),
            (lv, ga, bottom, lvr, low, (-1, 1), down_ok, up_ok),
            (lv, ga, top, lvr, high, (-1, -1), up_ok, down_ok),
        ]
        out = []
        for i, (src, a, sr, dst, dr, where, sends, gets) in enumerate(plan):
            copy = pltpu.make_async_remote_copy(
                src_ref=src.at[a, sr, :], dst_ref=dst.at[a, dr, :],
                send_sem=hs.at[c, i], recv_sem=hr.at[c, i],
                device_id=dev(*where), device_id_type=MESH,
            )
            out.append((copy, sends, gets))
        return out

    def when(cond, fn):
        if cond is None:
            fn()
        else:
            pl.when(cond)(fn)

    pl.semaphore_wait(barrier, len(partners))
    for copy, sends, _ in halo(4, ex, 0, 8):
        when(sends, copy.start)

    def send_chunk(c, carry):
        for copy, sends, _ in halo(c, qx, 16 * c, 2 * c):
            when(sends, copy.start)
        return carry

    lax.fori_loop(0, 4, send_chunk, 0)
    swap_theta = pltpu.make_async_remote_copy(
        src_ref=thx, dst_ref=thr, send_sem=xs.at[0], recv_sem=xr.at[0], device_id=pair, device_id_type=MESH
    )
    swap_theta.start()

    for copy, _, gets in halo(4, ex, 0, 8):
        when(gets, copy.wait_recv)
    for rows in ((0, W), (W + 16, 32)):
        pack_edges(ex, 0, rows, 2, rv, lv, 8)
    o = ex[10]
    tabs[0] = o
    tabs[1] = 0.5 * ex[8] * o
    tabs[2] = 0.5 * ex[9] * o
    slot32 = iota((32, 128), 1) // 32

    def spread(x, k):
        y = jnp.where(slot32 == k, x, 0.0)
        y = y + pltpu.roll(y, 32, 1)
        return y + pltpu.roll(y, 64, 1)

    both = strips_of(rv[8], lv[8], rvr[8], lvr[8], 0, 32)
    for side in range(2):
        for k in range(8):
            ftab[side, k] = spread(both[side][k % 2], k // 2)
    both = strips_of(rv[9], lv[9], rvr[9], lvr[9], 0, 32)
    for side in range(2):
        even, odd = both[side]
        o = spread(even, 1)
        stabs[side, 0] = o
        stabs[side, 1] = 0.5 * spread(even, 0) * o
        stabs[side, 2] = 0.5 * spread(odd, 0) * o

    site = oix[...]
    site_col = jnp.broadcast_to(site % 128, (16, 128))
    site_row = jnp.broadcast_to(site // 128, (16, 128)) == iota((16, 128), 0)
    lane = iota((16, 128), 1)
    slot16 = lane % 32 < 16
    edge = (lane < W) | (lane >= 128 - W)

    def out_copy(c):
        at = pl.ds(16 * c, 16)
        return pltpu.make_async_copy(fin.at[at], fin_out.at[at], osem.at[c])

    def chunk(c, carry):
        m0 = 16 * c
        for copy, _, gets in halo(c, qx, m0, 2 * c):
            when(gets, copy.wait_recv)
        for rows in ((0, W), (W + 16, 32)):
            pack_edges(qx, m0, rows, 2, rv, lv, 2 * c)
        for p in range(16):
            fos[p] = coefs[3, pl.ds(m0 + p, 1), :] * ex[mode[m0 + p]]

        def keep(p, new):
            fin[m0 + p] = new

        advance(
            lambda p, a, n: qx[m0 + p, a : a + n, :], 16,
            [lambda p, t=t: coefs[t, pl.ds(m0 + p, 1), :] for t in range(3)],
            [lambda p, a, n, t=t: tabs[t, a : a + n, :] for t in range(3)],
            lambda p, a, n: fos[p, a : a + n, :], qs, lqs, es, mask, keep,
        )
        for n in range(2):
            gr = 2 * c + n
            both = strips_of(rv[gr], lv[gr], rvr[gr], lvr[gr], 0, 32)
            for side in range(2):
                for odd in range(2):
                    p = 4 * n + 2 * side + odd
                    qp[p] = both[side][odd]
                    f = None
                    for k in range(4):
                        x = ftab[side, mode[m0 + 8 * n + 2 * k + odd]]
                        f = x if f is None else jnp.where(slot32 == k, x, f)
                    fops[p] = pcoefs[3, odd, pl.ds(gr, 1), :] * f

        def keep_strip(p, new):
            endp[p] = new

        advance(
            lambda p, a, n: qp[p, a : a + n, :], 8,
            [lambda p, t=t: pcoefs[t, p % 2, pl.ds(2 * c + p // 4, 1), :] for t in range(3)],
            [lambda p, a, n, t=t: stabs[(p // 2) % 2, t, a : a + n, :] for t in range(3)],
            lambda p, a, n: fops[p, a : a + n, :], qps, lqps, eps, mask, keep_strip,
        )
        for n in range(2):
            for odd in range(2):
                ends = jnp.where(slot16, endp[4 * n + 2 + odd], endp[4 * n + odd])
                for k in range(4):
                    p = 8 * n + 2 * k + odd
                    moved = pltpu.roll(ends, (112 - 32 * k) % 128, 1)
                    whole = jnp.where(edge, moved, fin[m0 + p])
                    fin[m0 + p] = whole
                    seen = jnp.where(site_row, jnp.take_along_axis(whole, site_col, axis=1), 0.0)
                    oall[e, pl.ds(m0 + p, 1), :] = jnp.sum(seen, axis=0, keepdims=True)
        out_copy(c).start()
        return carry

    lax.fori_loop(0, 4, chunk, 0)

    swap_seen = pltpu.make_async_remote_copy(
        src_ref=oall.at[e], dst_ref=oall.at[e], send_sem=xs.at[1], recv_sem=xr.at[1],
        device_id=pair, device_id_type=MESH,
    )
    swap_seen.start()
    got_seen = pltpu.make_async_remote_copy(
        src_ref=oall.at[e], dst_ref=oall.at[1 - e], send_sem=xs.at[1], recv_sem=xr.at[1],
        device_id=pair, device_id_type=MESH,
    )
    got_seen.wait_recv()
    swap_theta.wait_recv()

    seen = jnp.concatenate([oall[0], oall[1]], axis=0)
    mean = jnp.sum(seen, axis=0, keepdims=True) * (1.0 / 128.0)
    scale = 1.0 / osg[...]
    anomaly = (seen - mean) * scale
    miss = jnp.broadcast_to((ova[...] - mean) * scale, (8, 128))
    dims = (((1,), (1,)), ((), ()))
    gram = lax.dot_general(anomaly, anomaly, dims, precision=HIGHEST, preferred_element_type=F32)
    cvec = lax.dot_general(miss, anomaly, dims, precision=HIGHEST, preferred_element_type=F32)
    gp[...] = gram.reshape(16, 8, 128)
    last = iota((8, 128), 0) == 7
    gp[15] = jnp.where(last, cvec, gram[120:128])

    def spread_out(src, dst, ssem, rsem, count, me, axis):
        outs, ins = [], []
        for d in range(1, count):
            j = lax.rem(me + d, count)
            where = {"gx": z, "gy": g, "ens": e, axis: j}
            outs.append(pltpu.make_async_remote_copy(
                src_ref=src(j), dst_ref=dst.at[me], send_sem=ssem.at[d], recv_sem=rsem.at[me],
                device_id=where, device_id_type=MESH))
            ins.append(pltpu.make_async_remote_copy(
                src_ref=src(j), dst_ref=dst.at[j], send_sem=ssem.at[d], recv_sem=rsem.at[j],
                device_id=where, device_id_type=MESH))
        return outs, ins

    rs[g] = gp[g]
    rs_out, rs_in = spread_out(lambda j: gp.at[j], rs, rss, rsr, ng, g, "gy")
    for c in rs_out:
        c.start()
    for c in rs_in:
        c.wait_recv()
    zs[z] = jnp.sum(rs[...], axis=0)
    z_out, z_in = spread_out(lambda j: zs.at[z], zs, zss, zsr, nz, z, "gx")
    for c in z_out:
        c.start()
    for c in z_in:
        c.wait_recv()
    ag[g] = jnp.sum(zs[...], axis=0)
    ag_out, ag_in = spread_out(lambda j: ag.at[g], ag, ags, agr, ng, g, "gy")
    for c in ag_out:
        c.start()

    th_all = thx[...] + thr[...]
    th_mean = jnp.sum(th_all, axis=1, keepdims=True) * (1.0 / 128.0)
    mat[16] = th_all - th_mean
    for c in ag_in:
        c.wait_recv()

    crow = ag[15, 7:8, :]
    sub, ln = iota((8, 128), 0), iota((8, 128), 1)
    tiles = [ag[t] for t in range(16)]
    tiles[15] = jnp.where(last, 0.0, tiles[15])
    total = tiles[0]
    for t in range(1, 16):
        total = total + tiles[t]
    total = jnp.sum(total, axis=0, keepdims=True)
    tiles[15] = jnp.where(last, -total, tiles[15])
    for t in range(16):
        mat[t] = tiles[t] + jnp.where(ln == sub + 8 * t, 127.0, 0.0)

    for k in range(16):
        base = 8 * k
        front = (ln >= base) & (ln < base + 8)
        piv = mat[k]
        cols = [jnp.broadcast_to(piv[:, base + j : base + j + 1], (8, 128)) for j in range(8)]
        row = jnp.where(front, jnp.where(ln == sub + base, 1.0, 0.0), piv)
        for i in range(8):
            at = [jnp.broadcast_to(cols[j][i : i + 1, :], (8, 128)) for j in range(i, 8)]
            inv = 1.0 / at[0]
            mine = sub == i
            step = jnp.where(mine, -1.0, cols[i])
            row = jnp.where(mine, 0.0, row) - step * (jnp.broadcast_to(row[i : i + 1, :], (8, 128)) * inv)
            for j in range(i + 1, 8):
                cols[j] = jnp.where(mine, 0.0, cols[j]) - step * (at[j - i] * inv)
        row = jnp.where(front, -row, row)
        rows = [jnp.broadcast_to(row[i : i + 1, :], (8, 128)) for i in range(8)]
        for t in range(k + 1, 17):
            x = mat[t]
            new = jnp.where(front, 0.0, x)
            for i in range(8):
                new = new - jnp.broadcast_to(x[:, base + i : base + i + 1], (8, 128)) * rows[i]
            mat[t] = new
    zt = mat[16]
    shift = jnp.sum(zt * crow, axis=1, keepdims=True)
    fresh = th_mean + 127.0 * zt + shift
    @pl.when(e == 0)
    def _():
        theta_out[...] = fresh[0:4, 0:64]

    @pl.when(e == 1)
    def _():
        theta_out[...] = fresh[0:4, 64:128]

    for copy, sends, _ in halo(4, ex, 0, 8):
        when(sends, copy.wait_send)

    def drain(c, carry):
        for copy, sends, _ in halo(c, qx, 16 * c, 2 * c):
            when(sends, copy.wait_send)
        out_copy(c).wait()
        return carry

    lax.fori_loop(0, 4, drain, 0)
    swap_theta.wait_send()
    swap_seen.wait_send()
    for c in rs_out + z_out + ag_out:
        c.wait_send()


def local(state, u_vel, v_vel, land, forcing, member_mode, theta, obs_index, obs_values, obs_sigma):
    hbm = pl.BlockSpec(memory_space=pl.ANY)
    vmem = pl.BlockSpec(memory_space=pltpu.VMEM)
    dma, v = pltpu.SemaphoreType.DMA, lambda *s: pltpu.VMEM(s, F32)
    return pl.pallas_call(
        kernel,
        out_shape=(jax.ShapeDtypeStruct(state.shape, F32), jax.ShapeDtypeStruct(theta.shape, F32)),
        in_specs=[hbm] * 10,
        out_specs=(hbm, vmem),
        scratch_shapes=[
            v(64, 32, 128), v(16, 32, 128), pltpu.VMEM((16, 128), jnp.int32),
            v(10, 32, 128), v(10, 32, 128), v(10, 32, 128), v(10, 32, 128),
            v(32, 128), v(3, 32, 128), v(2, 8, 32, 128), v(2, 3, 32, 128), v(4, 64, 128), v(4, 2, 8, 128),
            v(16, 32, 128), v(16, 32, 128), v(16, 32, 128), v(16, 32, 128),
            v(8, 32, 128), v(8, 32, 128), v(8, 32, 128), v(8, 32, 128), v(8, 32, 128), v(8, 16, 128),
            v(64, 16, 128), v(2, 64, 128), v(8, 128), v(8, 128),
            v(16, 8, 128), v(16, 8, 128), v(8, 8, 128), v(16, 8, 128), v(17, 8, 128),
            v(4, 64), pltpu.VMEM((1, 128), jnp.int32), v(1, 128), v(1, 128), pltpu.SMEM((64,), jnp.int32),
            dma((10,)), dma((4,)), dma((5, 8)), dma((5, 8)), dma((2,)), dma((2,)),
            dma((16,)), dma((16,)), dma((8,)), dma((8,)), dma((16,)), dma((16,)),
        ],
        compiler_params=pltpu.CompilerParams(collective_id=0, has_side_effects=True),
    )(member_mode, state, u_vel, v_vel, land, forcing, theta, obs_index, obs_values, obs_sigma)


def solution(mesh):
    in_specs = (
        P("ens", "gy", "gx"), P("gy", "gx"), P("gy", "gx"), P("gy", "gx"), P(None, "gy", "gx"),
        P("ens"), P("ens", None), P("gy", "gx", None), P("gy", "gx", None), P("gy", "gx", None),
    )
    out_specs = (P("ens", "gy", "gx"), P("ens", None))

    def run(state, u_vel, v_vel, land, forcing, member_mode, theta, obs_index, obs_values, obs_sigma):
        flat = [a.reshape(a.shape[1:]) for a in (obs_index, obs_values, obs_sigma)]
        fin, new = local(state, u_vel, v_vel, land, forcing, member_mode, theta.T, *flat)
        return fin, new.T

    return jax.shard_map(run, mesh=mesh, in_specs=in_specs, out_specs=out_specs, check_vma=False)
```

```python
import jax
import jax.numpy as jnp
from jax import lax
from jax.experimental import pallas as pl
from jax.experimental.pallas import tpu as pltpu
from jax.sharding import PartitionSpec as P

STEPS = 4
W = 2 * STEPS
MESH = pl.DeviceIdType.MESH
F32 = jnp.float32
HIGHEST = lax.Precision.HIGHEST
AHEAD = 4


def iota(shape, dim):
    return lax.broadcasted_iota(jnp.int32, shape, dim)


def pack_edges(ref, first, rows, count, r_ref, l_ref, group):
    lo, hi = rows
    slot = iota((hi - lo, 128), 1) // 16
    for n in range(count):
        right = left = None
        for k in range(8):
            x = ref[first + 8 * n + k, lo:hi, :]
            a = pltpu.roll(x, (16 * (k + 1)) % 128, 1) if k < 7 else x
            b = pltpu.roll(x, 16 * k, 1) if k else x
            right = a if right is None else jnp.where(slot == k, a, right)
            left = b if left is None else jnp.where(slot == k, b, left)
        r_ref[group + n, lo:hi, :] = right
        l_ref[group + n, lo:hi, :] = left


def strips_of(rv, lv, rvr, lvr, lo, hi):
    inner = iota((hi - lo, 128), 1) % 32 < 16
    left = (
        jnp.where(inner, rvr, pltpu.roll(lv, 16, 1)),
        jnp.where(inner, pltpu.roll(rvr, 112, 1), lv),
    )
    right = (
        jnp.where(inner, rv, pltpu.roll(lvr, 16, 1)),
        jnp.where(inner, pltpu.roll(rv, 112, 1), lvr),
    )
    return left, right


def advance(first, planes, coef, tables, forced, qs, lqs, es, mask, put):
    c0, c1, hy = coef
    ocean, uo, vo = tables
    for step in range(STEPS):
        lo = 2 * step
        nl = 4 * W - 2 - 4 * step
        nn = nl - 2
        for p in range(planes):
            get = (lambda a, n, p=p: first(p, a, n)) if step == 0 else (lambda a, n, p=p: qs[p, a : a + n, :])
            cen = get(lo + 1, nl)
            west = pltpu.roll(cen, 1, 1)
            east = pltpu.roll(cen, 127, 1)
            lap = (get(lo + 2, nl) + get(lo, nl)) + (west + east) - 4.0 * cen
            lqs[p, lo + 1 : lo + 1 + nl, :] = lap * mask[lo + 1 : lo + 1 + nl, :]
            es[p, lo + 1 : lo + 1 + nl, :] = east - west
        at = slice(lo + 2, lo + 2 + nn)
        for p in range(planes):
            get = (lambda a, n, p=p: first(p, a, n)) if step == 0 else (lambda a, n, p=p: qs[p, a : a + n, :])
            lap = lqs[p, at, :]
            around = (lqs[p, lo + 3 : lo + 3 + nn, :] + lqs[p, lo + 1 : lo + 1 + nn, :]) + (
                pltpu.roll(lap, 1, 1) + pltpu.roll(lap, 127, 1)
            )
            dy = get(lo + 3, nn) - get(lo + 1, nn)
            inner = c0(p) * get(lo + 2, nn) + c1(p) * lap - hy(p) * around + forced(p, lo + 2, nn)
            new = ocean(p, lo + 2, nn) * inner - (
                uo(p, lo + 2, nn) * es[p, at, :] + vo(p, lo + 2, nn) * dy
            )
            if step < STEPS - 1:
                qs[p, at, :] = new
            else:
                put(p, new)


def kernel(
    mode_in, state, u_vel, v_vel, land, forcing, theta, obs_index, obs_values, obs_sigma,
    fin_out, theta_out,
    qx, ex, landb, rv, lv, rvr, lvr, mask, tabs, ftab, stabs, coefs, pcoefs,
    qs, lqs, es, fos, qp, qps, lqps, eps, fops, endp, fin, oall, thx, thr,
    gp, rs, zs, ag, mat,
    pick, thl, oix, ova, osg, mode, lsem, osem, hs, hr, xs, xr, rss, rsr, zss, zsr, ags, agr,
):
    z, g, e = lax.axis_index("gx"), lax.axis_index("gy"), lax.axis_index("ens")
    nz, ng = 8, 16
    up_ok, down_ok = g > 0, g < ng - 1

    def dev(dz, dg):
        return {"gx": lax.rem(z + dz + nz, nz), "gy": lax.rem(g + dg + ng, ng), "ens": e}

    pair = {"gx": z, "gy": g, "ens": 1 - e}
    near = lax.rem(g // 8 + e, 2)

    def tile_holder(j):
        return {"gx": z, "gy": j, "ens": lax.rem(j // 8 + near, 2)}

    barrier = pltpu.get_barrier_semaphore()
    partners = [tile_holder(lax.rem(g + d, ng)) for d in range(1, ng)] + [dev(d, 0) for d in range(1, nz)] + [pair]
    partners += [dev(a, b) for a in (-1, 0, 1) for b in (-1, 1)]
    for where in partners:
        pl.semaphore_signal(barrier, inc=1, device_id=where, device_id_type=MESH)

    own = pl.ds(W, 16)
    loads = [
        pltpu.make_async_copy(state, qx.at[:, own, :], lsem.at[0]),
        pltpu.make_async_copy(forcing, ex.at[0:8, own, :], lsem.at[1]),
        pltpu.make_async_copy(u_vel, ex.at[8, own, :], lsem.at[2]),
        pltpu.make_async_copy(v_vel, ex.at[9, own, :], lsem.at[3]),
        pltpu.make_async_copy(land, landb, lsem.at[4]),
        pltpu.make_async_copy(theta, thl, lsem.at[5]),
        pltpu.make_async_copy(obs_index, oix, lsem.at[6]),
        pltpu.make_async_copy(obs_values, ova, lsem.at[7]),
        pltpu.make_async_copy(obs_sigma, osg, lsem.at[8]),
        pltpu.make_async_copy(mode_in, mode, lsem.at[9]),
    ]
    for c in loads:
        c.start()

    @pl.when(jnp.logical_not(up_ok))
    def _():
        for ref in (qx, ex, rvr, lvr):
            ref[:, 0:W, :] = jnp.zeros((ref.shape[0], W, 128), F32)

    @pl.when(jnp.logical_not(down_ok))
    def _():
        for ref in (qx, ex, rvr, lvr):
            ref[:, W + 16 :, :] = jnp.zeros((ref.shape[0], W, 128), F32)

    top, bottom, low, high = pl.ds(W, W), pl.ds(16, W), pl.ds(0, W), pl.ds(W + 16, W)

    def halo(c, planes, first, group):
        at, ga = pl.ds(first, 16), pl.ds(group, 2)
        plan = [
            (planes, at, top, planes, high, (0, -1), up_ok, down_ok),
            (planes, at, bottom, planes, low, (0, 1), down_ok, up_ok),
            (rv, ga, own, rvr, own, (1, 0), None, None),
            (lv, ga, own, lvr, own, (-1, 0), None, None),
            (rv, ga, bottom, rvr, low, (1, 1), down_ok, up_ok),
            (rv, ga, top, rvr, high, (1, -1), up_ok, down_ok),
            (lv, ga, bottom, lvr, low, (-1, 1), down_ok, up_ok),
            (lv, ga, top, lvr, high, (-1, -1), up_ok, down_ok),
        ]
        out = []
        for i, (src, a, sr, dst, dr, where, sends, gets) in enumerate(plan):
            copy = pltpu.make_async_remote_copy(
                src_ref=src.at[a, sr, :], dst_ref=dst.at[a, dr, :],
                send_sem=hs.at[c, i], recv_sem=hr.at[c, i],
                device_id=dev(*where), device_id_type=MESH,
            )
            out.append((copy, sends, gets))
        return out

    def when(cond, fn):
        if cond is None:
            fn()
        else:
            pl.when(cond)(fn)

    def send(copies):
        for copy, sends, _ in copies:
            when(sends, copy.start)

    for c in loads[1:5]:
        c.wait()
    ex[10, W : W + 16, :] = (1 - landb[...]).astype(F32)
    ex[11:16, W : W + 16, :] = jnp.zeros((5, 16, 128), F32)
    loads[0].wait()
    pack_edges(ex, 0, (W, W + 16), 2, rv, lv, 8)

    def pack_own(c, carry):
        pack_edges(qx, 16 * c, (W, W + 16), 2, rv, lv, 2 * c)
        return carry

    lax.fori_loop(0, 4, pack_own, 0)
    pl.semaphore_wait(barrier, len(partners))
    send(halo(4, ex, 0, 8))

    def send_chunk(c, carry):
        send(halo(c, qx, 16 * c, 2 * c))
        return carry

    lax.fori_loop(0, AHEAD, send_chunk, 0)

    for c in loads[5:]:
        c.wait()
    same = iota((64, 64), 0) == iota((64, 64), 1)

    def across(row):
        col = jnp.sum(jnp.where(same, jnp.broadcast_to(row, (64, 64)), 0.0), axis=1, keepdims=True)
        return jnp.broadcast_to(col, (64, 128))

    tt = thl[...]
    th = jnp.tanh(tt)
    hyper = 0.005 * (1.0 + 0.5 * th[1:2])
    coefs[0] = across(1.0 - 0.05 * (1.0 + 0.5 * th[2:3]))
    coefs[1] = across(0.05 * (1.0 + 0.5 * th[0:1]) + 4.0 * hyper)
    coefs[2] = across(hyper)
    coefs[3] = across(tt[3:4])
    thx[...] = jnp.zeros((8, 128), F32)

    @pl.when(e == 0)
    def _():
        thx[0:4, 0:64] = thl[...]

    @pl.when(e == 1)
    def _():
        thx[0:4, 64:128] = thl[...]

    slot8 = iota((8, 128), 1) // 32
    for t in range(4):
        for odd in range(2):
            acc = None
            for k in range(4):
                x = coefs[t, pl.ds(odd + 2 * k, 8, stride=8), :]
                acc = x if acc is None else jnp.where(slot8 == k, x, acc)
            pcoefs[t, odd] = acc
    row32 = iota((32, 128), 0)
    no_wall = (jnp.logical_or(row32 >= W, up_ok)) & (jnp.logical_or(row32 < W + 16, down_ok))
    mask[...] = no_wall.astype(F32)


    swap_theta = pltpu.make_async_remote_copy(
        src_ref=thx, dst_ref=thr, send_sem=xs.at[0], recv_sem=xr.at[0], device_id=pair, device_id_type=MESH
    )
    swap_theta.start()

    for copy, _, gets in halo(4, ex, 0, 8):
        when(gets, copy.wait_recv)
    for rows in ((0, W), (W + 16, 32)):
        pack_edges(ex, 0, rows, 2, rv, lv, 8)
    o = ex[10]
    tabs[0] = o
    tabs[1] = 0.5 * ex[8] * o
    tabs[2] = 0.5 * ex[9] * o
    slot32 = iota((32, 128), 1) // 32

    def spread(x, k):
        y = jnp.where(slot32 == k, x, 0.0)
        y = y + pltpu.roll(y, 32, 1)
        return y + pltpu.roll(y, 64, 1)

    both = strips_of(rv[8], lv[8], rvr[8], lvr[8], 0, 32)
    for side in range(2):
        for k in range(8):
            ftab[side, k] = spread(both[side][k % 2], k // 2)
    both = strips_of(rv[9], lv[9], rvr[9], lvr[9], 0, 32)
    for side in range(2):
        even, odd = both[side]
        o = spread(even, 1)
        stabs[side, 0] = o
        stabs[side, 1] = 0.5 * spread(even, 0) * o
        stabs[side, 2] = 0.5 * spread(odd, 0) * o

    site = oix[...]
    col_pick = jnp.broadcast_to(site % 128, (128, 128)) == iota((128, 128), 0)
    for n in range(3):
        pick[128 * n : 128 * n + 128, :] = col_pick.astype(F32).astype(jnp.bfloat16)
    site_row = jnp.broadcast_to(site // 128, (16, 128)) == iota((16, 128), 0)
    lane = iota((16, 128), 1)
    slot16 = lane % 32 < 16
    edge = (lane < W) | (lane >= 128 - W)

    out_copy = pltpu.make_async_copy(fin, fin_out, osem.at[0])

    def chunk(c, carry):
        m0 = 16 * c
        for copy, _, gets in halo(c, qx, m0, 2 * c):
            when(gets, copy.wait_recv)

        @pl.when(c + AHEAD < 4)
        def _():
            send_chunk(c + AHEAD, 0)

        for rows in ((0, W), (W + 16, 32)):
            pack_edges(qx, m0, rows, 2, rv, lv, 2 * c)
        for p in range(16):
            fos[p] = coefs[3, pl.ds(m0 + p, 1), :] * ex[mode[m0 + p]]

        def keep(p, new):
            fin[m0 + p] = new

        advance(
            lambda p, a, n: qx[m0 + p, a : a + n, :], 16,
            [lambda p, t=t: coefs[t, pl.ds(m0 + p, 1), :] for t in range(3)],
            [lambda p, a, n, t=t: tabs[t, a : a + n, :] for t in range(3)],
            lambda p, a, n: fos[p, a : a + n, :], qs, lqs, es, mask, keep,
        )
        for n in range(2):
            gr = 2 * c + n
            both = strips_of(rv[gr], lv[gr], rvr[gr], lvr[gr], 0, 32)
            for side in range(2):
                for odd in range(2):
                    p = 4 * n + 2 * side + odd
                    qp[p] = both[side][odd]
                    f = None
                    for k in range(4):
                        x = ftab[side, mode[m0 + 8 * n + 2 * k + odd]]
                        f = x if f is None else jnp.where(slot32 == k, x, f)
                    fops[p] = pcoefs[3, odd, pl.ds(gr, 1), :] * f

        def keep_strip(p, new):
            endp[8 * c + p] = new

        advance(
            lambda p, a, n: qp[p, a : a + n, :], 8,
            [lambda p, t=t: pcoefs[t, p % 2, pl.ds(2 * c + p // 4, 1), :] for t in range(3)],
            [lambda p, a, n, t=t: stabs[(p // 2) % 2, t, a : a + n, :] for t in range(3)],
            lambda p, a, n: fops[p, a : a + n, :], qps, lqps, eps, mask, keep_strip,
        )
        return carry

    lax.fori_loop(0, 4, chunk, 0)

    for c in range(4):
        for q in range(4):
            n, odd = q // 2, q % 2
            ends = jnp.where(slot16, endp[8 * c + 4 * n + 2 + odd], endp[8 * c + 4 * n + odd])
            for k in range(4):
                p = 16 * c + 8 * n + 2 * k + odd
                fin[p] = jnp.where(edge, pltpu.roll(ends, (112 - 32 * k) % 128, 1), fin[p])
    out_copy.start()
    for c in range(4):
        x = fin[16 * c : 16 * c + 16].reshape(256, 128)
        part, parts = x, []
        for _ in range(3):
            parts.append(part.astype(jnp.bfloat16))
            part = part - parts[-1].astype(F32)
        at_col = jnp.dot(jnp.concatenate(parts, axis=1), pick[...], preferred_element_type=F32)
        seen = jnp.where(site_row[None], at_col.reshape(16, 16, 128), 0.0)
        oall[e, 16 * c : 16 * c + 16, :] = jnp.sum(seen, axis=1)

    swap_seen = pltpu.make_async_remote_copy(
        src_ref=oall.at[e], dst_ref=oall.at[e], send_sem=xs.at[1], recv_sem=xr.at[1],
        device_id=pair, device_id_type=MESH,
    )
    swap_seen.start()
    got_seen = pltpu.make_async_remote_copy(
        src_ref=oall.at[e], dst_ref=oall.at[1 - e], send_sem=xs.at[1], recv_sem=xr.at[1],
        device_id=pair, device_id_type=MESH,
    )
    got_seen.wait_recv()
    swap_theta.wait_recv()

    seen = jnp.concatenate([oall[0], oall[1]], axis=0)
    mean = jnp.sum(seen, axis=0, keepdims=True) * (1.0 / 128.0)
    scale = 1.0 / osg[...]
    anomaly = (seen - mean) * scale
    miss = jnp.broadcast_to((ova[...] - mean) * scale, (8, 128))
    dims = (((1,), (1,)), ((), ()))
    gram = lax.dot_general(anomaly, anomaly, dims, precision=HIGHEST, preferred_element_type=F32)
    cvec = lax.dot_general(miss, anomaly, dims, precision=HIGHEST, preferred_element_type=F32)
    gp[...] = gram.reshape(16, 8, 128)
    last = iota((8, 128), 0) == 7
    gp[15] = jnp.where(last, cvec, gram[120:128])

    def spread_out(src, dst, ssem, rsem, count, me, place):
        outs, ins = [], []
        for d in range(1, count):
            j = lax.rem(me + d, count)
            where = place(j)
            outs.append(pltpu.make_async_remote_copy(
                src_ref=src(j), dst_ref=dst.at[me], send_sem=ssem.at[d], recv_sem=rsem.at[me],
                device_id=where, device_id_type=MESH))
            ins.append(pltpu.make_async_remote_copy(
                src_ref=src(j), dst_ref=dst.at[j], send_sem=ssem.at[d], recv_sem=rsem.at[j],
                device_id=where, device_id_type=MESH))
        return outs, ins

    rs[g] = gp[g]
    rs_out, rs_in = spread_out(lambda j: gp.at[j], rs, rss, rsr, ng, g, tile_holder)
    for c in rs_out:
        c.start()
    for c in rs_in:
        c.wait_recv()
    zs[z] = jnp.sum(rs[...], axis=0)
    z_out, z_in = spread_out(lambda j: zs.at[z], zs, zss, zsr, nz, z, lambda j: {"gx": j, "gy": g, "ens": e})
    for c in z_out:
        c.start()
    for c in z_in:
        c.wait_recv()
    ag[g] = jnp.sum(zs[...], axis=0)
    ag_out, ag_in = spread_out(lambda j: ag.at[g], ag, ags, agr, ng, g, tile_holder)
    for c in ag_out:
        c.start()

    th_all = thx[...] + thr[...]
    th_mean = jnp.sum(th_all, axis=1, keepdims=True) * (1.0 / 128.0)
    mat[16] = th_all - th_mean
    for c in ag_in:
        c.wait_recv()

    crow = ag[15, 7:8, :]
    sub, ln = iota((8, 128), 0), iota((8, 128), 1)
    tiles = [ag[t] for t in range(16)]
    tiles[15] = jnp.where(last, 0.0, tiles[15])
    total = tiles[0]
    for t in range(1, 16):
        total = total + tiles[t]
    total = jnp.sum(total, axis=0, keepdims=True)
    tiles[15] = jnp.where(last, -total, tiles[15])
    for t in range(16):
        mat[t] = tiles[t] + jnp.where(ln == sub + 8 * t, 127.0, 0.0)

    def lanes_of(x, base):
        return [jnp.broadcast_to(x[:, base + j : base + j + 1], (8, 128)) for j in range(8)]

    def row_of(x, i):
        return jnp.broadcast_to(x[i : i + 1, :], (8, 128))

    cols = lanes_of(tiles[0] + jnp.where(ln == sub, 127.0, 0.0), 0)
    for k in range(16):
        base = 8 * k
        front = (ln >= base) & (ln < base + 8)
        piv = mat[k]
        ahead = lanes_of(piv, base + 8) if k < 15 else []
        row = jnp.where(front, jnp.where(ln == sub + base, 1.0, 0.0), piv)
        for i in range(8):
            at = [row_of(cols[j], i) for j in range(i, 8)]
            inv = 1.0 / at[0]
            mine = sub == i
            step = jnp.where(mine, -1.0, cols[i])
            row = jnp.where(mine, 0.0, row) - step * (row_of(row, i) * inv)
            for j in range(i + 1, 8):
                cols[j] = jnp.where(mine, 0.0, cols[j]) - step * (at[j - i] * inv)
            ahead = [jnp.where(mine, 0.0, x) - step * (row_of(x, i) * inv) for x in ahead]
        row = jnp.where(front, -row, row)
        rows = [row_of(row, i) for i in range(8)]
        for t in range(k + 1, 17):
            x = mat[t]
            by = lanes_of(x, base)
            new = jnp.where(front, 0.0, x)
            for i in range(8):
                new = new - by[i] * rows[i]
            mat[t] = new
            if t == k + 1 and k < 15:
                cols = lanes_of(x, base + 8)
                for j in range(8):
                    for i in range(8):
                        cols[j] = cols[j] - by[i] * row_of(ahead[j], i)
    zt = mat[16]
    shift = jnp.sum(zt * crow, axis=1, keepdims=True)
    fresh = th_mean + 127.0 * zt + shift
    @pl.when(e == 0)
    def _():
        theta_out[...] = fresh[0:4, 0:64]

    @pl.when(e == 1)
    def _():
        theta_out[...] = fresh[0:4, 64:128]

    for copy, sends, _ in halo(4, ex, 0, 8):
        when(sends, copy.wait_send)

    def drain(c, carry):
        for copy, sends, _ in halo(c, qx, 16 * c, 2 * c):
            when(sends, copy.wait_send)
        return carry

    lax.fori_loop(0, 4, drain, 0)
    out_copy.wait()
    swap_theta.wait_send()
    swap_seen.wait_send()
    for c in rs_out + z_out + ag_out:
        c.wait_send()


def local(state, u_vel, v_vel, land, forcing, member_mode, theta, obs_index, obs_values, obs_sigma):
    hbm = pl.BlockSpec(memory_space=pl.ANY)
    vmem = pl.BlockSpec(memory_space=pltpu.VMEM)
    dma, v = pltpu.SemaphoreType.DMA, lambda *s: pltpu.VMEM(s, F32)
    return pl.pallas_call(
        kernel,
        out_shape=(jax.ShapeDtypeStruct(state.shape, F32), jax.ShapeDtypeStruct(theta.shape, F32)),
        in_specs=[hbm] * 10,
        out_specs=(hbm, vmem),
        scratch_shapes=[
            v(64, 32, 128), v(16, 32, 128), pltpu.VMEM((16, 128), jnp.int32),
            v(10, 32, 128), v(10, 32, 128), v(10, 32, 128), v(10, 32, 128),
            v(32, 128), v(3, 32, 128), v(2, 8, 32, 128), v(2, 3, 32, 128), v(4, 64, 128), v(4, 2, 8, 128),
            v(16, 32, 128), v(16, 32, 128), v(16, 32, 128), v(16, 32, 128),
            v(8, 32, 128), v(8, 32, 128), v(8, 32, 128), v(8, 32, 128), v(8, 32, 128), v(32, 16, 128),
            v(64, 16, 128), v(2, 64, 128), v(8, 128), v(8, 128),
            v(16, 8, 128), v(16, 8, 128), v(8, 8, 128), v(16, 8, 128), v(17, 8, 128),
            pltpu.VMEM((384, 128), jnp.bfloat16), v(4, 64), pltpu.VMEM((1, 128), jnp.int32), v(1, 128), v(1, 128), pltpu.SMEM((64,), jnp.int32),
            dma((10,)), dma((1,)), dma((5, 8)), dma((5, 8)), dma((2,)), dma((2,)),
            dma((16,)), dma((16,)), dma((8,)), dma((8,)), dma((16,)), dma((16,)),
        ],
        compiler_params=pltpu.CompilerParams(collective_id=0, has_side_effects=True),
    )(member_mode, state, u_vel, v_vel, land, forcing, theta, obs_index, obs_values, obs_sigma)


def solution(mesh):
    in_specs = (
        P("ens", "gy", "gx"), P("gy", "gx"), P("gy", "gx"), P("gy", "gx"), P(None, "gy", "gx"),
        P("ens"), P("ens", None), P("gy", "gx", None), P("gy", "gx", None), P("gy", "gx", None),
    )
    out_specs = (P("ens", "gy", "gx"), P("ens", None))

    def run(state, u_vel, v_vel, land, forcing, member_mode, theta, obs_index, obs_values, obs_sigma):
        flat = [a.reshape(a.shape[1:]) for a in (obs_index, obs_values, obs_sigma)]
        fin, new = local(state, u_vel, v_vel, land, forcing, member_mode, theta.T, *flat)
        return fin, new.T

    return jax.shard_map(run, mesh=mesh, in_specs=in_specs, out_specs=out_specs, check_vma=False)
```

```python
import jax
import jax.numpy as jnp
from jax import lax
from jax.experimental import pallas as pl
from jax.experimental.pallas import tpu as pltpu
from jax.sharding import PartitionSpec as P

STEPS = 4
W = 2 * STEPS
MESH = pl.DeviceIdType.MESH
F32 = jnp.float32
HIGHEST = lax.Precision.HIGHEST
AHEAD = 4


def iota(shape, dim):
    return lax.broadcasted_iota(jnp.int32, shape, dim)


def pack_edges(ref, first, rows, count, r_ref, l_ref, group):
    lo, hi = rows
    slot = iota((hi - lo, 128), 1) // 16
    for n in range(count):
        right = left = None
        for k in range(8):
            x = ref[first + 8 * n + k, lo:hi, :]
            a = pltpu.roll(x, (16 * (k + 1)) % 128, 1) if k < 7 else x
            b = pltpu.roll(x, 16 * k, 1) if k else x
            right = a if right is None else jnp.where(slot == k, a, right)
            left = b if left is None else jnp.where(slot == k, b, left)
        r_ref[group + n, lo:hi, :] = right
        l_ref[group + n, lo:hi, :] = left


def strips_of(rv, lv, rvr, lvr, lo, hi):
    inner = iota((hi - lo, 128), 1) % 32 < 16
    left = (
        jnp.where(inner, rvr, pltpu.roll(lv, 16, 1)),
        jnp.where(inner, pltpu.roll(rvr, 112, 1), lv),
    )
    right = (
        jnp.where(inner, rv, pltpu.roll(lvr, 16, 1)),
        jnp.where(inner, pltpu.roll(rv, 112, 1), lvr),
    )
    return left, right


def advance(first, planes, coef, tables, forced, qs, lqs, es, mask, put):
    c0, c1, hy = coef
    ocean, uo, vo = tables
    for step in range(STEPS):
        lo = 2 * step
        nl = 4 * W - 2 - 4 * step
        nn = nl - 2
        for p in range(planes):
            get = (lambda a, n, p=p: first(p, a, n)) if step == 0 else (lambda a, n, p=p: qs[p, a : a + n, :])
            cen = get(lo + 1, nl)
            west = pltpu.roll(cen, 1, 1)
            east = pltpu.roll(cen, 127, 1)
            lap = (get(lo + 2, nl) + get(lo, nl)) + (west + east) - 4.0 * cen
            lqs[p, lo + 1 : lo + 1 + nl, :] = lap * mask[lo + 1 : lo + 1 + nl, :]
            es[p, lo + 1 : lo + 1 + nl, :] = east - west
        at = slice(lo + 2, lo + 2 + nn)
        for p in range(planes):
            get = (lambda a, n, p=p: first(p, a, n)) if step == 0 else (lambda a, n, p=p: qs[p, a : a + n, :])
            lap = lqs[p, at, :]
            around = (lqs[p, lo + 3 : lo + 3 + nn, :] + lqs[p, lo + 1 : lo + 1 + nn, :]) + (
                pltpu.roll(lap, 1, 1) + pltpu.roll(lap, 127, 1)
            )
            dy = get(lo + 3, nn) - get(lo + 1, nn)
            inner = c0(p) * get(lo + 2, nn) + c1(p) * lap - hy(p) * around + forced(p, lo + 2, nn)
            new = ocean(p, lo + 2, nn) * inner - (
                uo(p, lo + 2, nn) * es[p, at, :] + vo(p, lo + 2, nn) * dy
            )
            if step < STEPS - 1:
                qs[p, at, :] = new
            else:
                put(p, new)


def kernel(
    mode_in, state, u_vel, v_vel, land, forcing, theta, obs_index, obs_values, obs_sigma,
    fin, sums, thetas,
    qx, ex, landb, rv, lv, rvr, lvr, mask, tabs, ftab, stabs, coefs, pcoefs,
    qs, lqs, es, fos, qp, qps, lqps, eps, fops, endp, oall, thx, thr,
    gp, rs, zs, ag,
    pick, thl, oix, ova, osg, mode, lsem, hs, hr, xs, xr, rss, rsr, zss, zsr, ags, agr,
):
    z, g, e = lax.axis_index("gx"), lax.axis_index("gy"), lax.axis_index("ens")
    nz, ng = 8, 16
    up_ok, down_ok = g > 0, g < ng - 1

    def dev(dz, dg):
        return {"gx": lax.rem(z + dz + nz, nz), "gy": lax.rem(g + dg + ng, ng), "ens": e}

    pair = {"gx": z, "gy": g, "ens": 1 - e}
    near = lax.rem(g // 8 + e, 2)

    def tile_holder(j):
        return {"gx": z, "gy": j, "ens": lax.rem(j // 8 + near, 2)}

    barrier = pltpu.get_barrier_semaphore()
    partners = [tile_holder(lax.rem(g + d, ng)) for d in range(1, ng)] + [dev(d, 0) for d in range(1, nz)] + [pair]
    partners += [dev(a, b) for a in (-1, 0, 1) for b in (-1, 1)]
    for where in partners:
        pl.semaphore_signal(barrier, inc=1, device_id=where, device_id_type=MESH)

    own = pl.ds(W, 16)
    loads = [
        pltpu.make_async_copy(state, qx.at[:, own, :], lsem.at[0]),
        pltpu.make_async_copy(forcing, ex.at[0:8, own, :], lsem.at[1]),
        pltpu.make_async_copy(u_vel, ex.at[8, own, :], lsem.at[2]),
        pltpu.make_async_copy(v_vel, ex.at[9, own, :], lsem.at[3]),
        pltpu.make_async_copy(land, landb, lsem.at[4]),
        pltpu.make_async_copy(theta, thl, lsem.at[5]),
        pltpu.make_async_copy(obs_index, oix, lsem.at[6]),
        pltpu.make_async_copy(obs_values, ova, lsem.at[7]),
        pltpu.make_async_copy(obs_sigma, osg, lsem.at[8]),
        pltpu.make_async_copy(mode_in, mode, lsem.at[9]),
    ]
    for c in loads:
        c.start()

    @pl.when(jnp.logical_not(up_ok))
    def _():
        for ref in (qx, ex, rvr, lvr):
            ref[:, 0:W, :] = jnp.zeros((ref.shape[0], W, 128), F32)

    @pl.when(jnp.logical_not(down_ok))
    def _():
        for ref in (qx, ex, rvr, lvr):
            ref[:, W + 16 :, :] = jnp.zeros((ref.shape[0], W, 128), F32)

    top, bottom, low, high = pl.ds(W, W), pl.ds(16, W), pl.ds(0, W), pl.ds(W + 16, W)

    def halo(c, planes, first, group):
        at, ga = pl.ds(first, 16), pl.ds(group, 2)
        plan = [
            (planes, at, top, planes, high, (0, -1), up_ok, down_ok),
            (planes, at, bottom, planes, low, (0, 1), down_ok, up_ok),
            (rv, ga, own, rvr, own, (1, 0), None, None),
            (lv, ga, own, lvr, own, (-1, 0), None, None),
            (rv, ga, bottom, rvr, low, (1, 1), down_ok, up_ok),
            (rv, ga, top, rvr, high, (1, -1), up_ok, down_ok),
            (lv, ga, bottom, lvr, low, (-1, 1), down_ok, up_ok),
            (lv, ga, top, lvr, high, (-1, -1), up_ok, down_ok),
        ]
        out = []
        for i, (src, a, sr, dst, dr, where, sends, gets) in enumerate(plan):
            copy = pltpu.make_async_remote_copy(
                src_ref=src.at[a, sr, :], dst_ref=dst.at[a, dr, :],
                send_sem=hs.at[c, i], recv_sem=hr.at[c, i],
                device_id=dev(*where), device_id_type=MESH,
            )
            out.append((copy, sends, gets))
        return out

    def when(cond, fn):
        if cond is None:
            fn()
        else:
            pl.when(cond)(fn)

    def send(copies):
        for copy, sends, _ in copies:
            when(sends, copy.start)

    for c in loads[1:5]:
        c.wait()
    ex[10, W : W + 16, :] = (1 - landb[...]).astype(F32)
    ex[11:16, W : W + 16, :] = jnp.zeros((5, 16, 128), F32)
    loads[0].wait()
    pack_edges(ex, 0, (W, W + 16), 2, rv, lv, 8)

    def pack_own(c, carry):
        pack_edges(qx, 16 * c, (W, W + 16), 2, rv, lv, 2 * c)
        return carry

    lax.fori_loop(0, 4, pack_own, 0)
    pl.semaphore_wait(barrier, len(partners))
    send(halo(4, ex, 0, 8))

    def send_chunk(c, carry):
        send(halo(c, qx, 16 * c, 2 * c))
        return carry

    lax.fori_loop(0, AHEAD, send_chunk, 0)

    for c in loads[5:]:
        c.wait()
    same = iota((64, 64), 0) == iota((64, 64), 1)

    def across(row):
        col = jnp.sum(jnp.where(same, jnp.broadcast_to(row, (64, 64)), 0.0), axis=1, keepdims=True)
        return jnp.broadcast_to(col, (64, 128))

    tt = thl[...]
    th = jnp.tanh(tt)
    hyper = 0.005 * (1.0 + 0.5 * th[1:2])
    coefs[0] = across(1.0 - 0.05 * (1.0 + 0.5 * th[2:3]))
    coefs[1] = across(0.05 * (1.0 + 0.5 * th[0:1]) + 4.0 * hyper)
    coefs[2] = across(hyper)
    coefs[3] = across(tt[3:4])
    thx[...] = jnp.zeros((8, 128), F32)

    @pl.when(e == 0)
    def _():
        thx[0:4, 0:64] = thl[...]

    @pl.when(e == 1)
    def _():
        thx[0:4, 64:128] = thl[...]

    slot8 = iota((8, 128), 1) // 32
    for t in range(4):
        for odd in range(2):
            acc = None
            for k in range(4):
                x = coefs[t, pl.ds(odd + 2 * k, 8, stride=8), :]
                acc = x if acc is None else jnp.where(slot8 == k, x, acc)
            pcoefs[t, odd] = acc
    row32 = iota((32, 128), 0)
    no_wall = (jnp.logical_or(row32 >= W, up_ok)) & (jnp.logical_or(row32 < W + 16, down_ok))
    mask[...] = no_wall.astype(F32)


    swap_theta = pltpu.make_async_remote_copy(
        src_ref=thx, dst_ref=thr, send_sem=xs.at[0], recv_sem=xr.at[0], device_id=pair, device_id_type=MESH
    )
    swap_theta.start()

    for copy, _, gets in halo(4, ex, 0, 8):
        when(gets, copy.wait_recv)
    for rows in ((0, W), (W + 16, 32)):
        pack_edges(ex, 0, rows, 2, rv, lv, 8)
    o = ex[10]
    tabs[0] = o
    tabs[1] = 0.5 * ex[8] * o
    tabs[2] = 0.5 * ex[9] * o
    slot32 = iota((32, 128), 1) // 32

    def spread(x, k):
        y = jnp.where(slot32 == k, x, 0.0)
        y = y + pltpu.roll(y, 32, 1)
        return y + pltpu.roll(y, 64, 1)

    both = strips_of(rv[8], lv[8], rvr[8], lvr[8], 0, 32)
    for side in range(2):
        for k in range(8):
            ftab[side, k] = spread(both[side][k % 2], k // 2)
    both = strips_of(rv[9], lv[9], rvr[9], lvr[9], 0, 32)
    for side in range(2):
        even, odd = both[side]
        o = spread(even, 1)
        stabs[side, 0] = o
        stabs[side, 1] = 0.5 * spread(even, 0) * o
        stabs[side, 2] = 0.5 * spread(odd, 0) * o

    site = oix[...]
    col_pick = jnp.broadcast_to(site % 128, (128, 128)) == iota((128, 128), 0)
    for n in range(3):
        pick[128 * n : 128 * n + 128, :] = col_pick.astype(F32).astype(jnp.bfloat16)
    site_row = jnp.broadcast_to(site // 128, (16, 128)) == iota((16, 128), 0)
    lane = iota((16, 128), 1)
    slot16 = lane % 32 < 16
    edge = (lane < W) | (lane >= 128 - W)

    def chunk(c, carry):
        m0 = 16 * c
        for copy, _, gets in halo(c, qx, m0, 2 * c):
            when(gets, copy.wait_recv)

        @pl.when(c + AHEAD < 4)
        def _():
            send_chunk(c + AHEAD, 0)

        for rows in ((0, W), (W + 16, 32)):
            pack_edges(qx, m0, rows, 2, rv, lv, 2 * c)
        for p in range(16):
            fos[p] = coefs[3, pl.ds(m0 + p, 1), :] * ex[mode[m0 + p]]

        def keep(p, new):
            fin[m0 + p] = new

        advance(
            lambda p, a, n: qx[m0 + p, a : a + n, :], 16,
            [lambda p, t=t: coefs[t, pl.ds(m0 + p, 1), :] for t in range(3)],
            [lambda p, a, n, t=t: tabs[t, a : a + n, :] for t in range(3)],
            lambda p, a, n: fos[p, a : a + n, :], qs, lqs, es, mask, keep,
        )
        for n in range(2):
            gr = 2 * c + n
            both = strips_of(rv[gr], lv[gr], rvr[gr], lvr[gr], 0, 32)
            for side in range(2):
                for odd in range(2):
                    p = 4 * n + 2 * side + odd
                    qp[p] = both[side][odd]
                    f = None
                    for k in range(4):
                        x = ftab[side, mode[m0 + 8 * n + 2 * k + odd]]
                        f = x if f is None else jnp.where(slot32 == k, x, f)
                    fops[p] = pcoefs[3, odd, pl.ds(gr, 1), :] * f

        def keep_strip(p, new):
            endp[8 * c + p] = new

        advance(
            lambda p, a, n: qp[p, a : a + n, :], 8,
            [lambda p, t=t: pcoefs[t, p % 2, pl.ds(2 * c + p // 4, 1), :] for t in range(3)],
            [lambda p, a, n, t=t: stabs[(p // 2) % 2, t, a : a + n, :] for t in range(3)],
            lambda p, a, n: fops[p, a : a + n, :], qps, lqps, eps, mask, keep_strip,
        )
        return carry

    lax.fori_loop(0, 4, chunk, 0)

    for c in range(4):
        for q in range(4):
            n, odd = q // 2, q % 2
            ends = jnp.where(slot16, endp[8 * c + 4 * n + 2 + odd], endp[8 * c + 4 * n + odd])
            for k in range(4):
                p = 16 * c + 8 * n + 2 * k + odd
                fin[p] = jnp.where(edge, pltpu.roll(ends, (112 - 32 * k) % 128, 1), fin[p])
    for c in range(4):
        x = fin[16 * c : 16 * c + 16].reshape(256, 128)
        part, parts = x, []
        for _ in range(3):
            parts.append(part.astype(jnp.bfloat16))
            part = part - parts[-1].astype(F32)
        at_col = jnp.dot(jnp.concatenate(parts, axis=1), pick[...], preferred_element_type=F32)
        seen = jnp.where(site_row[None], at_col.reshape(16, 16, 128), 0.0)
        oall[e, 16 * c : 16 * c + 16, :] = jnp.sum(seen, axis=1)

    swap_seen = pltpu.make_async_remote_copy(
        src_ref=oall.at[e], dst_ref=oall.at[e], send_sem=xs.at[1], recv_sem=xr.at[1],
        device_id=pair, device_id_type=MESH,
    )
    swap_seen.start()
    got_seen = pltpu.make_async_remote_copy(
        src_ref=oall.at[e], dst_ref=oall.at[1 - e], send_sem=xs.at[1], recv_sem=xr.at[1],
        device_id=pair, device_id_type=MESH,
    )
    got_seen.wait_recv()
    swap_theta.wait_recv()

    seen = jnp.concatenate([oall[0], oall[1]], axis=0)
    mean = jnp.sum(seen, axis=0, keepdims=True) * (1.0 / 128.0)
    scale = 1.0 / osg[...]
    anomaly = (seen - mean) * scale
    miss = jnp.broadcast_to((ova[...] - mean) * scale, (8, 128))
    dims = (((1,), (1,)), ((), ()))
    gram = lax.dot_general(anomaly, anomaly, dims, precision=HIGHEST, preferred_element_type=F32)
    cvec = lax.dot_general(miss, anomaly, dims, precision=HIGHEST, preferred_element_type=F32)
    gp[...] = gram.reshape(16, 8, 128)
    last = iota((8, 128), 0) == 7
    gp[15] = jnp.where(last, cvec, gram[120:128])

    def spread_out(src, dst, ssem, rsem, count, me, place):
        outs, ins = [], []
        for d in range(1, count):
            j = lax.rem(me + d, count)
            where = place(j)
            outs.append(pltpu.make_async_remote_copy(
                src_ref=src(j), dst_ref=dst.at[me], send_sem=ssem.at[d], recv_sem=rsem.at[me],
                device_id=where, device_id_type=MESH))
            ins.append(pltpu.make_async_remote_copy(
                src_ref=src(j), dst_ref=dst.at[j], send_sem=ssem.at[d], recv_sem=rsem.at[j],
                device_id=where, device_id_type=MESH))
        return outs, ins

    rs[g] = gp[g]
    rs_out, rs_in = spread_out(lambda j: gp.at[j], rs, rss, rsr, ng, g, tile_holder)
    for c in rs_out:
        c.start()
    for c in rs_in:
        c.wait_recv()
    zs[z] = jnp.sum(rs[...], axis=0)
    z_out, z_in = spread_out(lambda j: zs.at[z], zs, zss, zsr, nz, z, lambda j: {"gx": j, "gy": g, "ens": e})
    for c in z_out:
        c.start()
    for c in z_in:
        c.wait_recv()
    ag[g] = jnp.sum(zs[...], axis=0)
    ag_out, ag_in = spread_out(lambda j: ag.at[g], ag, ags, agr, ng, g, tile_holder)
    for c in ag_out:
        c.start()

    thetas[...] = thx[...] + thr[...]
    for c in ag_in:
        c.wait_recv()
    sums[...] = ag[...]

    for copy, sends, _ in halo(4, ex, 0, 8):
        when(sends, copy.wait_send)

    def drain(c, carry):
        for copy, sends, _ in halo(c, qx, 16 * c, 2 * c):
            when(sends, copy.wait_send)
        return carry

    lax.fori_loop(0, 4, drain, 0)
    swap_theta.wait_send()
    swap_seen.wait_send()
    for c in rs_out + z_out + ag_out:
        c.wait_send()


def solve(fin, sums, thetas, fin_out, theta_out, mat, sem):
    e = lax.axis_index("ens")
    out_copy = pltpu.make_async_copy(fin, fin_out, sem)
    out_copy.start()
    th_all = thetas[...]
    th_mean = jnp.sum(th_all, axis=1, keepdims=True) * (1.0 / 128.0)
    mat[16] = th_all - th_mean
    crow = sums[15, 7:8, :]
    sub, ln = iota((8, 128), 0), iota((8, 128), 1)
    last = sub == 7
    tiles = [sums[t] for t in range(16)]
    tiles[15] = jnp.where(last, 0.0, tiles[15])
    total = tiles[0]
    for t in range(1, 16):
        total = total + tiles[t]
    total = jnp.sum(total, axis=0, keepdims=True)
    tiles[15] = jnp.where(last, -total, tiles[15])
    for t in range(16):
        mat[t] = tiles[t] + jnp.where(ln == sub + 8 * t, 127.0, 0.0)

    def lanes_of(x, base):
        return [jnp.broadcast_to(x[:, base + j : base + j + 1], (8, 128)) for j in range(8)]

    def row_of(x, i):
        return jnp.broadcast_to(x[i : i + 1, :], (8, 128))

    cols = lanes_of(tiles[0] + jnp.where(ln == sub, 127.0, 0.0), 0)
    for k in range(16):
        base = 8 * k
        front = (ln >= base) & (ln < base + 8)
        piv = mat[k]
        ahead = lanes_of(piv, base + 8) if k < 15 else []
        row = jnp.where(front, jnp.where(ln == sub + base, 1.0, 0.0), piv)
        for i in range(8):
            at = [row_of(cols[j], i) for j in range(i, 8)]
            inv = 1.0 / at[0]
            mine = sub == i
            step = jnp.where(mine, -1.0, cols[i])
            row = jnp.where(mine, 0.0, row) - step * (row_of(row, i) * inv)
            for j in range(i + 1, 8):
                cols[j] = jnp.where(mine, 0.0, cols[j]) - step * (at[j - i] * inv)
            ahead = [jnp.where(mine, 0.0, x) - step * (row_of(x, i) * inv) for x in ahead]
        row = jnp.where(front, -row, row)
        rows = [row_of(row, i) for i in range(8)]
        for t in range(k + 1, 17):
            x = mat[t]
            by = lanes_of(x, base)
            new = jnp.where(front, 0.0, x)
            for i in range(8):
                new = new - by[i] * rows[i]
            mat[t] = new
            if t == k + 1 and k < 15:
                cols = lanes_of(x, base + 8)
                for j in range(8):
                    for i in range(8):
                        cols[j] = cols[j] - by[i] * row_of(ahead[j], i)
    zt = mat[16]
    shift = jnp.sum(zt * crow, axis=1, keepdims=True)
    fresh = th_mean + 127.0 * zt + shift
    @pl.when(e == 0)
    def _():
        theta_out[...] = fresh[0:4, 0:64]

    @pl.when(e == 1)
    def _():
        theta_out[...] = fresh[0:4, 64:128]

    out_copy.wait()


def local(state, u_vel, v_vel, land, forcing, member_mode, theta, *obs):
    args = (member_mode, state, u_vel, v_vel, land, forcing, theta, *obs)
    hbm = pl.BlockSpec(memory_space=pl.ANY)
    vmem = pl.BlockSpec(memory_space=pltpu.VMEM)
    dma, v = pltpu.SemaphoreType.DMA, lambda *s: pltpu.VMEM(s, F32)
    shape = jax.ShapeDtypeStruct
    fin, sums, thetas = pl.pallas_call(
        kernel,
        out_shape=(shape(state.shape, F32), shape((16, 8, 128), F32), shape((8, 128), F32)),
        in_specs=[pl.BlockSpec(memory_space=pltpu.HBM)] * 10,
        out_specs=(vmem, vmem, vmem),
        scratch_shapes=[
            v(64, 32, 128), v(16, 32, 128), pltpu.VMEM((16, 128), jnp.int32),
            v(10, 32, 128), v(10, 32, 128), v(10, 32, 128), v(10, 32, 128),
            v(32, 128), v(3, 32, 128), v(2, 8, 32, 128), v(2, 3, 32, 128), v(4, 64, 128), v(4, 2, 8, 128),
            v(16, 32, 128), v(16, 32, 128), v(16, 32, 128), v(16, 32, 128),
            v(8, 32, 128), v(8, 32, 128), v(8, 32, 128), v(8, 32, 128), v(8, 32, 128), v(32, 16, 128),
            v(2, 64, 128), v(8, 128), v(8, 128),
            v(16, 8, 128), v(16, 8, 128), v(8, 8, 128), v(16, 8, 128),
            pltpu.VMEM((384, 128), jnp.bfloat16), v(4, 64), pltpu.VMEM((1, 128), jnp.int32), v(1, 128), v(1, 128), pltpu.SMEM((64,), jnp.int32),
            dma((10,)), dma((5, 8)), dma((5, 8)), dma((2,)), dma((2,)),
            dma((16,)), dma((16,)), dma((8,)), dma((8,)), dma((16,)), dma((16,)),
        ],
        compiler_params=pltpu.CompilerParams(collective_id=0, has_side_effects=True, vmem_limit_bytes=20 * 2**20),
    )(*[pltpu.with_memory_space_constraint(a, pltpu.HBM) for a in args])
    return pl.pallas_call(
        solve,
        out_shape=(shape(state.shape, F32), shape(theta.shape, F32)),
        in_specs=[hbm, vmem, vmem],
        out_specs=(hbm, vmem),
        scratch_shapes=[v(17, 8, 128), dma(())],
        compiler_params=pltpu.CompilerParams(vmem_limit_bytes=8 * 2**20),
    )(fin, sums, thetas)


def solution(mesh):
    in_specs = (
        P("ens", "gy", "gx"), P("gy", "gx"), P("gy", "gx"), P("gy", "gx"), P(None, "gy", "gx"),
        P("ens"), P("ens", None), P("gy", "gx", None), P("gy", "gx", None), P("gy", "gx", None),
    )
    out_specs = (P("ens", "gy", "gx"), P("ens", None))

    def run(state, u_vel, v_vel, land, forcing, member_mode, theta, obs_index, obs_values, obs_sigma):
        flat = [a.reshape(a.shape[1:]) for a in (obs_index, obs_values, obs_sigma)]
        fin, new = local(state, u_vel, v_vel, land, forcing, member_mode, theta.T, *flat)
        return fin, new.T

    return jax.shard_map(run, mesh=mesh, in_specs=in_specs, out_specs=out_specs, check_vma=False)
```

```python
import jax
import jax.numpy as jnp
from jax import lax
from jax.experimental import pallas as pl
from jax.experimental.pallas import tpu as pltpu
from jax.sharding import PartitionSpec as P

STEPS = 4
W = 2 * STEPS
MESH = pl.DeviceIdType.MESH
F32 = jnp.float32
HIGHEST = lax.Precision.HIGHEST


def iota(shape, dim):
    return lax.broadcasted_iota(jnp.int32, shape, dim)


def pack_edges(ref, first, rows, count, r_ref, l_ref, group):
    lo, hi = rows
    slot = iota((hi - lo, 128), 1) // 16
    for n in range(count):
        right = left = None
        for k in range(8):
            x = ref[first + 8 * n + k, lo:hi, :]
            a = pltpu.roll(x, (16 * (k + 1)) % 128, 1) if k < 7 else x
            b = pltpu.roll(x, 16 * k, 1) if k else x
            right = a if right is None else jnp.where(slot == k, a, right)
            left = b if left is None else jnp.where(slot == k, b, left)
        r_ref[group + n, lo:hi, :] = right
        l_ref[group + n, lo:hi, :] = left


def strips_of(rv, lv, rvr, lvr, lo, hi):
    inner = iota((hi - lo, 128), 1) % 32 < 16
    left = (
        jnp.where(inner, rvr, pltpu.roll(lv, 16, 1)),
        jnp.where(inner, pltpu.roll(rvr, 112, 1), lv),
    )
    right = (
        jnp.where(inner, rv, pltpu.roll(lvr, 16, 1)),
        jnp.where(inner, pltpu.roll(rv, 112, 1), lvr),
    )
    return left, right


def advance(first, planes, coef, tables, forced, qs, lqs, es, mask, put):
    c0, c1, hy = coef
    ocean, uo, vo = tables
    for step in range(STEPS):
        lo = 2 * step
        nl = 4 * W - 2 - 4 * step
        nn = nl - 2
        for p in range(planes):
            get = (lambda a, n, p=p: first(p, a, n)) if step == 0 else (lambda a, n, p=p: qs[p, a : a + n, :])
            cen = get(lo + 1, nl)
            west = pltpu.roll(cen, 1, 1)
            east = pltpu.roll(cen, 127, 1)
            lap = (get(lo + 2, nl) + get(lo, nl)) + (west + east) - 4.0 * cen
            lqs[p, lo + 1 : lo + 1 + nl, :] = lap * mask[lo + 1 : lo + 1 + nl, :]
            es[p, lo + 1 : lo + 1 + nl, :] = east - west
        at = slice(lo + 2, lo + 2 + nn)
        for p in range(planes):
            get = (lambda a, n, p=p: first(p, a, n)) if step == 0 else (lambda a, n, p=p: qs[p, a : a + n, :])
            lap = lqs[p, at, :]
            around = (lqs[p, lo + 3 : lo + 3 + nn, :] + lqs[p, lo + 1 : lo + 1 + nn, :]) + (
                pltpu.roll(lap, 1, 1) + pltpu.roll(lap, 127, 1)
            )
            dy = get(lo + 3, nn) - get(lo + 1, nn)
            inner = c0(p) * get(lo + 2, nn) + c1(p) * lap - hy(p) * around + forced(p, lo + 2, nn)
            new = ocean(p, lo + 2, nn) * inner - (
                uo(p, lo + 2, nn) * es[p, at, :] + vo(p, lo + 2, nn) * dy
            )
            if step < STEPS - 1:
                qs[p, at, :] = new
            else:
                put(p, new)


def kernel(
    mode_in, state, u_vel, v_vel, land, forcing, theta, obs_index, obs_values, obs_sigma,
    fin, sums, thetas,
    qx, ex, landb, rv, lv, rvr, lvr, mask, tabs, ftab, stabs, coefs, pcoefs,
    qs, lqs, es, fos, qp, endp, oall, thx, thr,
    gp, rs, zs, ag,
    pick, thl, oix, ova, osg, mode, ysem, zsem, lsem, hs, hr, xs, xr, rss, rsr, zss, zsr, ags, agr,
):
    z, g, e = lax.axis_index("gx"), lax.axis_index("gy"), lax.axis_index("ens")
    nz, ng = 8, 16
    up_ok, down_ok = g > 0, g < ng - 1

    def dev(dz, dg):
        return {"gx": lax.rem(z + dz + nz, nz), "gy": lax.rem(g + dg + ng, ng), "ens": e}

    pair = {"gx": z, "gy": g, "ens": 1 - e}
    near = lax.rem(g // 8 + e, 2)

    def tile_holder(j):
        return {"gx": z, "gy": j, "ens": lax.rem(j // 8 + near, 2)}

    barrier = pltpu.get_barrier_semaphore()
    def along_y(d):
        return tile_holder(lax.rem(g + d + ng, ng))

    partners = [dev(a, b) for a in (-1, 0, 1) for b in (-1, 1)] + [dev(-1, 0), dev(1, 0), pair, along_y(-1), along_y(1)]
    for where in partners:
        pl.semaphore_signal(barrier, inc=1, device_id=where, device_id_type=MESH)

    own = pl.ds(W, 16)
    loads = [
        pltpu.make_async_copy(state, qx.at[:, own, :], lsem.at[0]),
        pltpu.make_async_copy(forcing, ex.at[0:8, own, :], lsem.at[1]),
        pltpu.make_async_copy(u_vel, ex.at[8, own, :], lsem.at[2]),
        pltpu.make_async_copy(v_vel, ex.at[9, own, :], lsem.at[3]),
        pltpu.make_async_copy(land, landb, lsem.at[4]),
        pltpu.make_async_copy(theta, thl, lsem.at[5]),
        pltpu.make_async_copy(obs_index, oix, lsem.at[6]),
        pltpu.make_async_copy(obs_values, ova, lsem.at[7]),
        pltpu.make_async_copy(obs_sigma, osg, lsem.at[8]),
        pltpu.make_async_copy(mode_in, mode, lsem.at[9]),
    ]
    for c in loads:
        c.start()

    @pl.when(jnp.logical_not(up_ok))
    def _():
        for ref in (qx, ex, rvr, lvr):
            ref[:, 0:W, :] = jnp.zeros((ref.shape[0], W, 128), F32)

    @pl.when(jnp.logical_not(down_ok))
    def _():
        for ref in (qx, ex, rvr, lvr):
            ref[:, W + 16 :, :] = jnp.zeros((ref.shape[0], W, 128), F32)

    top, bottom, low, high = pl.ds(W, W), pl.ds(16, W), pl.ds(0, W), pl.ds(W + 16, W)

    def halo(c, planes, first, group, rows):
        at, ga = pl.ds(first, 16), pl.ds(group, 2)
        plan = [
            (planes, at, top, planes, high, (0, -1), up_ok, down_ok),
            (planes, at, bottom, planes, low, (0, 1), down_ok, up_ok),
            (rv, ga, own, rvr, own, (1, 0), None, None),
            (lv, ga, own, lvr, own, (-1, 0), None, None),
            (rv, ga, bottom, rvr, low, (1, 1), down_ok, up_ok),
            (rv, ga, top, rvr, high, (1, -1), up_ok, down_ok),
            (lv, ga, bottom, lvr, low, (-1, 1), down_ok, up_ok),
            (lv, ga, top, lvr, high, (-1, -1), up_ok, down_ok),
        ]
        out = []
        for i in range(2) if rows else range(2, 8):
            src, a, sr, dst, dr, where, sends, gets = plan[i]
            copy = pltpu.make_async_remote_copy(
                src_ref=src.at[a, sr, :], dst_ref=dst.at[a, dr, :],
                send_sem=hs.at[c, i], recv_sem=hr.at[c, i],
                device_id=dev(*where), device_id_type=MESH,
            )
            out.append((copy, sends, gets))
        return out

    def when(cond, fn):
        if cond is None:
            fn()
        else:
            pl.when(cond)(fn)

    def send(copies):
        for copy, sends, _ in copies:
            when(sends, copy.start)

    for c in loads[1:5]:
        c.wait()
    ex[10, W : W + 16, :] = (1 - landb[...]).astype(F32)
    ex[11:16, W : W + 16, :] = jnp.zeros((5, 16, 128), F32)
    loads[0].wait()
    pl.semaphore_wait(barrier, len(partners))
    extra = (4, ex, 0, 8)

    def pass_word(step, along_z):
        far = 2**step
        for d in (-far, far):
            pl.semaphore_signal(ysem.at[step], inc=1, device_id=along_y(d), device_id_type=MESH)
            if along_z:
                pl.semaphore_signal(zsem.at[step], inc=1, device_id=dev(d, 0), device_id_type=MESH)

    def hear_word(step, along_z):
        pl.semaphore_wait(ysem.at[step], 2)
        if along_z:
            pl.semaphore_wait(zsem.at[step], 2)

    pass_word(0, True)

    def member_chunk(c):
        return c, qx, 16 * c, 2 * c

    send(halo(*extra, True))

    def send_rows(c, carry):
        send(halo(*member_chunk(c), True))
        return carry

    lax.fori_loop(0, 4, send_rows, 0)
    pack_edges(ex, 0, (W, W + 16), 2, rv, lv, 8)

    def pack_own(c, carry):
        pack_edges(qx, 16 * c, (W, W + 16), 2, rv, lv, 2 * c)
        return carry

    lax.fori_loop(0, 4, pack_own, 0)
    send(halo(*extra, False))

    def send_edges(c, carry):
        send(halo(*member_chunk(c), False))
        return carry

    lax.fori_loop(0, 4, send_edges, 0)

    for c in loads[5:]:
        c.wait()
    same = iota((64, 64), 0) == iota((64, 64), 1)

    def across(row):
        col = jnp.sum(jnp.where(same, jnp.broadcast_to(row, (64, 64)), 0.0), axis=1, keepdims=True)
        return jnp.broadcast_to(col, (64, 128))

    tt = thl[...]
    th = jnp.tanh(tt)
    hyper = 0.005 * (1.0 + 0.5 * th[1:2])
    coefs[0] = across(1.0 - 0.05 * (1.0 + 0.5 * th[2:3]))
    coefs[1] = across(0.05 * (1.0 + 0.5 * th[0:1]) + 4.0 * hyper)
    coefs[2] = across(hyper)
    coefs[3] = across(tt[3:4])
    thx[...] = jnp.zeros((8, 128), F32)

    @pl.when(e == 0)
    def _():
        thx[0:4, 0:64] = thl[...]

    @pl.when(e == 1)
    def _():
        thx[0:4, 64:128] = thl[...]

    slot8 = iota((8, 128), 1) // 32
    for t in range(4):
        for odd in range(2):
            acc = None
            for k in range(4):
                x = coefs[t, pl.ds(odd + 2 * k, 8, stride=8), :]
                acc = x if acc is None else jnp.where(slot8 == k, x, acc)
            pcoefs[t, odd] = acc
    row32 = iota((32, 128), 0)
    no_wall = (jnp.logical_or(row32 >= W, up_ok)) & (jnp.logical_or(row32 < W + 16, down_ok))
    mask[...] = no_wall.astype(F32)


    swap_theta = pltpu.make_async_remote_copy(
        src_ref=thx, dst_ref=thr, send_sem=xs.at[0], recv_sem=xr.at[0], device_id=pair, device_id_type=MESH
    )
    swap_theta.start()

    def wait_for(copies):
        for copy, _, gets in copies:
            when(gets, copy.wait_recv)

    site = oix[...]
    col_pick = jnp.broadcast_to(site % 128, (128, 128)) == iota((128, 128), 0)
    for n in range(3):
        pick[128 * n : 128 * n + 128, :] = col_pick.astype(F32).astype(jnp.bfloat16)
    site_row = jnp.broadcast_to(site // 128, (16, 128)) == iota((16, 128), 0)
    lane = iota((16, 128), 1)
    slot16 = lane % 32 < 16
    edge = (lane < W) | (lane >= 128 - W)
    slot32 = iota((32, 128), 1) // 32

    wait_for(halo(*extra, True))
    hear_word(0, True)
    pass_word(1, True)
    o = ex[10]
    tabs[0] = o
    tabs[1] = 0.5 * ex[8] * o
    tabs[2] = 0.5 * ex[9] * o

    def chunk(c, carry):
        m0 = 16 * c
        wait_for(halo(*member_chunk(c), True))
        for p in range(16):
            fos[p] = coefs[3, pl.ds(m0 + p, 1), :] * ex[mode[m0 + p]]

        def keep(p, new):
            fin[m0 + p] = new

        advance(
            lambda p, a, n: qx[m0 + p, a : a + n, :], 16,
            [lambda p, t=t: coefs[t, pl.ds(m0 + p, 1), :] for t in range(3)],
            [lambda p, a, n, t=t: tabs[t, a : a + n, :] for t in range(3)],
            lambda p, a, n: fos[p, a : a + n, :], qs, lqs, es, mask, keep,
        )
        return carry

    lax.fori_loop(0, 4, chunk, 0)

    hear_word(1, True)
    pass_word(2, False)
    for rows in ((0, W), (W + 16, 32)):
        pack_edges(ex, 0, rows, 2, rv, lv, 8)

    def pack_halo(c, carry):
        for rows in ((0, W), (W + 16, 32)):
            pack_edges(qx, 16 * c, rows, 2, rv, lv, 2 * c)
        return carry

    lax.fori_loop(0, 4, pack_halo, 0)
    wait_for(halo(*extra, False))

    def spread(x, k):
        y = jnp.where(slot32 == k, x, 0.0)
        y = y + pltpu.roll(y, 32, 1)
        return y + pltpu.roll(y, 64, 1)

    both = strips_of(rv[8], lv[8], rvr[8], lvr[8], 0, 32)
    for side in range(2):
        for k in range(8):
            ftab[side, k] = spread(both[side][k % 2], k // 2)
    both = strips_of(rv[9], lv[9], rvr[9], lvr[9], 0, 32)
    for side in range(2):
        even, odd = both[side]
        o = spread(even, 1)
        stabs[side, 0] = o
        stabs[side, 1] = 0.5 * spread(even, 0) * o
        stabs[side, 2] = 0.5 * spread(odd, 0) * o

    def edges_here(c, carry):
        wait_for(halo(*member_chunk(c), False))
        return carry

    lax.fori_loop(0, 4, edges_here, 0)

    def strips(c, carry):
        for n in range(4):
            gr = 4 * c + n
            both = strips_of(rv[gr], lv[gr], rvr[gr], lvr[gr], 0, 32)
            for side in range(2):
                for odd in range(2):
                    p = 4 * n + 2 * side + odd
                    qp[p] = both[side][odd]
                    f = None
                    for k in range(4):
                        x = ftab[side, mode[8 * gr + 2 * k + odd]]
                        f = x if f is None else jnp.where(slot32 == k, x, f)
                    fos[p] = pcoefs[3, odd, pl.ds(gr, 1), :] * f

        def keep(p, new):
            endp[16 * c + p] = new

        advance(
            lambda p, a, n: qp[p, a : a + n, :], 16,
            [lambda p, t=t: pcoefs[t, p % 2, pl.ds(4 * c + p // 4, 1), :] for t in range(3)],
            [lambda p, a, n, t=t: stabs[(p // 2) % 2, t, a : a + n, :] for t in range(3)],
            lambda p, a, n: fos[p, a : a + n, :], qs, lqs, es, mask, keep,
        )
        return carry

    lax.fori_loop(0, 2, strips, 0)

    for c in range(4):
        for q in range(4):
            n, odd = q // 2, q % 2
            ends = jnp.where(slot16, endp[8 * c + 4 * n + 2 + odd], endp[8 * c + 4 * n + odd])
            for k in range(4):
                p = 16 * c + 8 * n + 2 * k + odd
                fin[p] = jnp.where(edge, pltpu.roll(ends, (112 - 32 * k) % 128, 1), fin[p])
    for c in range(4):
        x = fin[16 * c : 16 * c + 16].reshape(256, 128)
        part, parts = x, []
        for _ in range(3):
            parts.append(part.astype(jnp.bfloat16))
            part = part - parts[-1].astype(F32)
        at_col = jnp.dot(jnp.concatenate(parts, axis=1), pick[...], preferred_element_type=F32)
        seen = jnp.where(site_row[None], at_col.reshape(16, 16, 128), 0.0)
        oall[e, 16 * c : 16 * c + 16, :] = jnp.sum(seen, axis=1)

    swap_seen = pltpu.make_async_remote_copy(
        src_ref=oall.at[e], dst_ref=oall.at[e], send_sem=xs.at[1], recv_sem=xr.at[1],
        device_id=pair, device_id_type=MESH,
    )
    swap_seen.start()
    got_seen = pltpu.make_async_remote_copy(
        src_ref=oall.at[e], dst_ref=oall.at[1 - e], send_sem=xs.at[1], recv_sem=xr.at[1],
        device_id=pair, device_id_type=MESH,
    )
    got_seen.wait_recv()
    swap_theta.wait_recv()

    seen = jnp.concatenate([oall[0], oall[1]], axis=0)
    mean = jnp.sum(seen, axis=0, keepdims=True) * (1.0 / 128.0)
    scale = 1.0 / osg[...]
    anomaly = (seen - mean) * scale
    miss = jnp.broadcast_to((ova[...] - mean) * scale, (8, 128))
    dims = (((1,), (1,)), ((), ()))
    gram = lax.dot_general(anomaly, anomaly, dims, precision=HIGHEST, preferred_element_type=F32)
    cvec = lax.dot_general(miss, anomaly, dims, precision=HIGHEST, preferred_element_type=F32)
    gp[...] = gram.reshape(16, 8, 128)
    last = iota((8, 128), 0) == 7
    gp[15] = jnp.where(last, cvec, gram[120:128])

    def spread_out(src, dst, ssem, rsem, count, me, place):
        outs, ins = [], []
        for d in range(1, count):
            j = lax.rem(me + d, count)
            where = place(j)
            outs.append(pltpu.make_async_remote_copy(
                src_ref=src(j), dst_ref=dst.at[me], send_sem=ssem.at[d], recv_sem=rsem.at[me],
                device_id=where, device_id_type=MESH))
            ins.append(pltpu.make_async_remote_copy(
                src_ref=src(j), dst_ref=dst.at[j], send_sem=ssem.at[d], recv_sem=rsem.at[j],
                device_id=where, device_id_type=MESH))
        return outs, ins

    hear_word(2, False)
    rs[g] = gp[g]
    rs_out, rs_in = spread_out(lambda j: gp.at[j], rs, rss, rsr, ng, g, tile_holder)
    for c in rs_out:
        c.start()
    for c in rs_in:
        c.wait_recv()
    zs[z] = jnp.sum(rs[...], axis=0)
    z_out, z_in = spread_out(lambda j: zs.at[z], zs, zss, zsr, nz, z, lambda j: {"gx": j, "gy": g, "ens": e})
    for c in z_out:
        c.start()
    for c in z_in:
        c.wait_recv()
    ag[g] = jnp.sum(zs[...], axis=0)
    ag_out, ag_in = spread_out(lambda j: ag.at[g], ag, ags, agr, ng, g, tile_holder)
    for c in ag_out:
        c.start()

    thetas[...] = thx[...] + thr[...]
    for c in ag_in:
        c.wait_recv()
    sums[...] = ag[...]

    def drain(copies):
        for copy, sends, _ in copies:
            when(sends, copy.wait_send)

    drain(halo(*extra, True))
    drain(halo(*extra, False))

    def drain_chunk(c, carry):
        drain(halo(*member_chunk(c), True))
        drain(halo(*member_chunk(c), False))
        return carry

    lax.fori_loop(0, 4, drain_chunk, 0)
    swap_theta.wait_send()
    swap_seen.wait_send()
    for c in rs_out + z_out + ag_out:
        c.wait_send()


def solve(fin, sums, thetas, fin_out, theta_out, mat, sem):
    e = lax.axis_index("ens")
    out_copy = pltpu.make_async_copy(fin, fin_out, sem)
    out_copy.start()
    th_all = thetas[...]
    th_mean = jnp.sum(th_all, axis=1, keepdims=True) * (1.0 / 128.0)
    mat[16] = th_all - th_mean
    crow = sums[15, 7:8, :]
    sub, ln = iota((8, 128), 0), iota((8, 128), 1)
    last = sub == 7
    tiles = [sums[t] for t in range(16)]
    tiles[15] = jnp.where(last, 0.0, tiles[15])
    total = tiles[0]
    for t in range(1, 16):
        total = total + tiles[t]
    total = jnp.sum(total, axis=0, keepdims=True)
    tiles[15] = jnp.where(last, -total, tiles[15])
    for t in range(16):
        mat[t] = tiles[t] + jnp.where(ln == sub + 8 * t, 127.0, 0.0)

    def lanes_of(x, base):
        return [jnp.broadcast_to(x[:, base + j : base + j + 1], (8, 128)) for j in range(8)]

    def row_of(x, i):
        return jnp.broadcast_to(x[i : i + 1, :], (8, 128))

    cols = lanes_of(tiles[0] + jnp.where(ln == sub, 127.0, 0.0), 0)
    for k in range(16):
        base = 8 * k
        front = (ln >= base) & (ln < base + 8)
        piv = mat[k]
        ahead = lanes_of(piv, base + 8) if k < 15 else []
        row = jnp.where(front, jnp.where(ln == sub + base, 1.0, 0.0), piv)
        for i in range(8):
            at = [row_of(cols[j], i) for j in range(i, 8)]
            inv = 1.0 / at[0]
            mine = sub == i
            step = jnp.where(mine, -1.0, cols[i])
            row = jnp.where(mine, 0.0, row) - step * (row_of(row, i) * inv)
            for j in range(i + 1, 8):
                cols[j] = jnp.where(mine, 0.0, cols[j]) - step * (at[j - i] * inv)
            ahead = [jnp.where(mine, 0.0, x) - step * (row_of(x, i) * inv) for x in ahead]
        row = jnp.where(front, -row, row)
        rows = [row_of(row, i) for i in range(8)]
        for t in range(k + 1, 17):
            x = mat[t]
            by = lanes_of(x, base)
            new = jnp.where(front, 0.0, x)
            for i in range(8):
                new = new - by[i] * rows[i]
            mat[t] = new
            if t == k + 1 and k < 15:
                cols = lanes_of(x, base + 8)
                for j in range(8):
                    for i in range(8):
                        cols[j] = cols[j] - by[i] * row_of(ahead[j], i)
    zt = mat[16]
    shift = jnp.sum(zt * crow, axis=1, keepdims=True)
    fresh = th_mean + 127.0 * zt + shift
    @pl.when(e == 0)
    def _():
        theta_out[...] = fresh[0:4, 0:64]

    @pl.when(e == 1)
    def _():
        theta_out[...] = fresh[0:4, 64:128]

    out_copy.wait()


def local(state, u_vel, v_vel, land, forcing, member_mode, theta, *obs):
    args = (member_mode, state, u_vel, v_vel, land, forcing, theta, *obs)
    hbm = pl.BlockSpec(memory_space=pl.ANY)
    vmem = pl.BlockSpec(memory_space=pltpu.VMEM)
    dma, v = pltpu.SemaphoreType.DMA, lambda *s: pltpu.VMEM(s, F32)
    shape = jax.ShapeDtypeStruct
    fin, sums, thetas = pl.pallas_call(
        kernel,
        out_shape=(shape(state.shape, F32), shape((16, 8, 128), F32), shape((8, 128), F32)),
        in_specs=[pl.BlockSpec(memory_space=pltpu.HBM)] * 10,
        out_specs=(vmem, vmem, vmem),
        scratch_shapes=[
            v(64, 32, 128), v(16, 32, 128), pltpu.VMEM((16, 128), jnp.int32),
            v(10, 32, 128), v(10, 32, 128), v(10, 32, 128), v(10, 32, 128),
            v(32, 128), v(3, 32, 128), v(2, 8, 32, 128), v(2, 3, 32, 128), v(4, 64, 128), v(4, 2, 8, 128),
            v(16, 32, 128), v(16, 32, 128), v(16, 32, 128), v(16, 32, 128),
            v(16, 32, 128), v(32, 16, 128),
            v(2, 64, 128), v(8, 128), v(8, 128),
            v(16, 8, 128), v(16, 8, 128), v(8, 8, 128), v(16, 8, 128),
            pltpu.VMEM((384, 128), jnp.bfloat16), v(4, 64), pltpu.VMEM((1, 128), jnp.int32), v(1, 128), v(1, 128), pltpu.SMEM((64,), jnp.int32),
            pltpu.SemaphoreType.REGULAR((3,)), pltpu.SemaphoreType.REGULAR((2,)), dma((10,)), dma((5, 8)), dma((5, 8)), dma((2,)), dma((2,)),
            dma((16,)), dma((16,)), dma((8,)), dma((8,)), dma((16,)), dma((16,)),
        ],
        compiler_params=pltpu.CompilerParams(collective_id=0, has_side_effects=True, vmem_limit_bytes=20 * 2**20),
    )(*[pltpu.with_memory_space_constraint(a, pltpu.HBM) for a in args])
    return pl.pallas_call(
        solve,
        out_shape=(shape(state.shape, F32), shape(theta.shape, F32)),
        in_specs=[hbm, vmem, vmem],
        out_specs=(hbm, vmem),
        scratch_shapes=[v(17, 8, 128), dma(())],
        compiler_params=pltpu.CompilerParams(vmem_limit_bytes=8 * 2**20),
    )(fin, sums, thetas)


def solution(mesh):
    in_specs = (
        P("ens", "gy", "gx"), P("gy", "gx"), P("gy", "gx"), P("gy", "gx"), P(None, "gy", "gx"),
        P("ens"), P("ens", None), P("gy", "gx", None), P("gy", "gx", None), P("gy", "gx", None),
    )
    out_specs = (P("ens", "gy", "gx"), P("ens", None))

    def run(state, u_vel, v_vel, land, forcing, member_mode, theta, obs_index, obs_values, obs_sigma):
        flat = [a.reshape(a.shape[1:]) for a in (obs_index, obs_values, obs_sigma)]
        fin, new = local(state, u_vel, v_vel, land, forcing, member_mode, theta.T, *flat)
        return fin, new.T

    return jax.shard_map(run, mesh=mesh, in_specs=in_specs, out_specs=out_specs, check_vma=False)
```

```python
import jax
import jax.numpy as jnp
from jax import lax
from jax.experimental import pallas as pl
from jax.experimental.pallas import tpu as pltpu
from jax.sharding import PartitionSpec as P

STEPS = 4
W = 2 * STEPS
MESH = pl.DeviceIdType.MESH
F32 = jnp.float32
HIGHEST = lax.Precision.HIGHEST


def iota(shape, dim):
    return lax.broadcasted_iota(jnp.int32, shape, dim)


def pack_edges(ref, first, rows, count, r_ref, l_ref, group):
    lo, hi = rows
    slot = iota((hi - lo, 128), 1) // 16
    for n in range(count):
        right = left = None
        for k in range(8):
            x = ref[first + 8 * n + k, lo:hi, :]
            a = pltpu.roll(x, (16 * (k + 1)) % 128, 1) if k < 7 else x
            b = pltpu.roll(x, 16 * k, 1) if k else x
            right = a if right is None else jnp.where(slot == k, a, right)
            left = b if left is None else jnp.where(slot == k, b, left)
        r_ref[group + n, lo:hi, :] = right
        l_ref[group + n, lo:hi, :] = left


def strips_of(rv, lv, rvr, lvr, lo, hi):
    inner = iota((hi - lo, 128), 1) % 32 < 16
    left = (
        jnp.where(inner, rvr, pltpu.roll(lv, 16, 1)),
        jnp.where(inner, pltpu.roll(rvr, 112, 1), lv),
    )
    right = (
        jnp.where(inner, rv, pltpu.roll(lvr, 16, 1)),
        jnp.where(inner, pltpu.roll(rv, 112, 1), lvr),
    )
    return left, right


def advance(first, planes, coef, tables, forced, qs, lqs, es, mask, put):
    c0, c1, hy = coef
    ocean, uo, vo = tables
    for step in range(STEPS):
        lo = 2 * step
        nl = 4 * W - 2 - 4 * step
        nn = nl - 2
        for p in range(planes):
            get = (lambda a, n, p=p: first(p, a, n)) if step == 0 else (lambda a, n, p=p: qs[p, a : a + n, :])
            cen = get(lo + 1, nl)
            west = pltpu.roll(cen, 1, 1)
            east = pltpu.roll(cen, 127, 1)
            lap = (get(lo + 2, nl) + get(lo, nl)) + (west + east) - 4.0 * cen
            lqs[p, lo + 1 : lo + 1 + nl, :] = lap * mask[lo + 1 : lo + 1 + nl, :]
            es[p, lo + 1 : lo + 1 + nl, :] = east - west
        at = slice(lo + 2, lo + 2 + nn)
        for p in range(planes):
            get = (lambda a, n, p=p: first(p, a, n)) if step == 0 else (lambda a, n, p=p: qs[p, a : a + n, :])
            lap = lqs[p, at, :]
            around = (lqs[p, lo + 3 : lo + 3 + nn, :] + lqs[p, lo + 1 : lo + 1 + nn, :]) + (
                pltpu.roll(lap, 1, 1) + pltpu.roll(lap, 127, 1)
            )
            dy = get(lo + 3, nn) - get(lo + 1, nn)
            inner = c0(p) * get(lo + 2, nn) + c1(p) * lap - hy(p) * around + forced(p, lo + 2, nn)
            new = ocean(p, lo + 2, nn) * inner - (
                uo(p, lo + 2, nn) * es[p, at, :] + vo(p, lo + 2, nn) * dy
            )
            if step < STEPS - 1:
                qs[p, at, :] = new
            else:
                put(p, new)


def kernel(
    mode_in, state, u_vel, v_vel, land, forcing, theta, obs_index, obs_values, obs_sigma,
    fin, sums, thetas,
    qx, ex, landb, rv, lv, rvr, lvr, mask, tabs, ftab, stabs, coefs, pcoefs,
    qs, lqs, es, fos, qp, endp, oall, thx, thr,
    gp, rs, zs, ag,
    pick, thl, oix, ova, osg, mode, ysem, zsem, lsem, hs, hr, xs, xr, rss, rsr, zss, zsr, ags, agr,
):
    z, g, e = lax.axis_index("gx"), lax.axis_index("gy"), lax.axis_index("ens")
    nz, ng = 8, 16
    up_ok, down_ok = g > 0, g < ng - 1

    def dev(dz, dg):
        return {"gx": lax.rem(z + dz + nz, nz), "gy": lax.rem(g + dg + ng, ng), "ens": e}

    pair = {"gx": z, "gy": g, "ens": 1 - e}
    near = lax.rem(g // 8 + e, 2)

    def tile_holder(j):
        return {"gx": z, "gy": j, "ens": lax.rem(j // 8 + near, 2)}

    barrier = pltpu.get_barrier_semaphore()
    def along_y(d):
        return tile_holder(lax.rem(g + d + ng, ng))

    partners = [dev(a, b) for a in (-1, 0, 1) for b in (-1, 1)] + [dev(-1, 0), dev(1, 0), pair, along_y(-1), along_y(1)]
    for where in partners:
        pl.semaphore_signal(barrier, inc=1, device_id=where, device_id_type=MESH)

    own = pl.ds(W, 16)
    loads = [
        pltpu.make_async_copy(state, qx.at[:, own, :], lsem.at[0]),
        pltpu.make_async_copy(forcing, ex.at[0:8, own, :], lsem.at[1]),
        pltpu.make_async_copy(u_vel, ex.at[8, own, :], lsem.at[2]),
        pltpu.make_async_copy(v_vel, ex.at[9, own, :], lsem.at[3]),
        pltpu.make_async_copy(land, landb, lsem.at[4]),
        pltpu.make_async_copy(theta, thl, lsem.at[5]),
        pltpu.make_async_copy(obs_index, oix, lsem.at[6]),
        pltpu.make_async_copy(obs_values, ova, lsem.at[7]),
        pltpu.make_async_copy(obs_sigma, osg, lsem.at[8]),
        pltpu.make_async_copy(mode_in, mode, lsem.at[9]),
    ]
    for c in loads:
        c.start()

    @pl.when(jnp.logical_not(up_ok))
    def _():
        for ref in (qx, ex, rvr, lvr):
            ref[:, 0:W, :] = jnp.zeros((ref.shape[0], W, 128), F32)

    @pl.when(jnp.logical_not(down_ok))
    def _():
        for ref in (qx, ex, rvr, lvr):
            ref[:, W + 16 :, :] = jnp.zeros((ref.shape[0], W, 128), F32)

    top, bottom, low, high = pl.ds(W, W), pl.ds(16, W), pl.ds(0, W), pl.ds(W + 16, W)

    def halo(c, planes, first, group, rows):
        at, ga = pl.ds(first, 16), pl.ds(group, 2)
        plan = [
            (planes, at, top, planes, high, (0, -1), up_ok, down_ok),
            (planes, at, bottom, planes, low, (0, 1), down_ok, up_ok),
            (rv, ga, own, rvr, own, (1, 0), None, None),
            (lv, ga, own, lvr, own, (-1, 0), None, None),
            (rv, ga, bottom, rvr, low, (1, 1), down_ok, up_ok),
            (rv, ga, top, rvr, high, (1, -1), up_ok, down_ok),
            (lv, ga, bottom, lvr, low, (-1, 1), down_ok, up_ok),
            (lv, ga, top, lvr, high, (-1, -1), up_ok, down_ok),
        ]
        out = []
        for i in range(2) if rows else range(2, 8):
            src, a, sr, dst, dr, where, sends, gets = plan[i]
            copy = pltpu.make_async_remote_copy(
                src_ref=src.at[a, sr, :], dst_ref=dst.at[a, dr, :],
                send_sem=hs.at[c, i], recv_sem=hr.at[c, i],
                device_id=dev(*where), device_id_type=MESH,
            )
            out.append((copy, sends, gets))
        return out

    def when(cond, fn):
        if cond is None:
            fn()
        else:
            pl.when(cond)(fn)

    def send(copies):
        for copy, sends, _ in copies:
            when(sends, copy.start)

    for c in loads[1:5]:
        c.wait()
    ex[10, W : W + 16, :] = (1 - landb[...]).astype(F32)
    ex[11:16, W : W + 16, :] = jnp.zeros((5, 16, 128), F32)
    loads[0].wait()
    pl.semaphore_wait(barrier, len(partners))
    extra = (4, ex, 0, 8)

    def pass_word(step, along_z):
        far = 2**step
        for d in (-far, far):
            pl.semaphore_signal(ysem.at[step], inc=1, device_id=along_y(d), device_id_type=MESH)
            if along_z:
                pl.semaphore_signal(zsem.at[step], inc=1, device_id=dev(d, 0), device_id_type=MESH)

    def hear_word(step, along_z):
        pl.semaphore_wait(ysem.at[step], 2)
        if along_z:
            pl.semaphore_wait(zsem.at[step], 2)

    pass_word(0, True)

    def member_chunk(c):
        return c, qx, 16 * c, 2 * c

    send(halo(*extra, True))

    def send_rows(c, carry):
        send(halo(*member_chunk(c), True))
        return carry

    lax.fori_loop(0, 4, send_rows, 0)
    pack_edges(ex, 0, (W, W + 16), 2, rv, lv, 8)

    def pack_own(c, carry):
        pack_edges(qx, 16 * c, (W, W + 16), 2, rv, lv, 2 * c)
        return carry

    lax.fori_loop(0, 4, pack_own, 0)
    send(halo(*extra, False))

    def send_edges(c, carry):
        send(halo(*member_chunk(c), False))
        return carry

    lax.fori_loop(0, 4, send_edges, 0)

    for c in loads[5:]:
        c.wait()
    same = iota((64, 64), 0) == iota((64, 64), 1)

    def across(row):
        col = jnp.sum(jnp.where(same, jnp.broadcast_to(row, (64, 64)), 0.0), axis=1, keepdims=True)
        return jnp.broadcast_to(col, (64, 128))

    tt = thl[...]
    th = jnp.tanh(tt)
    hyper = 0.005 * (1.0 + 0.5 * th[1:2])
    coefs[0] = across(1.0 - 0.05 * (1.0 + 0.5 * th[2:3]))
    coefs[1] = across(0.05 * (1.0 + 0.5 * th[0:1]) + 4.0 * hyper)
    coefs[2] = across(hyper)
    coefs[3] = across(tt[3:4])
    thx[...] = jnp.zeros((8, 128), F32)

    @pl.when(e == 0)
    def _():
        thx[0:4, 0:64] = thl[...]

    @pl.when(e == 1)
    def _():
        thx[0:4, 64:128] = thl[...]

    slot8 = iota((8, 128), 1) // 32
    for t in range(4):
        for odd in range(2):
            acc = None
            for k in range(4):
                x = coefs[t, pl.ds(odd + 2 * k, 8, stride=8), :]
                acc = x if acc is None else jnp.where(slot8 == k, x, acc)
            pcoefs[t, odd] = acc
    row32 = iota((32, 128), 0)
    no_wall = (jnp.logical_or(row32 >= W, up_ok)) & (jnp.logical_or(row32 < W + 16, down_ok))
    mask[...] = no_wall.astype(F32)


    swap_theta = pltpu.make_async_remote_copy(
        src_ref=thx, dst_ref=thr, send_sem=xs.at[0], recv_sem=xr.at[0], device_id=pair, device_id_type=MESH
    )
    swap_theta.start()

    def wait_for(copies):
        for copy, _, gets in copies:
            when(gets, copy.wait_recv)

    site = oix[...]
    col_pick = jnp.broadcast_to(site % 128, (128, 128)) == iota((128, 128), 0)
    for n in range(3):
        pick[128 * n : 128 * n + 128, :] = col_pick.astype(F32).astype(jnp.bfloat16)
    site_row = jnp.broadcast_to(site // 128, (16, 128)) == iota((16, 128), 0)
    lane = iota((16, 128), 1)
    slot16 = lane % 32 < 16
    edge = (lane < W) | (lane >= 128 - W)
    slot32 = iota((32, 128), 1) // 32

    wait_for(halo(*extra, True))
    hear_word(0, True)
    pass_word(1, True)
    o = ex[10]
    tabs[0] = o
    tabs[1] = 0.5 * ex[8] * o
    tabs[2] = 0.5 * ex[9] * o

    def chunk(c, carry):
        m0 = 16 * c
        wait_for(halo(*member_chunk(c), True))
        for p in range(16):
            fos[p] = coefs[3, pl.ds(m0 + p, 1), :] * ex[mode[m0 + p]]

        def keep(p, new):
            fin[m0 + p] = new

        advance(
            lambda p, a, n: qx[m0 + p, a : a + n, :], 16,
            [lambda p, t=t: coefs[t, pl.ds(m0 + p, 1), :] for t in range(3)],
            [lambda p, a, n, t=t: tabs[t, a : a + n, :] for t in range(3)],
            lambda p, a, n: fos[p, a : a + n, :], qs, lqs, es, mask, keep,
        )
        return carry

    lax.fori_loop(0, 4, chunk, 0)

    hear_word(1, True)
    pass_word(2, False)
    for rows in ((0, W), (W + 16, 32)):
        pack_edges(ex, 0, rows, 2, rv, lv, 8)

    def pack_halo(c, carry):
        for rows in ((0, W), (W + 16, 32)):
            pack_edges(qx, 16 * c, rows, 2, rv, lv, 2 * c)
        return carry

    lax.fori_loop(0, 4, pack_halo, 0)
    wait_for(halo(*extra, False))

    def spread(x, k):
        y = jnp.where(slot32 == k, x, 0.0)
        y = y + pltpu.roll(y, 32, 1)
        return y + pltpu.roll(y, 64, 1)

    both = strips_of(rv[8], lv[8], rvr[8], lvr[8], 0, 32)
    for side in range(2):
        for k in range(8):
            ftab[side, k] = spread(both[side][k % 2], k // 2)
    both = strips_of(rv[9], lv[9], rvr[9], lvr[9], 0, 32)
    for side in range(2):
        even, odd = both[side]
        o = spread(even, 1)
        stabs[side, 0] = o
        stabs[side, 1] = 0.5 * spread(even, 0) * o
        stabs[side, 2] = 0.5 * spread(odd, 0) * o

    def edges_here(c, carry):
        wait_for(halo(*member_chunk(c), False))
        return carry

    lax.fori_loop(0, 4, edges_here, 0)

    def strips(c, carry):
        for n in range(4):
            gr = 4 * c + n
            both = strips_of(rv[gr], lv[gr], rvr[gr], lvr[gr], 0, 32)
            for side in range(2):
                for odd in range(2):
                    p = 4 * n + 2 * side + odd
                    qp[p] = both[side][odd]
                    f = None
                    for k in range(4):
                        x = ftab[side, mode[8 * gr + 2 * k + odd]]
                        f = x if f is None else jnp.where(slot32 == k, x, f)
                    fos[p] = pcoefs[3, odd, pl.ds(gr, 1), :] * f

        def keep(p, new):
            endp[16 * c + p] = new

        advance(
            lambda p, a, n: qp[p, a : a + n, :], 16,
            [lambda p, t=t: pcoefs[t, p % 2, pl.ds(4 * c + p // 4, 1), :] for t in range(3)],
            [lambda p, a, n, t=t: stabs[(p // 2) % 2, t, a : a + n, :] for t in range(3)],
            lambda p, a, n: fos[p, a : a + n, :], qs, lqs, es, mask, keep,
        )
        return carry

    lax.fori_loop(0, 2, strips, 0)

    for c in range(4):
        for q in range(4):
            n, odd = q // 2, q % 2
            ends = jnp.where(slot16, endp[8 * c + 4 * n + 2 + odd], endp[8 * c + 4 * n + odd])
            for k in range(4):
                p = 16 * c + 8 * n + 2 * k + odd
                fin[p] = jnp.where(edge, pltpu.roll(ends, (112 - 32 * k) % 128, 1), fin[p])
    for c in range(4):
        x = fin[16 * c : 16 * c + 16].reshape(256, 128)
        part, parts = x, []
        for _ in range(3):
            parts.append(part.astype(jnp.bfloat16))
            part = part - parts[-1].astype(F32)
        at_col = jnp.dot(jnp.concatenate(parts, axis=1), pick[...], preferred_element_type=F32)
        seen = jnp.where(site_row[None], at_col.reshape(16, 16, 128), 0.0)
        oall[e, 16 * c : 16 * c + 16, :] = jnp.sum(seen, axis=1)

    swap_seen = pltpu.make_async_remote_copy(
        src_ref=oall.at[e], dst_ref=oall.at[e], send_sem=xs.at[1], recv_sem=xr.at[1],
        device_id=pair, device_id_type=MESH,
    )
    swap_seen.start()
    got_seen = pltpu.make_async_remote_copy(
        src_ref=oall.at[e], dst_ref=oall.at[1 - e], send_sem=xs.at[1], recv_sem=xr.at[1],
        device_id=pair, device_id_type=MESH,
    )
    got_seen.wait_recv()
    swap_theta.wait_recv()

    seen = jnp.concatenate([oall[0], oall[1]], axis=0)
    mean = jnp.sum(seen, axis=0, keepdims=True) * (1.0 / 128.0)
    scale = 1.0 / osg[...]
    anomaly = (seen - mean) * scale
    miss = jnp.broadcast_to((ova[...] - mean) * scale, (8, 128))
    dims = (((1,), (1,)), ((), ()))
    gram = lax.dot_general(anomaly, anomaly, dims, precision=HIGHEST, preferred_element_type=F32)
    cvec = lax.dot_general(miss, anomaly, dims, precision=HIGHEST, preferred_element_type=F32)
    last = iota((128, 128), 0) == 127
    gp[...] = jnp.where(last, cvec[0:1, :], gram).reshape(8, 16, 128)

    owner, mine = lax.rem(g, 2) == 1, g // 2

    def to(src, dst, ssem, rsem, where):
        return pltpu.make_async_remote_copy(
            src_ref=src, dst_ref=dst, send_sem=ssem, recv_sem=rsem, device_id=where, device_id_type=MESH
        )

    def rows_to_owner(d):
        j = lax.rem(mine + d, 8)
        return to(gp.at[j], rs.at[g], rss.at[d], rsr.at[g], tile_holder(2 * j + 1))

    def rows_to_gx(d):
        where = {"gx": lax.rem(z + d, nz), "gy": g, "ens": e}
        return to(zs.at[z], zs.at[z], zss.at[d], zsr.at[z], where)

    def rows_to_all(d):
        return to(ag.at[mine], ag.at[mine], ags.at[d], agr.at[mine], tile_holder(lax.rem(g + d, ng)))

    def arrived(ref, i, rsem, ssem):
        to(ref.at[i], ref.at[i], ssem, rsem.at[i], pair).wait_recv()

    hear_word(2, False)
    for d in range(1, 8):
        rows_to_owner(d).start()
    pl.when(jnp.logical_not(owner))(lambda: rows_to_owner(0).start())

    @pl.when(owner)
    def _():
        rs[g] = gp[mine]
        for d in range(1, ng):
            arrived(rs, lax.rem(g + d, ng), rsr, rss.at[0])
        zs[z] = jnp.sum(rs[...], axis=0)
        for d in range(1, nz):
            rows_to_gx(d).start()
        for d in range(1, nz):
            arrived(zs, lax.rem(z + d, nz), zsr, zss.at[0])
        ag[mine] = jnp.sum(zs[...], axis=0)
        for d in range(1, ng):
            rows_to_all(d).start()

    thetas[...] = thx[...] + thr[...]
    for d in range(1, 8):
        arrived(ag, lax.rem(mine + d, 8), agr, ags.at[0])
    pl.when(jnp.logical_not(owner))(lambda: arrived(ag, mine, agr, ags.at[0]))
    sums[...] = ag[...].reshape(16, 8, 128)

    def drain(copies):
        for copy, sends, _ in copies:
            when(sends, copy.wait_send)

    drain(halo(*extra, True))
    drain(halo(*extra, False))

    def drain_chunk(c, carry):
        drain(halo(*member_chunk(c), True))
        drain(halo(*member_chunk(c), False))
        return carry

    lax.fori_loop(0, 4, drain_chunk, 0)
    swap_theta.wait_send()
    swap_seen.wait_send()
    for d in range(1, 8):
        rows_to_owner(d).wait_send()
    pl.when(jnp.logical_not(owner))(lambda: rows_to_owner(0).wait_send())

    @pl.when(owner)
    def _():
        for d in range(1, nz):
            rows_to_gx(d).wait_send()
        for d in range(1, ng):
            rows_to_all(d).wait_send()


def solve(fin, sums, thetas, fin_out, theta_out, mat, sem):
    e = lax.axis_index("ens")
    out_copy = pltpu.make_async_copy(fin, fin_out, sem)
    out_copy.start()
    th_all = thetas[...]
    th_mean = jnp.sum(th_all, axis=1, keepdims=True) * (1.0 / 128.0)
    mat[16] = th_all - th_mean
    crow = sums[15, 7:8, :]
    sub, ln = iota((8, 128), 0), iota((8, 128), 1)
    last = sub == 7
    tiles = [sums[t] for t in range(16)]
    tiles[15] = jnp.where(last, 0.0, tiles[15])
    total = tiles[0]
    for t in range(1, 16):
        total = total + tiles[t]
    total = jnp.sum(total, axis=0, keepdims=True)
    tiles[15] = jnp.where(last, -total, tiles[15])
    for t in range(16):
        mat[t] = tiles[t] + jnp.where(ln == sub + 8 * t, 127.0, 0.0)

    def lanes_of(x, base):
        return [jnp.broadcast_to(x[:, base + j : base + j + 1], (8, 128)) for j in range(8)]

    def row_of(x, i):
        return jnp.broadcast_to(x[i : i + 1, :], (8, 128))

    cols = lanes_of(tiles[0] + jnp.where(ln == sub, 127.0, 0.0), 0)
    for k in range(16):
        base = 8 * k
        front = (ln >= base) & (ln < base + 8)
        piv = mat[k]
        ahead = lanes_of(piv, base + 8) if k < 15 else []
        row = jnp.where(front, jnp.where(ln == sub + base, 1.0, 0.0), piv)
        for i in range(8):
            at = [row_of(cols[j], i) for j in range(i, 8)]
            inv = 1.0 / at[0]
            mine = sub == i
            step = jnp.where(mine, -1.0, cols[i])
            row = jnp.where(mine, 0.0, row) - step * (row_of(row, i) * inv)
            for j in range(i + 1, 8):
                cols[j] = jnp.where(mine, 0.0, cols[j]) - step * (at[j - i] * inv)
            ahead = [jnp.where(mine, 0.0, x) - step * (row_of(x, i) * inv) for x in ahead]
        row = jnp.where(front, -row, row)
        rows = [row_of(row, i) for i in range(8)]
        for t in range(k + 1, 17):
            x = mat[t]
            by = lanes_of(x, base)
            new = jnp.where(front, 0.0, x)
            for i in range(8):
                new = new - by[i] * rows[i]
            mat[t] = new
            if t == k + 1 and k < 15:
                cols = lanes_of(x, base + 8)
                for j in range(8):
                    for i in range(8):
                        cols[j] = cols[j] - by[i] * row_of(ahead[j], i)
    zt = mat[16]
    shift = jnp.sum(zt * crow, axis=1, keepdims=True)
    fresh = th_mean + 127.0 * zt + shift
    @pl.when(e == 0)
    def _():
        theta_out[...] = fresh[0:4, 0:64]

    @pl.when(e == 1)
    def _():
        theta_out[...] = fresh[0:4, 64:128]

    out_copy.wait()


def local(state, u_vel, v_vel, land, forcing, member_mode, theta, *obs):
    args = (member_mode, state, u_vel, v_vel, land, forcing, theta, *obs)
    hbm = pl.BlockSpec(memory_space=pl.ANY)
    vmem = pl.BlockSpec(memory_space=pltpu.VMEM)
    dma, v = pltpu.SemaphoreType.DMA, lambda *s: pltpu.VMEM(s, F32)
    shape = jax.ShapeDtypeStruct
    fin, sums, thetas = pl.pallas_call(
        kernel,
        out_shape=(shape(state.shape, F32), shape((16, 8, 128), F32), shape((8, 128), F32)),
        in_specs=[pl.BlockSpec(memory_space=pltpu.HBM)] * 10,
        out_specs=(vmem, vmem, vmem),
        scratch_shapes=[
            v(64, 32, 128), v(16, 32, 128), pltpu.VMEM((16, 128), jnp.int32),
            v(10, 32, 128), v(10, 32, 128), v(10, 32, 128), v(10, 32, 128),
            v(32, 128), v(3, 32, 128), v(2, 8, 32, 128), v(2, 3, 32, 128), v(4, 64, 128), v(4, 2, 8, 128),
            v(16, 32, 128), v(16, 32, 128), v(16, 32, 128), v(16, 32, 128),
            v(16, 32, 128), v(32, 16, 128),
            v(2, 64, 128), v(8, 128), v(8, 128),
            v(8, 16, 128), v(16, 16, 128), v(8, 16, 128), v(8, 16, 128),
            pltpu.VMEM((384, 128), jnp.bfloat16), v(4, 64), pltpu.VMEM((1, 128), jnp.int32), v(1, 128), v(1, 128), pltpu.SMEM((64,), jnp.int32),
            pltpu.SemaphoreType.REGULAR((3,)), pltpu.SemaphoreType.REGULAR((2,)), dma((10,)), dma((5, 8)), dma((5, 8)), dma((2,)), dma((2,)),
            dma((8,)), dma((16,)), dma((8,)), dma((8,)), dma((16,)), dma((8,)),
        ],
        compiler_params=pltpu.CompilerParams(collective_id=0, has_side_effects=True, vmem_limit_bytes=20 * 2**20),
    )(*[pltpu.with_memory_space_constraint(a, pltpu.HBM) for a in args])
    return pl.pallas_call(
        solve,
        out_shape=(shape(state.shape, F32), shape(theta.shape, F32)),
        in_specs=[hbm, vmem, vmem],
        out_specs=(hbm, vmem),
        scratch_shapes=[v(17, 8, 128), dma(())],
        compiler_params=pltpu.CompilerParams(vmem_limit_bytes=8 * 2**20),
    )(fin, sums, thetas)


def solution(mesh):
    in_specs = (
        P("ens", "gy", "gx"), P("gy", "gx"), P("gy", "gx"), P("gy", "gx"), P(None, "gy", "gx"),
        P("ens"), P("ens", None), P("gy", "gx", None), P("gy", "gx", None), P("gy", "gx", None),
    )
    out_specs = (P("ens", "gy", "gx"), P("ens", None))

    def run(state, u_vel, v_vel, land, forcing, member_mode, theta, obs_index, obs_values, obs_sigma):
        flat = [a.reshape(a.shape[1:]) for a in (obs_index, obs_values, obs_sigma)]
        fin, new = local(state, u_vel, v_vel, land, forcing, member_mode, theta.T, *flat)
        return fin, new.T

    return jax.shard_map(run, mesh=mesh, in_specs=in_specs, out_specs=out_specs, check_vma=False)
```

```python
import jax
import jax.numpy as jnp
from jax import lax
from jax.experimental import pallas as pl
from jax.experimental.pallas import tpu as pltpu
from jax.sharding import PartitionSpec as P

STEPS = 4
W = 2 * STEPS
MESH = pl.DeviceIdType.MESH
F32 = jnp.float32
HIGHEST = lax.Precision.HIGHEST


def iota(shape, dim):
    return lax.broadcasted_iota(jnp.int32, shape, dim)


def pack_edges(ref, first, rows, count, r_ref, l_ref, group):
    lo, hi = rows
    slot = iota((hi - lo, 128), 1) // 16
    for n in range(count):
        right = left = None
        for k in range(8):
            x = ref[first + 8 * n + k, lo:hi, :]
            a = pltpu.roll(x, (16 * (k + 1)) % 128, 1) if k < 7 else x
            b = pltpu.roll(x, 16 * k, 1) if k else x
            right = a if right is None else jnp.where(slot == k, a, right)
            left = b if left is None else jnp.where(slot == k, b, left)
        r_ref[group + n, lo:hi, :] = right
        l_ref[group + n, lo:hi, :] = left


def strips_of(rv, lv, rvr, lvr, lo, hi):
    inner = iota((hi - lo, 128), 1) % 32 < 16
    left = (
        jnp.where(inner, rvr, pltpu.roll(lv, 16, 1)),
        jnp.where(inner, pltpu.roll(rvr, 112, 1), lv),
    )
    right = (
        jnp.where(inner, rv, pltpu.roll(lvr, 16, 1)),
        jnp.where(inner, pltpu.roll(rv, 112, 1), lvr),
    )
    return left, right


def advance(first, planes, coef, tables, forced, qs, lqs, es, mask, put):
    c0, c1, hy = coef
    ocean, uo, vo = tables
    for step in range(STEPS):
        lo = 2 * step
        nl = 4 * W - 2 - 4 * step
        nn = nl - 2
        for p in range(planes):
            get = (lambda a, n, p=p: first(p, a, n)) if step == 0 else (lambda a, n, p=p: qs[p, a : a + n, :])
            cen = get(lo + 1, nl)
            west = pltpu.roll(cen, 1, 1)
            east = pltpu.roll(cen, 127, 1)
            lap = (get(lo + 2, nl) + get(lo, nl)) + (west + east) - 4.0 * cen
            lqs[p, lo + 1 : lo + 1 + nl, :] = lap * mask[lo + 1 : lo + 1 + nl, :]
            es[p, lo + 1 : lo + 1 + nl, :] = east - west
        at = slice(lo + 2, lo + 2 + nn)
        for p in range(planes):
            get = (lambda a, n, p=p: first(p, a, n)) if step == 0 else (lambda a, n, p=p: qs[p, a : a + n, :])
            lap = lqs[p, at, :]
            around = (lqs[p, lo + 3 : lo + 3 + nn, :] + lqs[p, lo + 1 : lo + 1 + nn, :]) + (
                pltpu.roll(lap, 1, 1) + pltpu.roll(lap, 127, 1)
            )
            dy = get(lo + 3, nn) - get(lo + 1, nn)
            inner = c0(p) * get(lo + 2, nn) + c1(p) * lap - hy(p) * around + forced(p, lo + 2, nn)
            new = ocean(p, lo + 2, nn) * inner - (
                uo(p, lo + 2, nn) * es[p, at, :] + vo(p, lo + 2, nn) * dy
            )
            if step < STEPS - 1:
                qs[p, at, :] = new
            else:
                put(p, new)


def kernel(
    mode_in, state, u_vel, v_vel, land, forcing, theta, obs_index, obs_values, obs_sigma,
    fin, sums, thetas,
    qx, ex, landb, rv, lv, rvr, lvr, mask, tabs, ftab, stabs, coefs, pcoefs,
    qs, lqs, es, fos, qp, endp, oall, thx, thr,
    gp, rs, zs, ag,
    pick, thl, oix, ova, osg, mode, ysem, zsem, lsem, hs, hr, xs, xr, rss, rsr, zss, zsr, ags, agr,
):
    z, g, e = lax.axis_index("gx"), lax.axis_index("gy"), lax.axis_index("ens")
    nz, ng = 8, 16
    up_ok, down_ok = g > 0, g < ng - 1

    def dev(dz, dg):
        return {"gx": lax.rem(z + dz + nz, nz), "gy": lax.rem(g + dg + ng, ng), "ens": e}

    pair = {"gx": z, "gy": g, "ens": 1 - e}
    near = lax.rem(g // 8 + e, 2)

    def tile_holder(j):
        return {"gx": z, "gy": j, "ens": lax.rem(j // 8 + near, 2)}

    barrier = pltpu.get_barrier_semaphore()
    def along_y(d):
        return tile_holder(lax.rem(g + d + ng, ng))

    partners = [dev(a, b) for a in (-1, 0, 1) for b in (-1, 1)] + [dev(-1, 0), dev(1, 0), pair, along_y(-1), along_y(1)]
    for where in partners:
        pl.semaphore_signal(barrier, inc=1, device_id=where, device_id_type=MESH)

    own = pl.ds(W, 16)
    loads = [
        pltpu.make_async_copy(state, qx.at[:, own, :], lsem.at[0]),
        pltpu.make_async_copy(forcing, ex.at[0:8, own, :], lsem.at[1]),
        pltpu.make_async_copy(u_vel, ex.at[8, own, :], lsem.at[2]),
        pltpu.make_async_copy(v_vel, ex.at[9, own, :], lsem.at[3]),
        pltpu.make_async_copy(land, landb, lsem.at[4]),
        pltpu.make_async_copy(theta, thl, lsem.at[5]),
        pltpu.make_async_copy(obs_index, oix, lsem.at[6]),
        pltpu.make_async_copy(obs_values, ova, lsem.at[7]),
        pltpu.make_async_copy(obs_sigma, osg, lsem.at[8]),
        pltpu.make_async_copy(mode_in, mode, lsem.at[9]),
    ]
    for c in loads:
        c.start()

    @pl.when(jnp.logical_not(up_ok))
    def _():
        for ref in (qx, ex, rv, lv, rvr, lvr):
            ref[:, 0:W, :] = jnp.zeros((ref.shape[0], W, 128), F32)

    @pl.when(jnp.logical_not(down_ok))
    def _():
        for ref in (qx, ex, rv, lv, rvr, lvr):
            ref[:, W + 16 :, :] = jnp.zeros((ref.shape[0], W, 128), F32)

    top, bottom, low, high = pl.ds(W, W), pl.ds(16, W), pl.ds(0, W), pl.ds(W + 16, W)

    def halo(c, planes, first, group, rows):
        at, ga = pl.ds(first, 16 if planes is qx else 11), pl.ds(group, 2)
        plan = [
            (planes, at, top, planes, high, (0, -1), up_ok, down_ok),
            (planes, at, bottom, planes, low, (0, 1), down_ok, up_ok),
            (rv, ga, own, rvr, own, (1, 0), None, None),
            (lv, ga, own, lvr, own, (-1, 0), None, None),
            (rv, ga, bottom, rvr, low, (1, 1), down_ok, up_ok),
            (rv, ga, top, rvr, high, (1, -1), up_ok, down_ok),
            (lv, ga, bottom, lvr, low, (-1, 1), down_ok, up_ok),
            (lv, ga, top, lvr, high, (-1, -1), up_ok, down_ok),
            (rv, ga, top, rv, high, (0, -1), up_ok, down_ok),
            (rv, ga, bottom, rv, low, (0, 1), down_ok, up_ok),
            (lv, ga, top, lv, high, (0, -1), up_ok, down_ok),
            (lv, ga, bottom, lv, low, (0, 1), down_ok, up_ok),
        ]
        out = []
        for i in range(2) if rows else range(2, 12):
            src, a, sr, dst, dr, where, sends, gets = plan[i]
            copy = pltpu.make_async_remote_copy(
                src_ref=src.at[a, sr, :], dst_ref=dst.at[a, dr, :],
                send_sem=hs.at[c, i], recv_sem=hr.at[c, i],
                device_id=dev(*where), device_id_type=MESH,
            )
            out.append((copy, sends, gets))
        return out

    def when(cond, fn):
        if cond is None:
            fn()
        else:
            pl.when(cond)(fn)

    def send(copies):
        for copy, sends, _ in copies:
            when(sends, copy.start)

    for c in loads[1:5]:
        c.wait()
    ex[10, W : W + 16, :] = (1 - landb[...]).astype(F32)
    ex[11:16, W : W + 16, :] = jnp.zeros((5, 16, 128), F32)
    loads[0].wait()
    pl.semaphore_wait(barrier, len(partners))
    extra = (4, ex, 0, 8)

    def pass_word(step, along_z):
        far = 2**step
        for d in (-far, far):
            pl.semaphore_signal(ysem.at[step], inc=1, device_id=along_y(d), device_id_type=MESH)
            if along_z:
                pl.semaphore_signal(zsem.at[step], inc=1, device_id=dev(d, 0), device_id_type=MESH)

    def hear_word(step, along_z):
        pl.semaphore_wait(ysem.at[step], 2)
        if along_z:
            pl.semaphore_wait(zsem.at[step], 2)

    pass_word(0, True)

    def member_chunk(c):
        return c, qx, 16 * c, 2 * c

    send(halo(*extra, True))

    def send_rows(c, carry):
        send(halo(*member_chunk(c), True))
        return carry

    lax.fori_loop(0, 4, send_rows, 0)
    pack_edges(ex, 0, (W, W + 16), 2, rv, lv, 8)

    def pack_own(c, carry):
        pack_edges(qx, 16 * c, (W, W + 16), 2, rv, lv, 2 * c)
        return carry

    lax.fori_loop(0, 4, pack_own, 0)
    send(halo(*extra, False))

    def send_edges(c, carry):
        send(halo(*member_chunk(c), False))
        return carry

    lax.fori_loop(0, 4, send_edges, 0)

    for c in loads[5:]:
        c.wait()
    same = iota((64, 64), 0) == iota((64, 64), 1)

    def across(row):
        col = jnp.sum(jnp.where(same, jnp.broadcast_to(row, (64, 64)), 0.0), axis=1, keepdims=True)
        return jnp.broadcast_to(col, (64, 128))

    tt = thl[...]
    th = jnp.tanh(tt)
    hyper = 0.005 * (1.0 + 0.5 * th[1:2])
    coefs[0] = across(1.0 - 0.05 * (1.0 + 0.5 * th[2:3]))
    coefs[1] = across(0.05 * (1.0 + 0.5 * th[0:1]) + 4.0 * hyper)
    coefs[2] = across(hyper)
    coefs[3] = across(tt[3:4])
    thx[...] = jnp.zeros((8, 128), F32)

    @pl.when(e == 0)
    def _():
        thx[0:4, 0:64] = thl[...]

    @pl.when(e == 1)
    def _():
        thx[0:4, 64:128] = thl[...]

    slot8 = iota((8, 128), 1) // 32
    for t in range(4):
        for odd in range(2):
            acc = None
            for k in range(4):
                x = coefs[t, pl.ds(odd + 2 * k, 8, stride=8), :]
                acc = x if acc is None else jnp.where(slot8 == k, x, acc)
            pcoefs[t, odd] = acc
    row32 = iota((32, 128), 0)
    no_wall = (jnp.logical_or(row32 >= W, up_ok)) & (jnp.logical_or(row32 < W + 16, down_ok))
    mask[...] = no_wall.astype(F32)


    swap_theta = pltpu.make_async_remote_copy(
        src_ref=thx, dst_ref=thr, send_sem=xs.at[0], recv_sem=xr.at[0], device_id=pair, device_id_type=MESH
    )
    swap_theta.start()

    def wait_for(copies):
        for copy, _, gets in copies:
            when(gets, copy.wait_recv)

    site = oix[...]
    col_pick = jnp.broadcast_to(site % 128, (128, 128)) == iota((128, 128), 0)
    for n in range(3):
        pick[128 * n : 128 * n + 128, :] = col_pick.astype(F32).astype(jnp.bfloat16)
    site_row = jnp.broadcast_to(site // 128, (16, 128)) == iota((16, 128), 0)
    lane = iota((16, 128), 1)
    slot16 = lane % 32 < 16
    edge = (lane < W) | (lane >= 128 - W)
    slot32 = iota((32, 128), 1) // 32

    wait_for(halo(*extra, True))
    hear_word(0, True)
    pass_word(1, True)
    o = ex[10]
    tabs[0] = o
    tabs[1] = 0.5 * ex[8] * o
    tabs[2] = 0.5 * ex[9] * o

    def chunk(c, carry):
        m0 = 16 * c
        wait_for(halo(*member_chunk(c), True))
        for p in range(16):
            fos[p] = coefs[3, pl.ds(m0 + p, 1), :] * ex[mode[m0 + p]]

        def keep(p, new):
            fin[m0 + p] = new

        advance(
            lambda p, a, n: qx[m0 + p, a : a + n, :], 16,
            [lambda p, t=t: coefs[t, pl.ds(m0 + p, 1), :] for t in range(3)],
            [lambda p, a, n, t=t: tabs[t, a : a + n, :] for t in range(3)],
            lambda p, a, n: fos[p, a : a + n, :], qs, lqs, es, mask, keep,
        )
        return carry

    lax.fori_loop(0, 4, chunk, 0)

    hear_word(1, True)
    pass_word(2, False)
    wait_for(halo(*extra, False))

    def spread(x, k):
        y = jnp.where(slot32 == k, x, 0.0)
        y = y + pltpu.roll(y, 32, 1)
        return y + pltpu.roll(y, 64, 1)

    both = strips_of(rv[8], lv[8], rvr[8], lvr[8], 0, 32)
    for side in range(2):
        for k in range(8):
            ftab[side, k] = spread(both[side][k % 2], k // 2)
    both = strips_of(rv[9], lv[9], rvr[9], lvr[9], 0, 32)
    for side in range(2):
        even, odd = both[side]
        o = spread(even, 1)
        stabs[side, 0] = o
        stabs[side, 1] = 0.5 * spread(even, 0) * o
        stabs[side, 2] = 0.5 * spread(odd, 0) * o

    def edges_here(c, carry):
        wait_for(halo(*member_chunk(c), False))
        return carry

    lax.fori_loop(0, 4, edges_here, 0)

    def strips(c, carry):
        for n in range(4):
            gr = 4 * c + n
            both = strips_of(rv[gr], lv[gr], rvr[gr], lvr[gr], 0, 32)
            for side in range(2):
                for odd in range(2):
                    p = 4 * n + 2 * side + odd
                    qp[p] = both[side][odd]
                    f = None
                    for k in range(4):
                        x = ftab[side, mode[8 * gr + 2 * k + odd]]
                        f = x if f is None else jnp.where(slot32 == k, x, f)
                    fos[p] = pcoefs[3, odd, pl.ds(gr, 1), :] * f

        def keep(p, new):
            endp[16 * c + p] = new

        advance(
            lambda p, a, n: qp[p, a : a + n, :], 16,
            [lambda p, t=t: pcoefs[t, p % 2, pl.ds(4 * c + p // 4, 1), :] for t in range(3)],
            [lambda p, a, n, t=t: stabs[(p // 2) % 2, t, a : a + n, :] for t in range(3)],
            lambda p, a, n: fos[p, a : a + n, :], qs, lqs, es, mask, keep,
        )
        return carry

    lax.fori_loop(0, 2, strips, 0)

    for c in range(4):
        for q in range(4):
            n, odd = q // 2, q % 2
            ends = jnp.where(slot16, endp[8 * c + 4 * n + 2 + odd], endp[8 * c + 4 * n + odd])
            for k in range(4):
                p = 16 * c + 8 * n + 2 * k + odd
                fin[p] = jnp.where(edge, pltpu.roll(ends, (112 - 32 * k) % 128, 1), fin[p])
    for c in range(4):
        x = fin[16 * c : 16 * c + 16].reshape(256, 128)
        part, parts = x, []
        for _ in range(3):
            parts.append(part.astype(jnp.bfloat16))
            part = part - parts[-1].astype(F32)
        at_col = jnp.dot(jnp.concatenate(parts, axis=1), pick[...], preferred_element_type=F32)
        seen = jnp.where(site_row[None], at_col.reshape(16, 16, 128), 0.0)
        oall[e, 16 * c : 16 * c + 16, :] = jnp.sum(seen, axis=1)

    swap_seen = pltpu.make_async_remote_copy(
        src_ref=oall.at[e], dst_ref=oall.at[e], send_sem=xs.at[1], recv_sem=xr.at[1],
        device_id=pair, device_id_type=MESH,
    )
    swap_seen.start()
    got_seen = pltpu.make_async_remote_copy(
        src_ref=oall.at[e], dst_ref=oall.at[1 - e], send_sem=xs.at[1], recv_sem=xr.at[1],
        device_id=pair, device_id_type=MESH,
    )
    got_seen.wait_recv()
    swap_theta.wait_recv()

    seen = jnp.concatenate([oall[0], oall[1]], axis=0)
    mean = jnp.sum(seen, axis=0, keepdims=True) * (1.0 / 128.0)
    scale = 1.0 / osg[...]
    anomaly = (seen - mean) * scale
    miss = jnp.broadcast_to((ova[...] - mean) * scale, (8, 128))
    dims = (((1,), (1,)), ((), ()))
    gram = lax.dot_general(anomaly, anomaly, dims, precision=HIGHEST, preferred_element_type=F32)
    cvec = lax.dot_general(miss, anomaly, dims, precision=HIGHEST, preferred_element_type=F32)
    last = iota((128, 128), 0) == 127
    gp[...] = jnp.where(last, cvec[0:1, :], gram).reshape(8, 16, 128)

    owner, mine = lax.rem(g, 2) == 1, g // 2

    def to(src, dst, ssem, rsem, where):
        return pltpu.make_async_remote_copy(
            src_ref=src, dst_ref=dst, send_sem=ssem, recv_sem=rsem, device_id=where, device_id_type=MESH
        )

    def rows_to_owner(d):
        j = lax.rem(mine + d, 8)
        return to(gp.at[j], rs.at[g], rss.at[d], rsr.at[g], tile_holder(2 * j + 1))

    def rows_to_gx(d):
        where = {"gx": lax.rem(z + d, nz), "gy": g, "ens": e}
        return to(zs.at[z], zs.at[z], zss.at[d], zsr.at[z], where)

    def rows_to_all(d):
        return to(ag.at[mine], ag.at[mine], ags.at[d], agr.at[mine], tile_holder(lax.rem(g + d, ng)))

    def arrived(ref, i, rsem, ssem):
        to(ref.at[i], ref.at[i], ssem, rsem.at[i], pair).wait_recv()

    hear_word(2, False)
    for d in range(1, 8):
        rows_to_owner(d).start()
    pl.when(jnp.logical_not(owner))(lambda: rows_to_owner(0).start())

    @pl.when(owner)
    def _():
        rs[g] = gp[mine]
        for d in range(1, ng):
            arrived(rs, lax.rem(g + d, ng), rsr, rss.at[0])
        zs[z] = jnp.sum(rs[...], axis=0)
        for d in range(1, nz):
            rows_to_gx(d).start()
        for d in range(1, nz):
            arrived(zs, lax.rem(z + d, nz), zsr, zss.at[0])
        ag[mine] = jnp.sum(zs[...], axis=0)
        for d in range(1, ng):
            rows_to_all(d).start()

    thetas[...] = thx[...] + thr[...]
    for d in range(1, 8):
        arrived(ag, lax.rem(mine + d, 8), agr, ags.at[0])
    pl.when(jnp.logical_not(owner))(lambda: arrived(ag, mine, agr, ags.at[0]))
    sums[...] = ag[...].reshape(16, 8, 128)

    def drain(copies):
        for copy, sends, _ in copies:
            when(sends, copy.wait_send)

    drain(halo(*extra, True))
    drain(halo(*extra, False))

    def drain_chunk(c, carry):
        drain(halo(*member_chunk(c), True))
        drain(halo(*member_chunk(c), False))
        return carry

    lax.fori_loop(0, 4, drain_chunk, 0)
    swap_theta.wait_send()
    swap_seen.wait_send()
    for d in range(1, 8):
        rows_to_owner(d).wait_send()
    pl.when(jnp.logical_not(owner))(lambda: rows_to_owner(0).wait_send())

    @pl.when(owner)
    def _():
        for d in range(1, nz):
            rows_to_gx(d).wait_send()
        for d in range(1, ng):
            rows_to_all(d).wait_send()


def solve(fin, sums, thetas, fin_out, theta_out, mat, sem):
    e = lax.axis_index("ens")
    out_copy = pltpu.make_async_copy(fin, fin_out, sem)
    out_copy.start()
    th_all = thetas[...]
    th_mean = jnp.sum(th_all, axis=1, keepdims=True) * (1.0 / 128.0)
    mat[16] = th_all - th_mean
    crow = sums[15, 7:8, :]
    sub, ln = iota((8, 128), 0), iota((8, 128), 1)
    last = sub == 7
    tiles = [sums[t] for t in range(16)]
    tiles[15] = jnp.where(last, 0.0, tiles[15])
    total = tiles[0]
    for t in range(1, 16):
        total = total + tiles[t]
    total = jnp.sum(total, axis=0, keepdims=True)
    tiles[15] = jnp.where(last, -total, tiles[15])
    for t in range(16):
        mat[t] = tiles[t] + jnp.where(ln == sub + 8 * t, 127.0, 0.0)

    def lanes_of(x, base):
        return [jnp.broadcast_to(x[:, base + j : base + j + 1], (8, 128)) for j in range(8)]

    def row_of(x, i):
        return jnp.broadcast_to(x[i : i + 1, :], (8, 128))

    cols = lanes_of(tiles[0] + jnp.where(ln == sub, 127.0, 0.0), 0)
    for k in range(16):
        base = 8 * k
        front = (ln >= base) & (ln < base + 8)
        piv = mat[k]
        ahead = lanes_of(piv, base + 8) if k < 15 else []
        row = jnp.where(front, jnp.where(ln == sub + base, 1.0, 0.0), piv)
        scale = jnp.zeros((8, 128), F32)
        for i in range(8):
            inv = 1.0 / row_of(cols[i], i)
            mine = sub == i
            step = jnp.where(mine, 0.0, cols[i]) * inv
            scale = jnp.where(mine, inv, scale)
            row = row - step * row_of(row, i)
            for j in range(i + 1, 8):
                cols[j] = cols[j] - step * row_of(cols[j], i)
            ahead = [x - step * row_of(x, i) for x in ahead]
        row = row * scale
        ahead = [x * scale for x in ahead]
        row = jnp.where(front, -row, row)
        rows = [row_of(row, i) for i in range(8)]
        for t in range(k + 1, 17):
            x = mat[t]
            by = lanes_of(x, base)
            new = jnp.where(front, 0.0, x)
            for i in range(8):
                new = new - by[i] * rows[i]
            mat[t] = new
            if t == k + 1 and k < 15:
                cols = lanes_of(x, base + 8)
                for j in range(8):
                    for i in range(8):
                        cols[j] = cols[j] - by[i] * row_of(ahead[j], i)
    zt = mat[16]
    shift = jnp.sum(zt * crow, axis=1, keepdims=True)
    fresh = th_mean + 127.0 * zt + shift
    @pl.when(e == 0)
    def _():
        theta_out[...] = fresh[0:4, 0:64]

    @pl.when(e == 1)
    def _():
        theta_out[...] = fresh[0:4, 64:128]

    out_copy.wait()


def local(state, u_vel, v_vel, land, forcing, member_mode, theta, *obs):
    args = (member_mode, state, u_vel, v_vel, land, forcing, theta, *obs)
    hbm = pl.BlockSpec(memory_space=pl.ANY)
    vmem = pl.BlockSpec(memory_space=pltpu.VMEM)
    dma, v = pltpu.SemaphoreType.DMA, lambda *s: pltpu.VMEM(s, F32)
    shape = jax.ShapeDtypeStruct
    fin, sums, thetas = pl.pallas_call(
        kernel,
        out_shape=(shape(state.shape, F32), shape((16, 8, 128), F32), shape((8, 128), F32)),
        in_specs=[pl.BlockSpec(memory_space=pltpu.HBM)] * 10,
        out_specs=(vmem, vmem, vmem),
        scratch_shapes=[
            v(64, 32, 128), v(16, 32, 128), pltpu.VMEM((16, 128), jnp.int32),
            v(10, 32, 128), v(10, 32, 128), v(10, 32, 128), v(10, 32, 128),
            v(32, 128), v(3, 32, 128), v(2, 8, 32, 128), v(2, 3, 32, 128), v(4, 64, 128), v(4, 2, 8, 128),
            v(16, 32, 128), v(16, 32, 128), v(16, 32, 128), v(16, 32, 128),
            v(16, 32, 128), v(32, 16, 128),
            v(2, 64, 128), v(8, 128), v(8, 128),
            v(8, 16, 128), v(16, 16, 128), v(8, 16, 128), v(8, 16, 128),
            pltpu.VMEM((384, 128), jnp.bfloat16), v(4, 64), pltpu.VMEM((1, 128), jnp.int32), v(1, 128), v(1, 128), pltpu.SMEM((64,), jnp.int32),
            pltpu.SemaphoreType.REGULAR((3,)), pltpu.SemaphoreType.REGULAR((2,)), dma((10,)), dma((5, 12)), dma((5, 12)), dma((2,)), dma((2,)),
            dma((8,)), dma((16,)), dma((8,)), dma((8,)), dma((16,)), dma((8,)),
        ],
        compiler_params=pltpu.CompilerParams(collective_id=0, has_side_effects=True, vmem_limit_bytes=20 * 2**20),
    )(*[pltpu.with_memory_space_constraint(a, pltpu.HBM) for a in args])
    return pl.pallas_call(
        solve,
        out_shape=(shape(state.shape, F32), shape(theta.shape, F32)),
        in_specs=[hbm, vmem, vmem],
        out_specs=(hbm, vmem),
        scratch_shapes=[v(17, 8, 128), dma(())],
        compiler_params=pltpu.CompilerParams(vmem_limit_bytes=8 * 2**20),
    )(fin, sums, thetas)


def solution(mesh):
    in_specs = (
        P("ens", "gy", "gx"), P("gy", "gx"), P("gy", "gx"), P("gy", "gx"), P(None, "gy", "gx"),
        P("ens"), P("ens", None), P("gy", "gx", None), P("gy", "gx", None), P("gy", "gx", None),
    )
    out_specs = (P("ens", "gy", "gx"), P("ens", None))

    def run(state, u_vel, v_vel, land, forcing, member_mode, theta, obs_index, obs_values, obs_sigma):
        flat = [a.reshape(a.shape[1:]) for a in (obs_index, obs_values, obs_sigma)]
        fin, new = local(state, u_vel, v_vel, land, forcing, member_mode, theta.T, *flat)
        return fin, new.T

    return jax.shard_map(run, mesh=mesh, in_specs=in_specs, out_specs=out_specs, check_vma=False)
```

```python
import jax
import jax.numpy as jnp
from jax import lax
from jax.experimental import pallas as pl
from jax.experimental.pallas import tpu as pltpu
from jax.sharding import PartitionSpec as P

STEPS = 4
W = 2 * STEPS
MESH = pl.DeviceIdType.MESH
F32 = jnp.float32
HIGHEST = lax.Precision.HIGHEST


def iota(shape, dim):
    return lax.broadcasted_iota(jnp.int32, shape, dim)


def pack_edges(ref, first, rows, count, r_ref, l_ref, group):
    lo, hi = rows
    slot = iota((hi - lo, 128), 1) // 16
    for n in range(count):
        right = left = None
        for k in range(8):
            x = ref[first + 8 * n + k, lo:hi, :]
            a = pltpu.roll(x, (16 * (k + 1)) % 128, 1) if k < 7 else x
            b = pltpu.roll(x, 16 * k, 1) if k else x
            right = a if right is None else jnp.where(slot == k, a, right)
            left = b if left is None else jnp.where(slot == k, b, left)
        r_ref[group + n, lo:hi, :] = right
        l_ref[group + n, lo:hi, :] = left


def strips_of(rv, lv, rvr, lvr, lo, hi):
    inner = iota((hi - lo, 128), 1) % 32 < 16
    left = (
        jnp.where(inner, rvr, pltpu.roll(lv, 16, 1)),
        jnp.where(inner, pltpu.roll(rvr, 112, 1), lv),
    )
    right = (
        jnp.where(inner, rv, pltpu.roll(lvr, 16, 1)),
        jnp.where(inner, pltpu.roll(rv, 112, 1), lvr),
    )
    return left, right


def advance(first, planes, coef, tables, forced, qs, lqs, es, mask, put):
    c0, c1, hy = coef
    ocean, uo, vo = tables
    for step in range(STEPS):
        lo = 2 * step
        nl = 4 * W - 2 - 4 * step
        nn = nl - 2
        for p in range(planes):
            get = (lambda a, n, p=p: first(p, a, n)) if step == 0 else (lambda a, n, p=p: qs[p, a : a + n, :])
            cen = get(lo + 1, nl)
            west = pltpu.roll(cen, 1, 1)
            east = pltpu.roll(cen, 127, 1)
            lap = (get(lo + 2, nl) + get(lo, nl)) + (west + east) - 4.0 * cen
            lqs[p, lo + 1 : lo + 1 + nl, :] = lap * mask[lo + 1 : lo + 1 + nl, :]
            es[p, lo + 1 : lo + 1 + nl, :] = east - west
        at = slice(lo + 2, lo + 2 + nn)
        for p in range(planes):
            get = (lambda a, n, p=p: first(p, a, n)) if step == 0 else (lambda a, n, p=p: qs[p, a : a + n, :])
            lap = lqs[p, at, :]
            around = (lqs[p, lo + 3 : lo + 3 + nn, :] + lqs[p, lo + 1 : lo + 1 + nn, :]) + (
                pltpu.roll(lap, 1, 1) + pltpu.roll(lap, 127, 1)
            )
            dy = get(lo + 3, nn) - get(lo + 1, nn)
            inner = c0(p) * get(lo + 2, nn) + c1(p) * lap - hy(p) * around + forced(p, lo + 2, nn)
            new = ocean(p, lo + 2, nn) * inner - (
                uo(p, lo + 2, nn) * es[p, at, :] + vo(p, lo + 2, nn) * dy
            )
            if step < STEPS - 1:
                qs[p, at, :] = new
            else:
                put(p, new)


def kernel(
    mode_in, state, u_vel, v_vel, land, forcing, theta, obs_index, obs_values, obs_sigma,
    fin, sums, thetas,
    qx, ex, landb, rv, lv, rvr, lvr, mask, tabs, ftab, stabs, coefs, pcoefs,
    qs, lqs, es, fos, qp, endp, oall, thx, thr,
    gp, rs, zs, ag,
    pick, thl, oix, ova, osg, mode, ysem, zsem, lsem, hs, hr, xs, xr, rss, rsr, zss, zsr, ags, agr,
):
    z, g, e = lax.axis_index("gx"), lax.axis_index("gy"), lax.axis_index("ens")
    nz, ng = 8, 16
    up_ok, down_ok = g > 0, g < ng - 1

    def dev(dz, dg):
        return {"gx": lax.rem(z + dz + nz, nz), "gy": lax.rem(g + dg + ng, ng), "ens": e}

    pair = {"gx": z, "gy": g, "ens": 1 - e}
    near = lax.rem(g // 8 + e, 2)

    def tile_holder(j):
        return {"gx": z, "gy": j, "ens": lax.rem(j // 8 + near, 2)}

    barrier = pltpu.get_barrier_semaphore()
    def along_y(d):
        return tile_holder(lax.rem(g + d + ng, ng))

    partners = [dev(a, b) for a in (-1, 0, 1) for b in (-1, 1)] + [dev(-1, 0), dev(1, 0), pair, along_y(-1), along_y(1)]
    for where in partners:
        pl.semaphore_signal(barrier, inc=1, device_id=where, device_id_type=MESH)

    own = pl.ds(W, 16)
    loads = [
        pltpu.make_async_copy(state, qx.at[:, own, :], lsem.at[0]),
        pltpu.make_async_copy(forcing, ex.at[0:8, own, :], lsem.at[1]),
        pltpu.make_async_copy(u_vel, ex.at[8, own, :], lsem.at[2]),
        pltpu.make_async_copy(v_vel, ex.at[9, own, :], lsem.at[3]),
        pltpu.make_async_copy(land, landb, lsem.at[4]),
        pltpu.make_async_copy(theta, thl, lsem.at[5]),
        pltpu.make_async_copy(obs_index, oix, lsem.at[6]),
        pltpu.make_async_copy(obs_values, ova, lsem.at[7]),
        pltpu.make_async_copy(obs_sigma, osg, lsem.at[8]),
        pltpu.make_async_copy(mode_in, mode, lsem.at[9]),
    ]
    for c in loads:
        c.start()

    @pl.when(jnp.logical_not(up_ok))
    def _():
        for ref in (qx, ex, rv, lv, rvr, lvr):
            ref[:, 0:W, :] = jnp.zeros((ref.shape[0], W, 128), F32)

    @pl.when(jnp.logical_not(down_ok))
    def _():
        for ref in (qx, ex, rv, lv, rvr, lvr):
            ref[:, W + 16 :, :] = jnp.zeros((ref.shape[0], W, 128), F32)

    top, bottom, low, high = pl.ds(W, W), pl.ds(16, W), pl.ds(0, W), pl.ds(W + 16, W)

    def halo(c, planes, first, group, rows):
        at, ga = pl.ds(first, 16 if planes is qx else 11), pl.ds(group, 2)
        plan = [
            (planes, at, top, planes, high, (0, -1), up_ok, down_ok),
            (planes, at, bottom, planes, low, (0, 1), down_ok, up_ok),
            (rv, ga, own, rvr, own, (1, 0), None, None),
            (lv, ga, own, lvr, own, (-1, 0), None, None),
            (rv, ga, bottom, rvr, low, (1, 1), down_ok, up_ok),
            (rv, ga, top, rvr, high, (1, -1), up_ok, down_ok),
            (lv, ga, bottom, lvr, low, (-1, 1), down_ok, up_ok),
            (lv, ga, top, lvr, high, (-1, -1), up_ok, down_ok),
            (rv, ga, top, rv, high, (0, -1), up_ok, down_ok),
            (rv, ga, bottom, rv, low, (0, 1), down_ok, up_ok),
            (lv, ga, top, lv, high, (0, -1), up_ok, down_ok),
            (lv, ga, bottom, lv, low, (0, 1), down_ok, up_ok),
        ]
        out = []
        for i in range(2) if rows else range(2, 12):
            src, a, sr, dst, dr, where, sends, gets = plan[i]
            copy = pltpu.make_async_remote_copy(
                src_ref=src.at[a, sr, :], dst_ref=dst.at[a, dr, :],
                send_sem=hs.at[c, i], recv_sem=hr.at[c, i],
                device_id=dev(*where), device_id_type=MESH,
            )
            out.append((copy, sends, gets))
        return out

    def when(cond, fn):
        if cond is None:
            fn()
        else:
            pl.when(cond)(fn)

    def send(copies):
        for copy, sends, _ in copies:
            when(sends, copy.start)

    for c in loads[1:5]:
        c.wait()
    ex[10, W : W + 16, :] = (1 - landb[...]).astype(F32)
    ex[11:16, W : W + 16, :] = jnp.zeros((5, 16, 128), F32)
    loads[0].wait()
    pl.semaphore_wait(barrier, len(partners))
    extra = (4, ex, 0, 8)

    def pass_word(step, along_z):
        far = 2**step
        for d in (-far, far):
            pl.semaphore_signal(ysem.at[step], inc=1, device_id=along_y(d), device_id_type=MESH)
            if along_z:
                pl.semaphore_signal(zsem.at[step], inc=1, device_id=dev(d, 0), device_id_type=MESH)

    def hear_word(step, along_z):
        pl.semaphore_wait(ysem.at[step], 2)
        if along_z:
            pl.semaphore_wait(zsem.at[step], 2)

    pass_word(0, True)

    def member_chunk(c):
        return c, qx, 16 * c, 2 * c

    send(halo(*extra, True))

    def send_rows(c, carry):
        send(halo(*member_chunk(c), True))
        return carry

    lax.fori_loop(0, 4, send_rows, 0)
    pack_edges(ex, 0, (W, W + 16), 2, rv, lv, 8)

    def pack_own(c, carry):
        pack_edges(qx, 16 * c, (W, W + 16), 2, rv, lv, 2 * c)
        return carry

    lax.fori_loop(0, 4, pack_own, 0)
    send(halo(*extra, False))

    def send_edges(c, carry):
        send(halo(*member_chunk(c), False))
        return carry

    lax.fori_loop(0, 4, send_edges, 0)

    for c in loads[5:]:
        c.wait()
    same = iota((64, 64), 0) == iota((64, 64), 1)

    def across(row):
        col = jnp.sum(jnp.where(same, jnp.broadcast_to(row, (64, 64)), 0.0), axis=1, keepdims=True)
        return jnp.broadcast_to(col, (64, 128))

    tt = thl[...]
    th = jnp.tanh(tt)
    hyper = 0.005 * (1.0 + 0.5 * th[1:2])
    coefs[0] = across(1.0 - 0.05 * (1.0 + 0.5 * th[2:3]))
    coefs[1] = across(0.05 * (1.0 + 0.5 * th[0:1]) + 4.0 * hyper)
    coefs[2] = across(hyper)
    coefs[3] = across(tt[3:4])
    thx[...] = jnp.zeros((8, 128), F32)

    @pl.when(e == 0)
    def _():
        thx[0:4, 0:64] = thl[...]

    @pl.when(e == 1)
    def _():
        thx[0:4, 64:128] = thl[...]

    slot8 = iota((8, 128), 1) // 32
    for t in range(4):
        for odd in range(2):
            acc = None
            for k in range(4):
                x = coefs[t, pl.ds(odd + 2 * k, 8, stride=8), :]
                acc = x if acc is None else jnp.where(slot8 == k, x, acc)
            pcoefs[t, odd] = acc
    row32 = iota((32, 128), 0)
    no_wall = (jnp.logical_or(row32 >= W, up_ok)) & (jnp.logical_or(row32 < W + 16, down_ok))
    mask[...] = no_wall.astype(F32)


    swap_theta = pltpu.make_async_remote_copy(
        src_ref=thx, dst_ref=thr, send_sem=xs.at[0], recv_sem=xr.at[0], device_id=pair, device_id_type=MESH
    )
    swap_theta.start()

    def wait_for(copies):
        for copy, _, gets in copies:
            when(gets, copy.wait_recv)

    site = oix[...]
    col_pick = jnp.broadcast_to(site % 128, (128, 128)) == iota((128, 128), 0)
    for n in range(3):
        pick[128 * n : 128 * n + 128, :] = col_pick.astype(F32).astype(jnp.bfloat16)
    site_row = jnp.broadcast_to(site // 128, (16, 128)) == iota((16, 128), 0)
    lane = iota((16, 128), 1)
    slot16 = lane % 32 < 16
    edge = (lane < W) | (lane >= 128 - W)
    slot32 = iota((32, 128), 1) // 32

    wait_for(halo(*extra, True))
    hear_word(0, True)
    pass_word(1, True)
    o = ex[10]
    tabs[0] = o
    tabs[1] = 0.5 * ex[8] * o
    tabs[2] = 0.5 * ex[9] * o

    def chunk(c, carry):
        m0 = 16 * c
        wait_for(halo(*member_chunk(c), True))
        for p in range(16):
            fos[p] = coefs[3, pl.ds(m0 + p, 1), :] * ex[mode[m0 + p]]

        def keep(p, new):
            fin[m0 + p] = new

        advance(
            lambda p, a, n: qx[m0 + p, a : a + n, :], 16,
            [lambda p, t=t: coefs[t, pl.ds(m0 + p, 1), :] for t in range(3)],
            [lambda p, a, n, t=t: tabs[t, a : a + n, :] for t in range(3)],
            lambda p, a, n: fos[p, a : a + n, :], qs, lqs, es, mask, keep,
        )
        return carry

    lax.fori_loop(0, 4, chunk, 0)

    hear_word(1, True)
    pass_word(2, False)
    wait_for(halo(*extra, False))

    def spread(x, k):
        y = jnp.where(slot32 == k, x, 0.0)
        y = y + pltpu.roll(y, 32, 1)
        return y + pltpu.roll(y, 64, 1)

    both = strips_of(rv[8], lv[8], rvr[8], lvr[8], 0, 32)
    for side in range(2):
        for k in range(8):
            ftab[side, k] = spread(both[side][k % 2], k // 2)
    both = strips_of(rv[9], lv[9], rvr[9], lvr[9], 0, 32)
    for side in range(2):
        even, odd = both[side]
        o = spread(even, 1)
        stabs[side, 0] = o
        stabs[side, 1] = 0.5 * spread(even, 0) * o
        stabs[side, 2] = 0.5 * spread(odd, 0) * o

    def edges_here(c, carry):
        wait_for(halo(*member_chunk(c), False))
        return carry

    lax.fori_loop(0, 4, edges_here, 0)

    def strips(c, carry):
        for n in range(4):
            gr = 4 * c + n
            both = strips_of(rv[gr], lv[gr], rvr[gr], lvr[gr], 0, 32)
            for side in range(2):
                for odd in range(2):
                    p = 4 * n + 2 * side + odd
                    qp[p] = both[side][odd]
                    f = None
                    for k in range(4):
                        x = ftab[side, mode[8 * gr + 2 * k + odd]]
                        f = x if f is None else jnp.where(slot32 == k, x, f)
                    fos[p] = pcoefs[3, odd, pl.ds(gr, 1), :] * f

        def keep(p, new):
            endp[16 * c + p] = new

        advance(
            lambda p, a, n: qp[p, a : a + n, :], 16,
            [lambda p, t=t: pcoefs[t, p % 2, pl.ds(4 * c + p // 4, 1), :] for t in range(3)],
            [lambda p, a, n, t=t: stabs[(p // 2) % 2, t, a : a + n, :] for t in range(3)],
            lambda p, a, n: fos[p, a : a + n, :], qs, lqs, es, mask, keep,
        )
        return carry

    lax.fori_loop(0, 2, strips, 0)

    for c in range(4):
        for q in range(4):
            n, odd = q // 2, q % 2
            ends = jnp.where(slot16, endp[8 * c + 4 * n + 2 + odd], endp[8 * c + 4 * n + odd])
            for k in range(4):
                p = 16 * c + 8 * n + 2 * k + odd
                fin[p] = jnp.where(edge, pltpu.roll(ends, (112 - 32 * k) % 128, 1), fin[p])
    for c in range(4):
        x = fin[16 * c : 16 * c + 16].reshape(256, 128)
        part, parts = x, []
        for _ in range(3):
            parts.append(part.astype(jnp.bfloat16))
            part = part - parts[-1].astype(F32)
        at_col = jnp.dot(jnp.concatenate(parts, axis=1), pick[...], preferred_element_type=F32)
        seen = jnp.where(site_row[None], at_col.reshape(16, 16, 128), 0.0)
        oall[e, 16 * c : 16 * c + 16, :] = jnp.sum(seen, axis=1)

    swap_seen = pltpu.make_async_remote_copy(
        src_ref=oall.at[e], dst_ref=oall.at[e], send_sem=xs.at[1], recv_sem=xr.at[1],
        device_id=pair, device_id_type=MESH,
    )
    swap_seen.start()
    got_seen = pltpu.make_async_remote_copy(
        src_ref=oall.at[e], dst_ref=oall.at[1 - e], send_sem=xs.at[1], recv_sem=xr.at[1],
        device_id=pair, device_id_type=MESH,
    )
    got_seen.wait_recv()
    swap_theta.wait_recv()

    seen = jnp.concatenate([oall[0], oall[1]], axis=0)
    mean = jnp.sum(seen, axis=0, keepdims=True) * (1.0 / 128.0)
    scale = 1.0 / osg[...]
    anomaly = (seen - mean) * scale
    miss = jnp.broadcast_to((ova[...] - mean) * scale, (8, 128))
    dims = (((1,), (1,)), ((), ()))
    gram = lax.dot_general(anomaly, anomaly, dims, precision=HIGHEST, preferred_element_type=F32)
    cvec = lax.dot_general(miss, anomaly, dims, precision=HIGHEST, preferred_element_type=F32)
    last = iota((128, 128), 0) == 127
    gp[...] = jnp.where(last, cvec[0:1, :], gram).reshape(8, 16, 128)

    owner, mine = lax.rem(g, 2) == 1, g // 2

    def to(src, dst, ssem, rsem, where):
        return pltpu.make_async_remote_copy(
            src_ref=src, dst_ref=dst, send_sem=ssem, recv_sem=rsem, device_id=where, device_id_type=MESH
        )

    def rows_to_owner(d):
        j = lax.rem(mine + d, 8)
        return to(gp.at[j], rs.at[g], rss.at[d], rsr.at[g], tile_holder(2 * j + 1))

    def rows_to_gx(d):
        where = {"gx": lax.rem(z + d, nz), "gy": g, "ens": e}
        return to(zs.at[z], zs.at[z], zss.at[d], zsr.at[z], where)

    def rows_to_all(d):
        return to(ag.at[mine], ag.at[mine], ags.at[d], agr.at[mine], tile_holder(lax.rem(g + d, ng)))

    def arrived(ref, i, rsem, ssem):
        to(ref.at[i], ref.at[i], ssem, rsem.at[i], pair).wait_recv()

    hear_word(2, False)
    for d in range(1, 8):
        rows_to_owner(d).start()
    pl.when(jnp.logical_not(owner))(lambda: rows_to_owner(0).start())

    @pl.when(owner)
    def _():
        rs[g] = gp[mine]
        for d in range(1, ng):
            arrived(rs, lax.rem(g + d, ng), rsr, rss.at[0])
        zs[z] = jnp.sum(rs[...], axis=0)
        for d in range(1, nz):
            rows_to_gx(d).start()
        for d in range(1, nz):
            arrived(zs, lax.rem(z + d, nz), zsr, zss.at[0])
        ag[mine] = jnp.sum(zs[...], axis=0)
        for d in range(1, ng):
            rows_to_all(d).start()

    thetas[...] = thx[...] + thr[...]
    def drain(copies):
        for copy, sends, _ in copies:
            when(sends, copy.wait_send)

    drain(halo(*extra, True))
    drain(halo(*extra, False))

    def drain_chunk(c, carry):
        drain(halo(*member_chunk(c), True))
        drain(halo(*member_chunk(c), False))
        return carry

    lax.fori_loop(0, 4, drain_chunk, 0)
    swap_theta.wait_send()
    swap_seen.wait_send()
    for d in range(1, 8):
        rows_to_owner(d).wait_send()
    pl.when(jnp.logical_not(owner))(lambda: rows_to_owner(0).wait_send())

    @pl.when(owner)
    def _():
        for d in range(1, nz):
            rows_to_gx(d).wait_send()

    for d in range(1, 8):
        arrived(ag, lax.rem(mine + d, 8), agr, ags.at[0])
    pl.when(jnp.logical_not(owner))(lambda: arrived(ag, mine, agr, ags.at[0]))
    sums[...] = ag[...].reshape(16, 8, 128)

    @pl.when(owner)
    def _():
        for d in range(1, ng):
            rows_to_all(d).wait_send()


def solve(fin, sums, thetas, fin_out, theta_out, mat, sem):
    e = lax.axis_index("ens")
    out_copy = pltpu.make_async_copy(fin, fin_out, sem)
    out_copy.start()
    th_all = thetas[...]
    th_mean = jnp.sum(th_all, axis=1, keepdims=True) * (1.0 / 128.0)
    mat[16] = th_all - th_mean
    crow = sums[15, 7:8, :]
    sub, ln = iota((8, 128), 0), iota((8, 128), 1)
    last = sub == 7
    tiles = [sums[t] for t in range(16)]
    tiles[15] = jnp.where(last, 0.0, tiles[15])
    total = tiles[0]
    for t in range(1, 16):
        total = total + tiles[t]
    total = jnp.sum(total, axis=0, keepdims=True)
    tiles[15] = jnp.where(last, -total, tiles[15])
    for t in range(16):
        mat[t] = tiles[t] + jnp.where(ln == sub + 8 * t, 127.0, 0.0)

    def lanes_of(x, base):
        return [jnp.broadcast_to(x[:, base + j : base + j + 1], (8, 128)) for j in range(8)]

    def row_of(x, i):
        return jnp.broadcast_to(x[i : i + 1, :], (8, 128))

    cols = lanes_of(tiles[0] + jnp.where(ln == sub, 127.0, 0.0), 0)
    for k in range(16):
        base = 8 * k
        front = (ln >= base) & (ln < base + 8)
        piv = mat[k]
        ahead = lanes_of(piv, base + 8) if k < 15 else []
        row = jnp.where(front, jnp.where(ln == sub + base, 1.0, 0.0), piv)
        scale = jnp.zeros((8, 128), F32)
        for i in range(8):
            inv = 1.0 / row_of(cols[i], i)
            mine = sub == i
            step = jnp.where(mine, 0.0, cols[i]) * inv
            scale = jnp.where(mine, inv, scale)
            row = row - step * row_of(row, i)
            for j in range(i + 1, 8):
                cols[j] = cols[j] - step * row_of(cols[j], i)
            ahead = [x - step * row_of(x, i) for x in ahead]
        row = row * scale
        ahead = [x * scale for x in ahead]
        row = jnp.where(front, -row, row)
        rows = [row_of(row, i) for i in range(8)]
        for t in range(k + 1, 17):
            x = mat[t]
            by = lanes_of(x, base)
            new = jnp.where(front, 0.0, x)
            for i in range(8):
                new = new - by[i] * rows[i]
            mat[t] = new
            if t == k + 1 and k < 15:
                cols = lanes_of(x, base + 8)
                for j in range(8):
                    for i in range(8):
                        cols[j] = cols[j] - by[i] * row_of(ahead[j], i)
    zt = mat[16]
    shift = jnp.sum(zt * crow, axis=1, keepdims=True)
    fresh = th_mean + 127.0 * zt + shift
    @pl.when(e == 0)
    def _():
        theta_out[...] = fresh[0:4, 0:64]

    @pl.when(e == 1)
    def _():
        theta_out[...] = fresh[0:4, 64:128]

    out_copy.wait()


def local(state, u_vel, v_vel, land, forcing, member_mode, theta, *obs):
    args = (member_mode, state, u_vel, v_vel, land, forcing, theta, *obs)
    hbm = pl.BlockSpec(memory_space=pl.ANY)
    vmem = pl.BlockSpec(memory_space=pltpu.VMEM)
    dma, v = pltpu.SemaphoreType.DMA, lambda *s: pltpu.VMEM(s, F32)
    shape = jax.ShapeDtypeStruct
    fin, sums, thetas = pl.pallas_call(
        kernel,
        out_shape=(shape(state.shape, F32), shape((16, 8, 128), F32), shape((8, 128), F32)),
        in_specs=[pl.BlockSpec(memory_space=pltpu.HBM)] * 10,
        out_specs=(vmem, vmem, vmem),
        scratch_shapes=[
            v(64, 32, 128), v(16, 32, 128), pltpu.VMEM((16, 128), jnp.int32),
            v(10, 32, 128), v(10, 32, 128), v(10, 32, 128), v(10, 32, 128),
            v(32, 128), v(3, 32, 128), v(2, 8, 32, 128), v(2, 3, 32, 128), v(4, 64, 128), v(4, 2, 8, 128),
            v(16, 32, 128), v(16, 32, 128), v(16, 32, 128), v(16, 32, 128),
            v(16, 32, 128), v(32, 16, 128),
            v(2, 64, 128), v(8, 128), v(8, 128),
            v(8, 16, 128), v(16, 16, 128), v(8, 16, 128), v(8, 16, 128),
            pltpu.VMEM((384, 128), jnp.bfloat16), v(4, 64), pltpu.VMEM((1, 128), jnp.int32), v(1, 128), v(1, 128), pltpu.SMEM((64,), jnp.int32),
            pltpu.SemaphoreType.REGULAR((3,)), pltpu.SemaphoreType.REGULAR((2,)), dma((10,)), dma((5, 12)), dma((5, 12)), dma((2,)), dma((2,)),
            dma((8,)), dma((16,)), dma((8,)), dma((8,)), dma((16,)), dma((8,)),
        ],
        compiler_params=pltpu.CompilerParams(collective_id=0, has_side_effects=True, vmem_limit_bytes=20 * 2**20),
    )(*[pltpu.with_memory_space_constraint(a, pltpu.HBM) for a in args])
    return pl.pallas_call(
        solve,
        out_shape=(shape(state.shape, F32), shape(theta.shape, F32)),
        in_specs=[hbm, vmem, vmem],
        out_specs=(hbm, vmem),
        scratch_shapes=[v(17, 8, 128), dma(())],
        compiler_params=pltpu.CompilerParams(vmem_limit_bytes=8 * 2**20),
    )(fin, sums, thetas)


def solution(mesh):
    in_specs = (
        P("ens", "gy", "gx"), P("gy", "gx"), P("gy", "gx"), P("gy", "gx"), P(None, "gy", "gx"),
        P("ens"), P("ens", None), P("gy", "gx", None), P("gy", "gx", None), P("gy", "gx", None),
    )
    out_specs = (P("ens", "gy", "gx"), P("ens", None))

    def run(state, u_vel, v_vel, land, forcing, member_mode, theta, obs_index, obs_values, obs_sigma):
        flat = [a.reshape(a.shape[1:]) for a in (obs_index, obs_values, obs_sigma)]
        fin, new = local(state, u_vel, v_vel, land, forcing, member_mode, theta.T, *flat)
        return fin, new.T

    return jax.shard_map(run, mesh=mesh, in_specs=in_specs, out_specs=out_specs, check_vma=False)
```

```python
import jax
import jax.numpy as jnp
from jax import lax
from jax.experimental import pallas as pl
from jax.experimental.pallas import tpu as pltpu
from jax.sharding import PartitionSpec as P

STEPS = 4
W = 2 * STEPS
MESH = pl.DeviceIdType.MESH
F32 = jnp.float32
HIGHEST = lax.Precision.HIGHEST


def iota(shape, dim):
    return lax.broadcasted_iota(jnp.int32, shape, dim)


def pack_edges(ref, first, rows, count, r_ref, l_ref, group):
    lo, hi = rows
    slot = iota((hi - lo, 128), 1) // 16
    for n in range(count):
        right = left = None
        for k in range(8):
            x = ref[first + 8 * n + k, lo:hi, :]
            a = pltpu.roll(x, (16 * (k + 1)) % 128, 1) if k < 7 else x
            b = pltpu.roll(x, 16 * k, 1) if k else x
            right = a if right is None else jnp.where(slot == k, a, right)
            left = b if left is None else jnp.where(slot == k, b, left)
        r_ref[group + n, lo:hi, :] = right
        l_ref[group + n, lo:hi, :] = left


def strips_of(rv, lv, rvr, lvr, lo, hi):
    inner = iota((hi - lo, 128), 1) % 32 < 16
    left = (
        jnp.where(inner, rvr, pltpu.roll(lv, 16, 1)),
        jnp.where(inner, pltpu.roll(rvr, 112, 1), lv),
    )
    right = (
        jnp.where(inner, rv, pltpu.roll(lvr, 16, 1)),
        jnp.where(inner, pltpu.roll(rv, 112, 1), lvr),
    )
    return left, right


def advance(first, planes, coef, tables, forced, qs, lqs, es, mask, put):
    c0, c1, hy = coef
    ocean, uo, vo = tables
    for step in range(STEPS):
        lo = 2 * step
        nl = 4 * W - 2 - 4 * step
        nn = nl - 2
        for p in range(planes):
            get = (lambda a, n, p=p: first(p, a, n)) if step == 0 else (lambda a, n, p=p: qs[p, a : a + n, :])
            cen = get(lo + 1, nl)
            west = pltpu.roll(cen, 1, 1)
            east = pltpu.roll(cen, 127, 1)
            lap = (get(lo + 2, nl) + get(lo, nl)) + (west + east) - 4.0 * cen
            lqs[p, lo + 1 : lo + 1 + nl, :] = lap * mask[lo + 1 : lo + 1 + nl, :]
            es[p, lo + 1 : lo + 1 + nl, :] = east - west
        at = slice(lo + 2, lo + 2 + nn)
        for p in range(planes):
            get = (lambda a, n, p=p: first(p, a, n)) if step == 0 else (lambda a, n, p=p: qs[p, a : a + n, :])
            lap = lqs[p, at, :]
            around = (lqs[p, lo + 3 : lo + 3 + nn, :] + lqs[p, lo + 1 : lo + 1 + nn, :]) + (
                pltpu.roll(lap, 1, 1) + pltpu.roll(lap, 127, 1)
            )
            dy = get(lo + 3, nn) - get(lo + 1, nn)
            inner = c0(p) * get(lo + 2, nn) + c1(p) * lap - hy(p) * around + forced(p, lo + 2, nn)
            new = ocean(p, lo + 2, nn) * inner - (
                uo(p, lo + 2, nn) * es[p, at, :] + vo(p, lo + 2, nn) * dy
            )
            if step < STEPS - 1:
                qs[p, at, :] = new
            else:
                put(p, new)


def kernel(
    mode_in, state, u_vel, v_vel, land, forcing, theta, obs_index, obs_values, obs_sigma,
    fin, sums, thetas,
    qx, ex, landb, rv, lv, rvr, lvr, mask, tabs, ftab, stabs, coefs, pcoefs,
    qs, lqs, es, fos, qp, endp, oall, thx, thr,
    gp, rs, zs, ag,
    pick, thl, oix, ova, osg, mode, ysem, zsem, lsem, hs, hr, xs, xr, rss, rsr, zss, zsr, ags, agr,
):
    z, g, e = lax.axis_index("gx"), lax.axis_index("gy"), lax.axis_index("ens")
    nz, ng = 8, 16
    up_ok, down_ok = g > 0, g < ng - 1

    def dev(dz, dg):
        return {"gx": lax.rem(z + dz + nz, nz), "gy": lax.rem(g + dg + ng, ng), "ens": e}

    pair = {"gx": z, "gy": g, "ens": 1 - e}
    near = lax.rem(g // 8 + e, 2)

    def tile_holder(j):
        return {"gx": z, "gy": j, "ens": lax.rem(j // 8 + near, 2)}

    barrier = pltpu.get_barrier_semaphore()
    def along_y(d):
        return tile_holder(lax.rem(g + d + ng, ng))

    partners = [dev(a, b) for a in (-1, 0, 1) for b in (-1, 1)] + [dev(-1, 0), dev(1, 0), pair, along_y(-1), along_y(1)]
    for where in partners:
        pl.semaphore_signal(barrier, inc=1, device_id=where, device_id_type=MESH)

    own = pl.ds(W, 16)
    loads = [
        pltpu.make_async_copy(state, qx.at[:, own, :], lsem.at[0]),
        pltpu.make_async_copy(forcing, ex.at[0:8, own, :], lsem.at[1]),
        pltpu.make_async_copy(u_vel, ex.at[8, own, :], lsem.at[2]),
        pltpu.make_async_copy(v_vel, ex.at[9, own, :], lsem.at[3]),
        pltpu.make_async_copy(land, landb, lsem.at[4]),
        pltpu.make_async_copy(theta, thl, lsem.at[5]),
        pltpu.make_async_copy(obs_index, oix, lsem.at[6]),
        pltpu.make_async_copy(obs_values, ova, lsem.at[7]),
        pltpu.make_async_copy(obs_sigma, osg, lsem.at[8]),
        pltpu.make_async_copy(mode_in, mode, lsem.at[9]),
    ]
    for c in loads:
        c.start()

    @pl.when(jnp.logical_not(up_ok))
    def _():
        for ref in (qx, ex, rv, lv, rvr, lvr):
            ref[:, 0:W, :] = jnp.zeros((ref.shape[0], W, 128), F32)

    @pl.when(jnp.logical_not(down_ok))
    def _():
        for ref in (qx, ex, rv, lv, rvr, lvr):
            ref[:, W + 16 :, :] = jnp.zeros((ref.shape[0], W, 128), F32)

    top, bottom, low, high = pl.ds(W, W), pl.ds(16, W), pl.ds(0, W), pl.ds(W + 16, W)

    def halo(c, planes, first, group, rows):
        at, ga = pl.ds(first, 16 if planes is qx else 11), pl.ds(group, 2)
        plan = [
            (planes, at, top, planes, high, (0, -1), up_ok, down_ok),
            (planes, at, bottom, planes, low, (0, 1), down_ok, up_ok),
            (rv, ga, own, rvr, own, (1, 0), None, None),
            (lv, ga, own, lvr, own, (-1, 0), None, None),
            (rv, ga, bottom, rvr, low, (1, 1), down_ok, up_ok),
            (rv, ga, top, rvr, high, (1, -1), up_ok, down_ok),
            (lv, ga, bottom, lvr, low, (-1, 1), down_ok, up_ok),
            (lv, ga, top, lvr, high, (-1, -1), up_ok, down_ok),
            (rv, ga, top, rv, high, (0, -1), up_ok, down_ok),
            (rv, ga, bottom, rv, low, (0, 1), down_ok, up_ok),
            (lv, ga, top, lv, high, (0, -1), up_ok, down_ok),
            (lv, ga, bottom, lv, low, (0, 1), down_ok, up_ok),
        ]
        out = []
        for i in range(2) if rows else range(2, 12):
            src, a, sr, dst, dr, where, sends, gets = plan[i]
            copy = pltpu.make_async_remote_copy(
                src_ref=src.at[a, sr, :], dst_ref=dst.at[a, dr, :],
                send_sem=hs.at[c, i], recv_sem=hr.at[c, i],
                device_id=dev(*where), device_id_type=MESH,
            )
            out.append((copy, sends, gets))
        return out

    def when(cond, fn):
        if cond is None:
            fn()
        else:
            pl.when(cond)(fn)

    def send(copies):
        for copy, sends, _ in copies:
            when(sends, copy.start)

    for c in loads[1:5]:
        c.wait()
    ex[10, W : W + 16, :] = (1 - landb[...]).astype(F32)
    ex[11:16, W : W + 16, :] = jnp.zeros((5, 16, 128), F32)
    loads[0].wait()
    pl.semaphore_wait(barrier, len(partners))
    extra = (4, ex, 0, 8)

    def pass_word(step, along_z):
        far = 2**step
        for d in (-far, far):
            pl.semaphore_signal(ysem.at[step], inc=1, device_id=along_y(d), device_id_type=MESH)
            if along_z:
                pl.semaphore_signal(zsem.at[step], inc=1, device_id=dev(d, 0), device_id_type=MESH)

    def hear_word(step, along_z):
        pl.semaphore_wait(ysem.at[step], 2)
        if along_z:
            pl.semaphore_wait(zsem.at[step], 2)

    pass_word(0, True)

    def member_chunk(c):
        return c, qx, 16 * c, 2 * c

    send(halo(*extra, True))

    def send_rows(c, carry):
        send(halo(*member_chunk(c), True))
        return carry

    lax.fori_loop(0, 4, send_rows, 0)
    pack_edges(ex, 0, (W, W + 16), 2, rv, lv, 8)

    def pack_own(c, carry):
        pack_edges(qx, 16 * c, (W, W + 16), 2, rv, lv, 2 * c)
        return carry

    lax.fori_loop(0, 4, pack_own, 0)
    send(halo(*extra, False))

    def send_edges(c, carry):
        send(halo(*member_chunk(c), False))
        return carry

    lax.fori_loop(0, 4, send_edges, 0)

    for c in loads[5:]:
        c.wait()
    same = iota((64, 64), 0) == iota((64, 64), 1)

    def across(row):
        col = jnp.sum(jnp.where(same, jnp.broadcast_to(row, (64, 64)), 0.0), axis=1, keepdims=True)
        return jnp.broadcast_to(col, (64, 128))

    tt = thl[...]
    th = jnp.tanh(tt)
    hyper = 0.005 * (1.0 + 0.5 * th[1:2])
    coefs[0] = across(1.0 - 0.05 * (1.0 + 0.5 * th[2:3]))
    coefs[1] = across(0.05 * (1.0 + 0.5 * th[0:1]) + 4.0 * hyper)
    coefs[2] = across(hyper)
    coefs[3] = across(tt[3:4])
    thx[...] = jnp.zeros((8, 128), F32)

    @pl.when(e == 0)
    def _():
        thx[0:4, 0:64] = thl[...]

    @pl.when(e == 1)
    def _():
        thx[0:4, 64:128] = thl[...]

    slot8 = iota((8, 128), 1) // 32
    for t in range(4):
        for odd in range(2):
            acc = None
            for k in range(4):
                x = coefs[t, pl.ds(odd + 2 * k, 8, stride=8), :]
                acc = x if acc is None else jnp.where(slot8 == k, x, acc)
            pcoefs[t, odd] = acc
    row32 = iota((32, 128), 0)
    no_wall = (jnp.logical_or(row32 >= W, up_ok)) & (jnp.logical_or(row32 < W + 16, down_ok))
    mask[...] = no_wall.astype(F32)


    swap_theta = pltpu.make_async_remote_copy(
        src_ref=thx, dst_ref=thr, send_sem=xs.at[0], recv_sem=xr.at[0], device_id=pair, device_id_type=MESH
    )
    swap_theta.start()

    def wait_for(copies):
        for copy, _, gets in copies:
            when(gets, copy.wait_recv)

    site = oix[...]
    col_pick = jnp.broadcast_to(site % 128, (128, 128)) == iota((128, 128), 0)
    for n in range(3):
        pick[128 * n : 128 * n + 128, :] = col_pick.astype(F32).astype(jnp.bfloat16)
    site_row = jnp.broadcast_to(site // 128, (16, 128)) == iota((16, 128), 0)
    lane = iota((16, 128), 1)
    slot16 = lane % 32 < 16
    edge = (lane < W) | (lane >= 128 - W)
    slot32 = iota((32, 128), 1) // 32

    wait_for(halo(*extra, True))
    hear_word(0, True)
    pass_word(1, True)
    o = ex[10]
    tabs[0] = o
    tabs[1] = 0.5 * ex[8] * o
    tabs[2] = 0.5 * ex[9] * o

    def chunk(c, carry):
        m0 = 16 * c
        wait_for(halo(*member_chunk(c), True))
        for p in range(16):
            fos[p] = coefs[3, pl.ds(m0 + p, 1), :] * ex[mode[m0 + p]]

        def keep(p, new):
            fin[m0 + p] = new

        advance(
            lambda p, a, n: qx[m0 + p, a : a + n, :], 16,
            [lambda p, t=t: coefs[t, pl.ds(m0 + p, 1), :] for t in range(3)],
            [lambda p, a, n, t=t: tabs[t, a : a + n, :] for t in range(3)],
            lambda p, a, n: fos[p, a : a + n, :], qs, lqs, es, mask, keep,
        )
        return carry

    lax.fori_loop(0, 4, chunk, 0)

    hear_word(1, True)
    pass_word(2, False)
    wait_for(halo(*extra, False))

    def spread(x, k):
        y = jnp.where(slot32 == k, x, 0.0)
        y = y + pltpu.roll(y, 32, 1)
        return y + pltpu.roll(y, 64, 1)

    both = strips_of(rv[8], lv[8], rvr[8], lvr[8], 0, 32)
    for side in range(2):
        for k in range(8):
            ftab[side, k] = spread(both[side][k % 2], k // 2)
    both = strips_of(rv[9], lv[9], rvr[9], lvr[9], 0, 32)
    for side in range(2):
        even, odd = both[side]
        o = spread(even, 1)
        stabs[side, 0] = o
        stabs[side, 1] = 0.5 * spread(even, 0) * o
        stabs[side, 2] = 0.5 * spread(odd, 0) * o

    def edges_here(c, carry):
        wait_for(halo(*member_chunk(c), False))
        return carry

    lax.fori_loop(0, 4, edges_here, 0)

    def strips(c, carry):
        for n in range(8):
            gr = 8 * c + n
            both = strips_of(rv[gr], lv[gr], rvr[gr], lvr[gr], 0, 32)
            for side in range(2):
                for odd in range(2):
                    p = 4 * n + 2 * side + odd
                    qp[p] = both[side][odd]
                    f = None
                    for k in range(4):
                        x = ftab[side, mode[8 * gr + 2 * k + odd]]
                        f = x if f is None else jnp.where(slot32 == k, x, f)
                    fos[p] = pcoefs[3, odd, pl.ds(gr, 1), :] * f

        def keep(p, new):
            endp[32 * c + p] = new

        advance(
            lambda p, a, n: qp[p, a : a + n, :], 32,
            [lambda p, t=t: pcoefs[t, p % 2, pl.ds(8 * c + p // 4, 1), :] for t in range(3)],
            [lambda p, a, n, t=t: stabs[(p // 2) % 2, t, a : a + n, :] for t in range(3)],
            lambda p, a, n: fos[p, a : a + n, :], qs, lqs, es, mask, keep,
        )
        return carry

    strips(0, 0)

    for c in range(4):
        for q in range(4):
            n, odd = q // 2, q % 2
            ends = jnp.where(slot16, endp[8 * c + 4 * n + 2 + odd], endp[8 * c + 4 * n + odd])
            for k in range(4):
                p = 16 * c + 8 * n + 2 * k + odd
                fin[p] = jnp.where(edge, pltpu.roll(ends, (112 - 32 * k) % 128, 1), fin[p])
    for c in range(4):
        x = fin[16 * c : 16 * c + 16].reshape(256, 128)
        part, parts = x, []
        for _ in range(3):
            parts.append(part.astype(jnp.bfloat16))
            part = part - parts[-1].astype(F32)
        at_col = jnp.dot(jnp.concatenate(parts, axis=1), pick[...], preferred_element_type=F32)
        seen = jnp.where(site_row[None], at_col.reshape(16, 16, 128), 0.0)
        oall[e, 16 * c : 16 * c + 16, :] = jnp.sum(seen, axis=1)

    swap_seen = pltpu.make_async_remote_copy(
        src_ref=oall.at[e], dst_ref=oall.at[e], send_sem=xs.at[1], recv_sem=xr.at[1],
        device_id=pair, device_id_type=MESH,
    )
    swap_seen.start()
    got_seen = pltpu.make_async_remote_copy(
        src_ref=oall.at[e], dst_ref=oall.at[1 - e], send_sem=xs.at[1], recv_sem=xr.at[1],
        device_id=pair, device_id_type=MESH,
    )
    got_seen.wait_recv()
    swap_theta.wait_recv()

    seen = jnp.concatenate([oall[0], oall[1]], axis=0)
    mean = jnp.sum(seen, axis=0, keepdims=True) * (1.0 / 128.0)
    scale = 1.0 / osg[...]
    anomaly = (seen - mean) * scale
    miss = jnp.broadcast_to((ova[...] - mean) * scale, (8, 128))
    dims = (((1,), (1,)), ((), ()))
    gram = lax.dot_general(anomaly, anomaly, dims, precision=HIGHEST, preferred_element_type=F32)
    cvec = lax.dot_general(miss, anomaly, dims, precision=HIGHEST, preferred_element_type=F32)
    last = iota((128, 128), 0) == 127
    gp[...] = jnp.where(last, cvec[0:1, :], gram).reshape(8, 16, 128)

    owner, mine = lax.rem(g, 2) == 1, g // 2

    def to(src, dst, ssem, rsem, where):
        return pltpu.make_async_remote_copy(
            src_ref=src, dst_ref=dst, send_sem=ssem, recv_sem=rsem, device_id=where, device_id_type=MESH
        )

    def rows_to_owner(d):
        j = lax.rem(mine + d, 8)
        return to(gp.at[j], rs.at[g], rss.at[d], rsr.at[g], tile_holder(2 * j + 1))

    def rows_to_gx(d):
        where = {"gx": lax.rem(z + d, nz), "gy": g, "ens": e}
        return to(zs.at[z], zs.at[z], zss.at[d], zsr.at[z], where)

    def rows_to_all(d):
        return to(ag.at[mine], ag.at[mine], ags.at[d], agr.at[mine], tile_holder(lax.rem(g + d, ng)))

    def arrived(ref, i, rsem, ssem):
        to(ref.at[i], ref.at[i], ssem, rsem.at[i], pair).wait_recv()

    hear_word(2, False)
    for d in range(1, 8):
        rows_to_owner(d).start()
    pl.when(jnp.logical_not(owner))(lambda: rows_to_owner(0).start())

    @pl.when(owner)
    def _():
        rs[g] = gp[mine]
        for d in range(1, ng):
            arrived(rs, lax.rem(g + d, ng), rsr, rss.at[0])
        zs[z] = jnp.sum(rs[...], axis=0)
        for d in range(1, nz):
            rows_to_gx(d).start()
        for d in range(1, nz):
            arrived(zs, lax.rem(z + d, nz), zsr, zss.at[0])
        ag[mine] = jnp.sum(zs[...], axis=0)
        for d in range(1, ng):
            rows_to_all(d).start()

    thetas[...] = thx[...] + thr[...]
    def drain(copies):
        for copy, sends, _ in copies:
            when(sends, copy.wait_send)

    drain(halo(*extra, True))
    drain(halo(*extra, False))

    def drain_chunk(c, carry):
        drain(halo(*member_chunk(c), True))
        drain(halo(*member_chunk(c), False))
        return carry

    lax.fori_loop(0, 4, drain_chunk, 0)
    swap_theta.wait_send()
    swap_seen.wait_send()
    for d in range(1, 8):
        rows_to_owner(d).wait_send()
    pl.when(jnp.logical_not(owner))(lambda: rows_to_owner(0).wait_send())

    @pl.when(owner)
    def _():
        for d in range(1, nz):
            rows_to_gx(d).wait_send()

    for d in range(1, 8):
        arrived(ag, lax.rem(mine + d, 8), agr, ags.at[0])
    pl.when(jnp.logical_not(owner))(lambda: arrived(ag, mine, agr, ags.at[0]))
    sums[...] = ag[...].reshape(16, 8, 128)

    @pl.when(owner)
    def _():
        for d in range(1, ng):
            rows_to_all(d).wait_send()


def solve(fin, sums, thetas, fin_out, theta_out, mat, sem):
    e = lax.axis_index("ens")
    out_copy = pltpu.make_async_copy(fin, fin_out, sem)
    out_copy.start()
    th_all = thetas[...]
    th_mean = jnp.sum(th_all, axis=1, keepdims=True) * (1.0 / 128.0)
    mat[16] = th_all - th_mean
    crow = sums[15, 7:8, :]
    sub, ln = iota((8, 128), 0), iota((8, 128), 1)
    last = sub == 7
    tiles = [sums[t] for t in range(16)]
    tiles[15] = jnp.where(last, 0.0, tiles[15])
    total = tiles[0]
    for t in range(1, 16):
        total = total + tiles[t]
    total = jnp.sum(total, axis=0, keepdims=True)
    tiles[15] = jnp.where(last, -total, tiles[15])
    for t in range(16):
        mat[t] = tiles[t] + jnp.where(ln == sub + 8 * t, 127.0, 0.0)

    def lanes_of(x, base):
        return [jnp.broadcast_to(x[:, base + j : base + j + 1], (8, 128)) for j in range(8)]

    def row_of(x, i):
        return jnp.broadcast_to(x[i : i + 1, :], (8, 128))

    cols = lanes_of(tiles[0] + jnp.where(ln == sub, 127.0, 0.0), 0)
    for k in range(16):
        base = 8 * k
        front = (ln >= base) & (ln < base + 8)
        piv = mat[k]
        ahead = lanes_of(piv, base + 8) if k < 15 else []
        row = jnp.where(front, jnp.where(ln == sub + base, 1.0, 0.0), piv)
        scale = jnp.zeros((8, 128), F32)
        for i in range(8):
            inv = 1.0 / row_of(cols[i], i)
            mine = sub == i
            step = jnp.where(mine, 0.0, cols[i]) * inv
            scale = jnp.where(mine, inv, scale)
            row = row - step * row_of(row, i)
            for j in range(i + 1, 8):
                cols[j] = cols[j] - step * row_of(cols[j], i)
            ahead = [x - step * row_of(x, i) for x in ahead]
        row = row * scale
        ahead = [x * scale for x in ahead]
        row = jnp.where(front, -row, row)
        rows = [row_of(row, i) for i in range(8)]
        for t in range(k + 1, 17):
            x = mat[t]
            by = lanes_of(x, base)
            new = jnp.where(front, 0.0, x)
            for i in range(8):
                new = new - by[i] * rows[i]
            mat[t] = new
            if t == k + 1 and k < 15:
                cols = lanes_of(x, base + 8)
                for j in range(8):
                    for i in range(8):
                        cols[j] = cols[j] - by[i] * row_of(ahead[j], i)
    zt = mat[16]
    shift = jnp.sum(zt * crow, axis=1, keepdims=True)
    fresh = th_mean + 127.0 * zt + shift
    @pl.when(e == 0)
    def _():
        theta_out[...] = fresh[0:4, 0:64]

    @pl.when(e == 1)
    def _():
        theta_out[...] = fresh[0:4, 64:128]

    out_copy.wait()


def local(state, u_vel, v_vel, land, forcing, member_mode, theta, *obs):
    args = (member_mode, state, u_vel, v_vel, land, forcing, theta, *obs)
    hbm = pl.BlockSpec(memory_space=pl.ANY)
    vmem = pl.BlockSpec(memory_space=pltpu.VMEM)
    dma, v = pltpu.SemaphoreType.DMA, lambda *s: pltpu.VMEM(s, F32)
    shape = jax.ShapeDtypeStruct
    fin, sums, thetas = pl.pallas_call(
        kernel,
        out_shape=(shape(state.shape, F32), shape((16, 8, 128), F32), shape((8, 128), F32)),
        in_specs=[pl.BlockSpec(memory_space=pltpu.HBM)] * 10,
        out_specs=(vmem, vmem, vmem),
        scratch_shapes=[
            v(64, 32, 128), v(16, 32, 128), pltpu.VMEM((16, 128), jnp.int32),
            v(10, 32, 128), v(10, 32, 128), v(10, 32, 128), v(10, 32, 128),
            v(32, 128), v(3, 32, 128), v(2, 8, 32, 128), v(2, 3, 32, 128), v(4, 64, 128), v(4, 2, 8, 128),
            v(32, 32, 128), v(32, 32, 128), v(32, 32, 128), v(32, 32, 128),
            v(32, 32, 128), v(32, 16, 128),
            v(2, 64, 128), v(8, 128), v(8, 128),
            v(8, 16, 128), v(16, 16, 128), v(8, 16, 128), v(8, 16, 128),
            pltpu.VMEM((384, 128), jnp.bfloat16), v(4, 64), pltpu.VMEM((1, 128), jnp.int32), v(1, 128), v(1, 128), pltpu.SMEM((64,), jnp.int32),
            pltpu.SemaphoreType.REGULAR((3,)), pltpu.SemaphoreType.REGULAR((2,)), dma((10,)), dma((5, 12)), dma((5, 12)), dma((2,)), dma((2,)),
            dma((8,)), dma((16,)), dma((8,)), dma((8,)), dma((16,)), dma((8,)),
        ],
        compiler_params=pltpu.CompilerParams(collective_id=0, has_side_effects=True, vmem_limit_bytes=20 * 2**20),
    )(*[pltpu.with_memory_space_constraint(a, pltpu.HBM) for a in args])
    return pl.pallas_call(
        solve,
        out_shape=(shape(state.shape, F32), shape(theta.shape, F32)),
        in_specs=[hbm, vmem, vmem],
        out_specs=(hbm, vmem),
        scratch_shapes=[v(17, 8, 128), dma(())],
        compiler_params=pltpu.CompilerParams(vmem_limit_bytes=8 * 2**20),
    )(fin, sums, thetas)


def solution(mesh):
    in_specs = (
        P("ens", "gy", "gx"), P("gy", "gx"), P("gy", "gx"), P("gy", "gx"), P(None, "gy", "gx"),
        P("ens"), P("ens", None), P("gy", "gx", None), P("gy", "gx", None), P("gy", "gx", None),
    )
    out_specs = (P("ens", "gy", "gx"), P("ens", None))

    def run(state, u_vel, v_vel, land, forcing, member_mode, theta, obs_index, obs_values, obs_sigma):
        flat = [a.reshape(a.shape[1:]) for a in (obs_index, obs_values, obs_sigma)]
        fin, new = local(state, u_vel, v_vel, land, forcing, member_mode, theta.T, *flat)
        return fin, new.T

    return jax.shard_map(run, mesh=mesh, in_specs=in_specs, out_specs=out_specs, check_vma=False)
```
